8 devices in a mesh: fsdp: 2 (over z, y), tp: 4 (over x, core).
Axes of the slice: x: 2, y: 2, z: 1, core: 2. Of those that a mesh axis runs over, the one named last changes fastest.
Arguments:
- x: bfloat16 [16384, 6144], P(('fsdp', 'tp'))
- gamma: float32 [6144], replicated
- w1: bfloat16 [6144, 24576], P('fsdp', 'tp')
- w2: bfloat16 [24576, 6144], P('tp', 'fsdp')
Outputs:
- output: bfloat16 [16384, 6144], P(('fsdp', 'tp'))
All inputs are finite; a program needn't handle non-finite values.
Results may differ from the reference program's by a relative error of at most 0.001.
Values are sent between devices in bfloat16 or wider.
A program may use at most 1 GiB of HBM per device.

```python
import jax
import jax.numpy as jnp
from jax import lax

D = 6144
F = 24576
ROWS = 2048
FSDP = 2
TP = 4

TOK = FSDP * TP * ROWS
BLK = min(ROWS, 512)
EPS = 1e-6


def setup_inputs(seed: int = 0) -> dict:
    k = jax.random.split(jax.random.key(seed), 4)
    x = jax.random.normal(k[0], (TOK, D), jnp.float32).astype(jnp.bfloat16)
    gamma = jax.random.uniform(k[1], (D,), jnp.float32, 0.5, 1.5)
    w1 = (jax.random.normal(k[2], (D, F), jnp.float32) * D ** -0.5).astype(jnp.bfloat16)
    w2 = (jax.random.normal(k[3], (F, D), jnp.float32) * F ** -0.5).astype(jnp.bfloat16)
    return {"x": x, "gamma": gamma, "w1": w1, "w2": w2}


def _block(x, gamma, w1, w2):
    xf = x.astype(jnp.float32)
    mu = jnp.mean(xf, axis=-1, keepdims=True)
    var = jnp.mean(jnp.square(xf - mu), axis=-1, keepdims=True)
    xn = ((xf - mu) * lax.rsqrt(var + EPS) * gamma).astype(jnp.bfloat16)
    h = jax.nn.gelu(jnp.dot(xn, w1, preferred_element_type=jnp.float32), approximate=True).astype(jnp.bfloat16)
    y = jnp.dot(h, w2, preferred_element_type=jnp.float32)
    return (xf + y).astype(jnp.bfloat16)


def reference(x, gamma, w1, w2):
    xb = x.reshape(TOK // BLK, BLK, D)
    yb = lax.map(lambda blk: _block(blk, gamma, w1, w2), xb)
    return yb.reshape(TOK, D)
```

```python
import functools

import jax
import jax.numpy as jnp
from jax import lax
from jax.experimental import pallas as pl
from jax.experimental.pallas import tpu as pltpu
from jax.sharding import PartitionSpec as P

EPS = 1e-6
F32 = jnp.float32
BF16 = jnp.bfloat16
MESH = pl.DeviceIdType.MESH

N1 = 12
N2 = 6
NX = 8
AHEAD = 3
LAG = 2


def _where(cond, a, b):
    return jnp.where(cond, jnp.int32(a), jnp.int32(b))


def _mm1_step(s):
    segs = (
        (0, 0, 2, 0),
        (16, 0, 1, 2),
        (24, 4, 3, 0),
        (48, 0, 1, 3),
        (64, 8, 2, 2),
        (76, 8, 2, 0),
        (80, 11, 2, 2),
        (84, 9, 2, 0),
    )
    start, c0, nm, m0 = (jnp.int32(v) for v in segs[0])
    for g in segs[1:]:
        late = s >= g[0]
        start, c0, nm, m0 = (_where(late, new, old) for new, old in zip(g, (start, c0, nm, m0)))
    u = s - start
    pair = u // nm
    return c0 + pair // 2, pair % 2, m0 + u % nm


def _mm2_visit(v):
    n = 2 * N2
    u = v - LAG
    mid_own = u % 2
    mid = _where(mid_own == 1, u // 2, LAG + u // 2)
    own = _where(v < LAG, 0, _where(v < 2 * n - LAG, mid_own, 1))
    k = _where(v < LAG, v, _where(v < 2 * n - LAG, mid, v - n))
    return own, k


def _kernel(
    x, gamma, w1, w2,
    y, xn, w1far, w1so, w1sf, w2far, w2so, w2sf, h, psend, precv,
    act, wb, hout, pout, pin, xin, yout, gam,
    act_sem, w_sem, h_sem, io_sem,
    xn_s, xn_r, w1y_s, w1y_r, w1c_s, w1c_r, w1f_s, w1f_r,
    w2y_s, w2y_r, w2c_s, w2c_r, w2f_s, w2f_r, p_s, p_r,
):
    a = lax.axis_index("fsdp")
    b = lax.axis_index("tp")
    to_y = {"fsdp": 1 - a}
    to_x = {"tp": lax.rem(b + 2, 4)}
    to_c = {"tp": b + 1 - 2 * lax.rem(b, 2)}
    rows, d = x.shape
    half, fq = w1.shape
    sub = rows // 4
    tile = rows // 2
    c1 = fq // N1
    c2 = half // N2
    piece = rows // NX
    near = pl.multiple_of(a * half, half)
    away = pl.multiple_of((1 - a) * half, half)

    def remote(src, dst, ssem, rsem, to):
        return pltpu.make_async_remote_copy(
            src_ref=src, dst_ref=dst, send_sem=ssem, recv_sem=rsem, device_id=to, device_id_type=MESH
        )

    def cols1(j):
        return pl.ds(pl.multiple_of(j * c1, c1), c1)

    def cols2(k):
        return pl.ds(pl.multiple_of(k * c2, c2), c2)

    def w1_y(j):
        return remote(w1.at[:, cols1(j)], w1far.at[:, cols1(j)], w1y_s.at[j], w1y_r.at[j], to_y)

    def w1_c(j):
        return remote(w1.at[:, cols1(j)], w1so.at[:, cols1(j)], w1c_s.at[j], w1c_r.at[j], to_c)

    def w1_f(j):
        return remote(w1far.at[:, cols1(j)], w1sf.at[:, cols1(j)], w1f_s.at[j], w1f_r.at[j], to_c)

    def w2_y(k):
        return remote(w2.at[:, cols2(k)], w2far.at[:, cols2(k)], w2y_s.at[k], w2y_r.at[k], to_y)

    def w2_c(k):
        return remote(w2.at[:, cols2(k)], w2so.at[:, cols2(k)], w2c_s.at[k], w2c_r.at[k], to_c)

    def w2_f(k):
        return remote(w2far.at[:, cols2(k)], w2sf.at[:, cols2(k)], w2f_s.at[k], w2f_r.at[k], to_c)

    def xrows(t):
        return pl.ds(pl.multiple_of(t * piece, piece), piece)

    def xn_x(t):
        return remote(xn.at[xrows(t)], xn.at[xrows(t + NX)], xn_s.at[t], xn_r.at[t], to_x)

    def p_x(i, k):
        at = (pl.ds(pl.multiple_of(i * sub, sub), sub), cols2(k))
        return remote(psend.at[at], precv.at[at], p_s.at[k * 4 + i], p_r.at[k * 4 + i], to_x)

    barrier = pltpu.get_barrier_semaphore()
    for to in (to_y, to_x, to_c):
        pl.semaphore_signal(barrier, inc=1, device_id=to, device_id_type=MESH)
    pl.semaphore_wait(barrier, 3)

    for j in range(AHEAD):
        w1_y(j).start()

    @pl.loop(0, N1)
    def _(j):
        w1_c(j).start()

    for i, off in enumerate((near, away)):
        g = pltpu.make_async_copy(gamma.at[:, pl.ds(off, half)], gam.at[:, i * half : (i + 1) * half], io_sem.at[i])
        g.start()

    def x_in(t, slot):
        return [
            pltpu.make_async_copy(
                x.at[xrows(t), pl.ds(off, half)],
                act.at[slot, 0:piece, i * half : (i + 1) * half],
                act_sem.at[slot, i],
            )
            for i, off in enumerate((near, away))
        ]

    for c in x_in(0, 0):
        c.start()
    for i, off in enumerate((near, away)):
        pltpu.make_async_copy(
            gamma.at[:, pl.ds(off, half)], gam.at[:, i * half : (i + 1) * half], io_sem.at[i]
        ).wait()

    @pl.loop(0, NX)
    def _(t):
        slot = t % 2

        @pl.when(t + 1 < NX)
        def _():
            for c in x_in(t + 1, 1 - slot):
                c.start()

        for c in x_in(t, slot):
            c.wait()

        @pl.loop(0, piece // 16)
        def _(r):
            at = pl.multiple_of(r * 16, 16)
            xs = act[slot, pl.ds(at, 16), 0:d].astype(F32)
            xc = xs - jnp.mean(xs, axis=1, keepdims=True)
            var = jnp.mean(xc * xc, axis=1, keepdims=True)
            act[slot, pl.ds(piece + at, 16), 0:d] = (xc * lax.rsqrt(var + EPS) * gam[...]).astype(BF16)

        out = pltpu.make_async_copy(act.at[slot, piece : 2 * piece, 0:d], xn.at[xrows(t)], io_sem.at[2])
        out.start()
        out.wait()

        @pl.when(t < NX // 2)
        def _():
            xn_x(t).start()

    def a1_in(m, slot):
        return [
            pltpu.make_async_copy(
                xn.at[pl.ds(pl.multiple_of(m * tile + r * sub, sub), sub)],
                act.at[slot, :, r * d : (r + 1) * d],
                act_sem.at[slot, r],
            )
            for r in range(2)
        ]

    def w1_in(j, q, slot, go):
        def pair(own, far):
            for i, ref in enumerate((own, far)):
                c = pltpu.make_async_copy(
                    ref.at[:, cols1(j)], wb.at[slot, i * half : (i + 1) * half], w_sem.at[slot, i]
                )
                c.start() if go else c.wait()

        if not go:
            pair(w1, w1far)
            return

        @pl.when(q == 0)
        def _():
            pair(w1, w1far)

        @pl.when(q == 1)
        def _():
            pair(w1so, w1sf)

    def arrive1(s):
        j, q, m = _mm1_step(s)
        first = m == _where(j < 8, 0, 2)

        @pl.when(first & (q == 0))
        def _():
            w1_y(j).wait_recv()
            w1_f(j).start()

            @pl.when(j + AHEAD < N1)
            def _():
                w1_y(j + AHEAD).start()

            @pl.when(j + AHEAD >= N1)
            def _():
                w2_y(j + AHEAD - N1).start()

            @pl.when(j == 2)
            def _():
                for t in range(NX // 2, NX):
                    xn_x(t).start()

            @pl.when(j == 4)
            def _():
                for k in range(N2):
                    w2_c(k).start()

        @pl.when(first & (q == 1))
        def _():
            w1_c(j).wait_recv()
            w1_f(j).wait_recv()

        @pl.when(s == 16)
        def _():
            for t in range(NX // 2):
                xn_x(t).wait_recv()

        @pl.when(s == 48)
        def _():
            for t in range(NX // 2, NX):
                xn_x(t).wait_recv()

    def load1(s, aslot, wslot, a_new, w_new):
        j, q, m = _mm1_step(s)

        @pl.when(a_new)
        def _():
            for c in a1_in(m, aslot):
                c.start()

        @pl.when(w_new)
        def _():
            w1_in(j, q, wslot, True)

    def h_out(s):
        j, q, m = _mm1_step(s)
        col = pl.multiple_of(q * fq + j * c1, c1)
        return pltpu.make_async_copy(
            hout.at[s % 2], h.at[pl.ds(pl.multiple_of(m * tile, tile), tile), pl.ds(col, c1)], h_sem.at[s % 2]
        )

    def first_product(lo, hi):
        arrive1(lo)
        load1(lo, 0, 0, True, True)

        def step(s, carry):
            aslot, wslot, a_fresh, w_fresh = carry
            j, q, m = _mm1_step(s)
            nj, nq, nm = _mm1_step(s + 1)
            more = s + 1 < hi
            a_new = more & (nm != m)
            w_new = more & ((nj != j) | (nq != q))
            na = _where(a_new, 1 - aslot, aslot)
            nw = _where(w_new, 1 - wslot, wslot)

            @pl.when(more)
            def _():
                arrive1(s + 1)

            load1(s + 1, na, nw, a_new, w_new)

            @pl.when(a_fresh == 1)
            def _():
                for c in a1_in(m, aslot):
                    c.wait()

            @pl.when(w_fresh == 1)
            def _():
                w1_in(j, q, wslot, False)

            @pl.when(s >= lo + 2)
            def _():
                h_out(s - 2).wait()

            for r in range(2):
                u = jnp.dot(act[aslot, :, r * d : (r + 1) * d], wb[wslot, 0:d], preferred_element_type=F32)
                hout[s % 2, r * sub : (r + 1) * sub] = jax.nn.gelu(u, approximate=True).astype(BF16)
            h_out(s).start()
            return na, nw, _where(a_new, 1, 0), _where(w_new, 1, 0)

        one, nil = jnp.int32(1), jnp.int32(0)
        lax.fori_loop(lo, hi, step, (nil, nil, one, one))
        h_out(hi - 2).wait()
        h_out(hi - 1).wait()

    def a2_in(own, i, slot):
        at = pl.multiple_of(_where(own == 1, 0, rows) + i * sub, sub)
        return pltpu.make_async_copy(h.at[pl.ds(at, sub)], act.at[slot], act_sem.at[slot, 0])

    def w2_in(k, slot, go):
        def pair(kk, own, sib):
            for i, ref in enumerate((own, sib)):
                c = pltpu.make_async_copy(
                    ref.at[:, cols2(kk)], wb.at[slot, i * fq : (i + 1) * fq], w_sem.at[slot, i]
                )
                c.start() if go else c.wait()

        if not go:
            pair(0, w2, w2so)
            return

        @pl.when(k < N2)
        def _():
            pair(k, w2, w2so)

        @pl.when(k >= N2)
        def _():
            pair(k - N2, w2far, w2sf)

    def arrive2(v):
        own, k = _mm2_visit(v)

        @pl.when((own == 0) & (k < N2))
        def _():
            w2_c(k).wait_recv()

        @pl.when((own == 0) & (k >= N2))
        def _():
            w2_f(k - N2).wait_recv()

        @pl.when((own == 0) & (k >= 1) & (k + AHEAD - 1 < N2))
        def _():
            w2_y(k + AHEAD - 1).start()

        @pl.when((own == 1) & (k >= 3) & (k < 3 + N2))
        def _():
            w2_y(k - 3).wait_recv()
            w2_f(k - 3).start()

    def second_product(lo, hi):
        arrive2(lo)
        own0, k0 = _mm2_visit(lo)
        a2_in(own0, 0, 0).start()
        w2_in(k0, 0, True)

        def step(s, carry):
            v, i = s // 4, s % 4
            own, k = _mm2_visit(v)
            aslot = (s - lo * 4) % 2
            wslot = (v - lo) % 2
            more = s + 1 < hi * 4
            nv, ni = (s + 1) // 4, (s + 1) % 4
            nown, nk = _mm2_visit(nv)

            @pl.when(more & (ni == 0))
            def _():
                arrive2(nv)
                w2_in(nk, 1 - wslot, True)

            @pl.when(more)
            def _():
                a2_in(nown, ni, 1 - aslot).start()

            a2_in(own, i, aslot).wait()

            @pl.when(i == 0)
            def _():
                w2_in(k, wslot, False)

            at = pl.ds(pl.multiple_of(i * sub, sub), sub)
            ycol = pl.multiple_of(_where(k < N2, near, away) + (k % N2) * c2, c2)
            x_tile = pltpu.make_async_copy(x.at[at, pl.ds(ycol, c2)], xin, io_sem.at[0])
            y_tile = pltpu.make_async_copy(yout, y.at[at, pl.ds(ycol, c2)], io_sem.at[3])

            @pl.when(own == 1)
            def _():
                x_tile.start()

            pout[...] = jnp.dot(act[aslot], wb[wslot], preferred_element_type=F32)

            @pl.when(own == 0)
            def _():
                out = pltpu.make_async_copy(pout, psend.at[at, cols2(k)], io_sem.at[1])
                out.start()
                out.wait()
                p_x(i, k).start()

            @pl.when(own == 1)
            def _():
                p_x(i, k).wait_recv()
                got = pltpu.make_async_copy(precv.at[at, cols2(k)], pin, io_sem.at[2])
                got.start()
                x_tile.wait()
                got.wait()
                yout[...] = (xin[...].astype(F32) + (pout[...] + pin[...])).astype(BF16)
                y_tile.start()
                y_tile.wait()

            return carry

        lax.fori_loop(lo * 4, hi * 4, step, jnp.int32(0))

    @pl.loop(0, 2)
    def _(phase):
        first_product(_where(phase == 0, 0, 84), _where(phase == 0, 84, 96))
        second_product(_where(phase == 0, 0, LAG), _where(phase == 0, LAG, 4 * N2))

    @pl.loop(0, N1)
    def _(j):
        w1_y(j).wait_send()
        w1_c(j).wait_send()
        w1_f(j).wait_send()

    @pl.loop(0, N2)
    def _(k):
        w2_y(k).wait_send()
        w2_c(k).wait_send()
        w2_f(k).wait_send()

    @pl.loop(0, NX)
    def _(t):
        xn_x(t).wait_send()

    @pl.loop(0, 2 * N2 * 4)
    def _(s):
        p_x(s % 4, s // 4).wait_send()


def solution(mesh):
    def body(x, gamma, w1, w2):
        rows, d = x.shape
        half, fq = w1.shape
        sub = rows // 4
        c1, c2 = fq // N1, half // N2

        def hbm(shape, dtype):
            return jax.ShapeDtypeStruct(shape, dtype)

        dma = pltpu.SemaphoreType.DMA
        outs = pl.pallas_call(
            _kernel,
            name="mlp",
            out_shape=(
                hbm((rows, d), BF16),
                hbm((2 * rows, d), BF16),
                hbm((half, fq), BF16),
                hbm((half, fq), BF16),
                hbm((half, fq), BF16),
                hbm((fq, half), BF16),
                hbm((fq, half), BF16),
                hbm((fq, half), BF16),
                hbm((2 * rows, 2 * fq), BF16),
                hbm((rows, d), F32),
                hbm((rows, d), F32),
            ),
            in_specs=[pl.BlockSpec(memory_space=pl.ANY)] * 4,
            out_specs=tuple([pl.BlockSpec(memory_space=pl.ANY)] * 11),
            scratch_shapes=[
                pltpu.VMEM((2, sub, 2 * d), BF16),
                pltpu.VMEM((2, 2 * fq, c2), BF16),
                pltpu.VMEM((2, 2 * sub, c1), BF16),
                pltpu.VMEM((sub, c2), F32),
                pltpu.VMEM((sub, c2), F32),
                pltpu.VMEM((sub, c2), BF16),
                pltpu.VMEM((sub, c2), BF16),
                pltpu.VMEM((1, d), F32),
                dma((2, 2)), dma((2, 2)), dma((2,)), dma((4,)),
                dma((NX,)), dma((NX,)),
                dma((N1,)), dma((N1,)), dma((N1,)), dma((N1,)), dma((N1,)), dma((N1,)),
                dma((N2,)), dma((N2,)), dma((N2,)), dma((N2,)), dma((N2,)), dma((N2,)),
                dma((8 * N2,)), dma((8 * N2,)),
            ],
            compiler_params=pltpu.CompilerParams(
                collective_id=0, has_side_effects=True, vmem_limit_bytes=66_000_000
            ),
        )(x, gamma.reshape(1, d), w1, w2)
        return outs[0]

    return jax.shard_map(
        body,
        mesh=mesh,
        in_specs=(P(("fsdp", "tp"), None), P(None), P("fsdp", "tp"), P("tp", "fsdp")),
        out_specs=P(("fsdp", "tp"), None),
        check_vma=False,
    )
```

```python
import functools

import jax
import jax.numpy as jnp
from jax import lax
from jax.experimental import pallas as pl
from jax.experimental.pallas import tpu as pltpu
from jax.sharding import PartitionSpec as P

EPS = 1e-6
F32 = jnp.float32
BF16 = jnp.bfloat16
MESH = pl.DeviceIdType.MESH

N1 = 12
N2 = 6
NX = 8
AHEAD = 3
LAG = 3


def _where(cond, a, b):
    return jnp.where(cond, jnp.int32(a), jnp.int32(b))


def _mm1_step(s):
    segs = (
        (0, 0, 2, 0),
        (16, 0, 1, 2),
        (24, 4, 3, 0),
        (48, 0, 1, 3),
        (64, 8, 2, 2),
        (76, 8, 2, 0),
    )
    start, c0, nm, m0 = (jnp.int32(v) for v in segs[0])
    for g in segs[1:]:
        late = s >= g[0]
        start, c0, nm, m0 = (_where(late, new, old) for new, old in zip(g, (start, c0, nm, m0)))
    u = s - start
    pair = u // nm
    return c0 + pair // 2, pair % 2, m0 + u % nm


def _mm2_visit(v):
    n = 2 * N2
    u = v - LAG
    mid_own = u % 2
    mid = _where(mid_own == 1, u // 2, LAG + u // 2)
    own = _where(v < LAG, 0, _where(v < 2 * n - LAG, mid_own, 1))
    k = _where(v < LAG, v, _where(v < 2 * n - LAG, mid, v - n))
    return own, k


def _kernel(
    x, gamma, w1, w2,
    y, xn, w1far, w1so, w1sf, w2far, w2so, w2sf, h, psend, precv,
    act, wb, hout, pout, pin, xin, yout, gam,
    act_sem, w_sem, h_sem, io_sem, tail_sem,
    xn_s, xn_r, w1y_s, w1y_r, w1c_s, w1c_r, w1f_s, w1f_r,
    w2y_s, w2y_r, w2c_s, w2c_r, w2f_s, w2f_r, p_s, p_r,
):
    a = lax.axis_index("fsdp")
    b = lax.axis_index("tp")
    to_y = {"fsdp": 1 - a}
    to_x = {"tp": lax.rem(b + 2, 4)}
    to_c = {"tp": b + 1 - 2 * lax.rem(b, 2)}
    rows, d = x.shape
    half, fq = w1.shape
    sub = rows // 4
    tile = rows // 2
    c1 = fq // N1
    c2 = half // N2
    cb = c1 // 2
    t0 = fq - c1
    piece = rows // NX
    near = pl.multiple_of(a * half, half)
    away = pl.multiple_of((1 - a) * half, half)

    def remote(src, dst, ssem, rsem, to):
        return pltpu.make_async_remote_copy(
            src_ref=src, dst_ref=dst, send_sem=ssem, recv_sem=rsem, device_id=to, device_id_type=MESH
        )

    def cols1(j):
        return pl.ds(pl.multiple_of(j * c1, c1), c1)

    def cols2(k):
        return pl.ds(pl.multiple_of(k * c2, c2), c2)

    def w1_y(j):
        return remote(w1.at[:, cols1(j)], w1far.at[:, cols1(j)], w1y_s.at[j], w1y_r.at[j], to_y)

    def w1_c(j):
        return remote(w1.at[:, cols1(j)], w1so.at[:, cols1(j)], w1c_s.at[j], w1c_r.at[j], to_c)

    def w1_f(j):
        return remote(w1far.at[:, cols1(j)], w1sf.at[:, cols1(j)], w1f_s.at[j], w1f_r.at[j], to_c)

    def cols_t(t):
        return pl.ds(t0 + t * cb, cb)

    def w1_yt(t):
        at = (slice(None), cols_t(t))
        return remote(w1.at[at], w1far.at[at], w1y_s.at[N1 - 1 + t], w1y_r.at[N1 - 1 + t], to_y)

    def w1_ft(t):
        at = (slice(None), cols_t(t))
        return remote(w1far.at[at], w1sf.at[at], w1f_s.at[N1 - 1 + t], w1f_r.at[N1 - 1 + t], to_c)

    def w2_y(k):
        return remote(w2.at[:, cols2(k)], w2far.at[:, cols2(k)], w2y_s.at[k], w2y_r.at[k], to_y)

    def w2_c(k):
        return remote(w2.at[:, cols2(k)], w2so.at[:, cols2(k)], w2c_s.at[k], w2c_r.at[k], to_c)

    def w2_f(k):
        return remote(w2far.at[:, cols2(k)], w2sf.at[:, cols2(k)], w2f_s.at[k], w2f_r.at[k], to_c)

    def xrows(t):
        return pl.ds(pl.multiple_of(t * piece, piece), piece)

    def xn_x(t):
        return remote(xn.at[xrows(t)], xn.at[xrows(t + NX)], xn_s.at[t], xn_r.at[t], to_x)

    def p_x(i, k):
        at = (pl.ds(pl.multiple_of(i * sub, sub), sub), cols2(k))
        return remote(psend.at[at], precv.at[at], p_s.at[k * 4 + i], p_r.at[k * 4 + i], to_x)

    barrier = pltpu.get_barrier_semaphore()
    for to in (to_y, to_x, to_c):
        pl.semaphore_signal(barrier, inc=1, device_id=to, device_id_type=MESH)
    pl.semaphore_wait(barrier, 3)

    for j in range(AHEAD):
        w1_y(j).start()

    @pl.loop(0, N1)
    def _(j):
        w1_c(j).start()

    for i, off in enumerate((near, away)):
        g = pltpu.make_async_copy(gamma.at[:, pl.ds(off, half)], gam.at[:, i * half : (i + 1) * half], io_sem.at[i])
        g.start()

    def x_in(t, slot):
        return [
            pltpu.make_async_copy(
                x.at[xrows(t), pl.ds(off, half)],
                act.at[slot, 0:piece, i * half : (i + 1) * half],
                act_sem.at[slot, i],
            )
            for i, off in enumerate((near, away))
        ]

    for c in x_in(0, 0):
        c.start()
    for i, off in enumerate((near, away)):
        pltpu.make_async_copy(
            gamma.at[:, pl.ds(off, half)], gam.at[:, i * half : (i + 1) * half], io_sem.at[i]
        ).wait()

    @pl.loop(0, NX)
    def _(t):
        slot = t % 2

        @pl.when(t + 1 < NX)
        def _():
            for c in x_in(t + 1, 1 - slot):
                c.start()

        for c in x_in(t, slot):
            c.wait()

        @pl.loop(0, piece // 16)
        def _(r):
            at = pl.multiple_of(r * 16, 16)
            xs = act[slot, pl.ds(at, 16), 0:d].astype(F32)
            xc = xs - jnp.mean(xs, axis=1, keepdims=True)
            var = jnp.mean(xc * xc, axis=1, keepdims=True)
            act[slot, pl.ds(piece + at, 16), 0:d] = (xc * lax.rsqrt(var + EPS) * gam[...]).astype(BF16)

        out = pltpu.make_async_copy(act.at[slot, piece : 2 * piece, 0:d], xn.at[xrows(t)], io_sem.at[2])
        out.start()
        out.wait()

        @pl.when(t < NX // 2)
        def _():
            xn_x(t).start()

    def a1_in(m, slot):
        return [
            pltpu.make_async_copy(
                xn.at[pl.ds(pl.multiple_of(m * tile + r * sub, sub), sub)],
                act.at[slot, :, r * d : (r + 1) * d],
                act_sem.at[slot, r],
            )
            for r in range(2)
        ]

    def w1_in(j, q, slot, go):
        def pair(own, far):
            for i, ref in enumerate((own, far)):
                c = pltpu.make_async_copy(
                    ref.at[:, cols1(j)], wb.at[slot, i * half : (i + 1) * half], w_sem.at[slot, i]
                )
                c.start() if go else c.wait()

        if not go:
            pair(w1, w1far)
            return

        @pl.when(q == 0)
        def _():
            pair(w1, w1far)

        @pl.when(q == 1)
        def _():
            pair(w1so, w1sf)

    def arrive1(s):
        j, q, m = _mm1_step(s)
        first = m == _where(j < 8, 0, 2)

        @pl.when(first & (q == 0))
        def _():
            w1_y(j).wait_recv()
            w1_f(j).start()

            @pl.when(j + AHEAD < N1 - 1)
            def _():
                w1_y(j + AHEAD).start()

            @pl.when(j + AHEAD == N1 - 1)
            def _():
                w1_yt(0).start()
                w1_yt(1).start()

            @pl.when(j == 2)
            def _():
                for t in range(NX // 2, NX):
                    xn_x(t).start()

            @pl.when(j == 4)
            def _():
                for k in range(N2):
                    w2_c(k).start()

        @pl.when(first & (q == 1))
        def _():
            w1_c(j).wait_recv()
            w1_f(j).wait_recv()

        @pl.when(s == 16)
        def _():
            for t in range(NX // 2):
                xn_x(t).wait_recv()

        @pl.when(s == 48)
        def _():
            for t in range(NX // 2, NX):
                xn_x(t).wait_recv()

    def load1(s, aslot, wslot, a_new, w_new):
        j, q, m = _mm1_step(s)

        @pl.when(a_new)
        def _():
            for c in a1_in(m, aslot):
                c.start()

        @pl.when(w_new)
        def _():
            w1_in(j, q, wslot, True)

    def h_out(s):
        j, q, m = _mm1_step(s)
        col = pl.multiple_of(q * fq + j * c1, c1)
        return pltpu.make_async_copy(
            hout.at[s % 2], h.at[pl.ds(pl.multiple_of(m * tile, tile), tile), pl.ds(col, c1)], h_sem.at[s % 2]
        )

    def first_product(lo, hi):
        arrive1(lo)
        load1(lo, 0, 0, True, True)

        def step(s, carry):
            aslot, wslot, a_fresh, w_fresh = carry
            j, q, m = _mm1_step(s)
            nj, nq, nm = _mm1_step(s + 1)
            more = s + 1 < hi
            a_new = more & (nm != m)
            w_new = more & ((nj != j) | (nq != q))
            na = _where(a_new, 1 - aslot, aslot)
            nw = _where(w_new, 1 - wslot, wslot)

            @pl.when(more)
            def _():
                arrive1(s + 1)

            load1(s + 1, na, nw, a_new, w_new)

            @pl.when(a_fresh == 1)
            def _():
                for c in a1_in(m, aslot):
                    c.wait()

            @pl.when(w_fresh == 1)
            def _():
                w1_in(j, q, wslot, False)

            @pl.when(s >= lo + 2)
            def _():
                h_out(s - 2).wait()

            for r in range(2):
                u = jnp.dot(act[aslot, :, r * d : (r + 1) * d], wb[wslot, 0:d], preferred_element_type=F32)
                hout[s % 2, r * sub : (r + 1) * sub] = jax.nn.gelu(u, approximate=True).astype(BF16)
            h_out(s).start()
            return na, nw, _where(a_new, 1, 0), _where(w_new, 1, 0)

        one, nil = jnp.int32(1), jnp.int32(0)
        lax.fori_loop(lo, hi, step, (nil, nil, one, one))
        h_out(hi - 2).wait()
        h_out(hi - 1).wait()

    def a2_in(own, i, slot):
        at = pl.multiple_of(_where(own == 1, 0, rows) + i * sub, sub)
        return pltpu.make_async_copy(h.at[pl.ds(at, sub)], act.at[slot], act_sem.at[slot, 0])

    def w2_in(k, slot, go):
        def pair(kk, own, sib):
            for i, ref in enumerate((own, sib)):
                c = pltpu.make_async_copy(
                    ref.at[:, cols2(kk)], wb.at[slot, i * fq : (i + 1) * fq], w_sem.at[slot, i]
                )
                c.start() if go else c.wait()

        if not go:
            pair(0, w2, w2so)
            return

        @pl.when(k < N2)
        def _():
            pair(k, w2, w2so)

        @pl.when(k >= N2)
        def _():
            pair(k - N2, w2far, w2sf)

    def arrive2(v):
        own, k = _mm2_visit(v)

        @pl.when((own == 0) & (k < N2))
        def _():
            w2_c(k).wait_recv()

        @pl.when((own == 0) & (k >= N2))
        def _():
            w2_f(k - N2).wait_recv()

        @pl.when((own == 0) & (k >= 1) & (k + AHEAD - 1 < N2))
        def _():
            w2_y(k + AHEAD - 1).start()

        @pl.when((own == 1) & (k >= 5 - LAG) & (k < 5 - LAG + N2))
        def _():
            w2_y(k - (5 - LAG)).wait_recv()
            w2_f(k - (5 - LAG)).start()

    def second_product(lo, hi):
        arrive2(lo)
        own0, k0 = _mm2_visit(lo)
        a2_in(own0, 0, 0).start()
        w2_in(k0, 0, True)

        def step(s, carry):
            v, i = s // 4, s % 4
            own, k = _mm2_visit(v)
            aslot = (s - lo * 4) % 2
            wslot = (v - lo) % 2
            more = s + 1 < hi * 4
            nv, ni = (s + 1) // 4, (s + 1) % 4
            nown, nk = _mm2_visit(nv)

            @pl.when(more & (ni == 0))
            def _():
                arrive2(nv)
                w2_in(nk, 1 - wslot, True)

            @pl.when(more)
            def _():
                a2_in(nown, ni, 1 - aslot).start()

            a2_in(own, i, aslot).wait()

            @pl.when(i == 0)
            def _():
                w2_in(k, wslot, False)

            at = pl.ds(pl.multiple_of(i * sub, sub), sub)
            ycol = pl.multiple_of(_where(k < N2, near, away) + (k % N2) * c2, c2)
            x_tile = pltpu.make_async_copy(x.at[at, pl.ds(ycol, c2)], xin, io_sem.at[0])
            y_tile = pltpu.make_async_copy(yout, y.at[at, pl.ds(ycol, c2)], io_sem.at[3])

            @pl.when(own == 1)
            def _():
                x_tile.start()

            pout[...] = jnp.dot(act[aslot], wb[wslot], preferred_element_type=F32)

            @pl.when(own == 0)
            def _():
                out = pltpu.make_async_copy(pout, psend.at[at, cols2(k)], io_sem.at[1])
                out.start()
                out.wait()
                p_x(i, k).start()

            @pl.when(own == 1)
            def _():
                p_x(i, k).wait_recv()
                got = pltpu.make_async_copy(precv.at[at, cols2(k)], pin, io_sem.at[2])
                got.start()
                x_tile.wait()
                got.wait()
                yout[...] = (xin[...].astype(F32) + (pout[...] + pin[...])).astype(BF16)
                y_tile.start()
                y_tile.wait()

            return carry

        lax.fori_loop(lo * 4, hi * 4, step, jnp.int32(0))

    def junction():
        def w_tail(t, part):
            refs = ((w1, w1so), (w1far, w1sf))[part]
            return [
                pltpu.make_async_copy(
                    refs[q].at[:, cols_t(t)],
                    wb.at[0, t * d + part * half : t * d + (part + 1) * half, q * cb : (q + 1) * cb],
                    tail_sem.at[t, part, q],
                )
                for q in range(2)
            ]

        def xn_in(i):
            at = pl.multiple_of(rows + i * sub, sub)
            return pltpu.make_async_copy(xn.at[pl.ds(at, sub)], act.at[1, :, 0:d], act_sem.at[1, 0])

        def h_at(i, q, col, width):
            return h.at[pl.ds(pl.multiple_of(rows + i * sub, sub), sub), q * fq + col : q * fq + col + width]

        def h_in(i):
            return [
                pltpu.make_async_copy(h_at(i, q, 0, t0), act.at[0, :, q * fq : q * fq + t0], act_sem.at[0, q])
                for q in range(2)
            ]

        def arrive(t):
            w1_yt(t).wait_recv()
            w1_ft(t).start()
            if t == 1:
                for k in range(AHEAD):
                    w2_y(k).start()
            w1_ft(t).wait_recv()
            for c in w_tail(t, 1):
                c.start()
            for part in range(2):
                for c in w_tail(t, part):
                    c.wait()

        w1_c(N1 - 1).wait_recv()
        for t in range(2):
            for c in w_tail(t, 0):
                c.start()
        xn_in(0).start()
        for c in h_in(0):
            c.start()
        w2_c(0).wait_recv()
        w2_in(jnp.int32(0), 1, True)
        arrive(0)
        w2_in(jnp.int32(0), 1, False)

        def tile_(i, carry):
            xn_in(i).wait()
            u = jnp.dot(act[1, :, 0:d], wb[0, 0:d], preferred_element_type=F32)
            g = jax.nn.gelu(u, approximate=True).astype(BF16)
            for c in h_in(i):
                c.wait()
            first = []
            for q in range(2):
                act[0, :, q * fq + t0 : q * fq + t0 + cb] = g[:, q * cb : (q + 1) * cb]
                first.append(
                    pltpu.make_async_copy(
                        act.at[0, :, q * fq + t0 : q * fq + t0 + cb], h_at(i, q, t0, cb), h_sem.at[q]
                    )
                )
                first[-1].start()
            n = fq - cb
            pout[...] = jnp.dot(act[0, :, 0:n], wb[1, 0:n], preferred_element_type=F32) + jnp.dot(
                act[0, :, fq : fq + n], wb[1, fq : fq + n], preferred_element_type=F32
            )
            for c in first:
                c.wait()

            @pl.when(i < 3)
            def _():
                for c in h_in(i + 1):
                    c.start()

            @pl.when(i == 0)
            def _():
                arrive(1)

            u = jnp.dot(act[1, :, 0:d], wb[0, d : 2 * d], preferred_element_type=F32)
            hout[0, 0:sub] = jax.nn.gelu(u, approximate=True).astype(BF16)

            @pl.when(i < 3)
            def _():
                xn_in(i + 1).start()

            second = []
            for q in range(2):
                second.append(
                    pltpu.make_async_copy(
                        hout.at[0, 0:sub, q * cb : (q + 1) * cb], h_at(i, q, t0 + cb, cb), h_sem.at[q]
                    )
                )
                second[-1].start()
            pout[...] += jnp.dot(hout[0, 0:sub, 0:cb], wb[1, n:fq], preferred_element_type=F32) + jnp.dot(
                hout[0, 0:sub, cb : 2 * cb], wb[1, fq + n : 2 * fq], preferred_element_type=F32
            )
            at = pl.ds(pl.multiple_of(i * sub, sub), sub)
            out = pltpu.make_async_copy(pout, psend.at[at, 0:c2], io_sem.at[1])
            out.start()
            out.wait()
            p_x(i, 0).start()
            for c in second:
                c.wait()
            return carry

        lax.fori_loop(0, 4, tile_, jnp.int32(0))

    @pl.loop(0, 2)
    def _(phase):
        first_product(_where(phase == 0, 0, 76), _where(phase == 0, 76, 92))
        pl.when(phase == 0)(junction)
        second_product(_where(phase == 0, 1, LAG), _where(phase == 0, LAG, 4 * N2))

    @pl.loop(0, N1 - 1)
    def _(j):
        w1_y(j).wait_send()
        w1_f(j).wait_send()

    for t in range(2):
        w1_yt(t).wait_send()
        w1_ft(t).wait_send()

    @pl.loop(0, N1)
    def _(j):
        w1_c(j).wait_send()

    @pl.loop(0, N2)
    def _(k):
        w2_y(k).wait_send()
        w2_c(k).wait_send()
        w2_f(k).wait_send()

    @pl.loop(0, NX)
    def _(t):
        xn_x(t).wait_send()

    @pl.loop(0, 2 * N2 * 4)
    def _(s):
        p_x(s % 4, s // 4).wait_send()


def _put(src, dst):
    dst[...] = src[...]


def solution(mesh):
    def body(x, gamma, w1, w2):
        rows, d = x.shape
        half, fq = w1.shape
        sub = rows // 4
        c1, c2 = fq // N1, half // N2

        def hbm(shape, dtype):
            return jax.ShapeDtypeStruct(shape, dtype)

        dma = pltpu.SemaphoreType.DMA
        outs = pl.pallas_call(
            _kernel,
            name="mlp",
            out_shape=(
                hbm((rows, d), BF16),
                hbm((2 * rows, d), BF16),
                hbm((half, fq), BF16),
                hbm((half, fq), BF16),
                hbm((half, fq), BF16),
                hbm((fq, half), BF16),
                hbm((fq, half), BF16),
                hbm((fq, half), BF16),
                hbm((2 * rows, 2 * fq), BF16),
                hbm((rows, d), F32),
                hbm((rows, d), F32),
            ),
            in_specs=[pl.BlockSpec(memory_space=pl.ANY)] * 4,
            out_specs=tuple([pl.BlockSpec(memory_space=pl.ANY)] * 11),
            scratch_shapes=[
                pltpu.VMEM((2, sub, 2 * d), BF16),
                pltpu.VMEM((2, 2 * fq, c2), BF16),
                pltpu.VMEM((2, 2 * sub, c1), BF16),
                pltpu.VMEM((sub, c2), F32),
                pltpu.VMEM((sub, c2), F32),
                pltpu.VMEM((sub, c2), BF16),
                pltpu.VMEM((sub, c2), BF16),
                pltpu.VMEM((1, d), F32),
                dma((2, 2)), dma((2, 2)), dma((2,)), dma((4,)), dma((2, 2, 2)),
                dma((NX,)), dma((NX,)),
                dma((N1 + 1,)), dma((N1 + 1,)), dma((N1,)), dma((N1,)), dma((N1 + 1,)), dma((N1 + 1,)),
                dma((N2,)), dma((N2,)), dma((N2,)), dma((N2,)), dma((N2,)), dma((N2,)),
                dma((8 * N2,)), dma((8 * N2,)),
            ],
            compiler_params=pltpu.CompilerParams(
                collective_id=0, has_side_effects=True, vmem_limit_bytes=66_000_000
            ),
        )(x, gamma.reshape(1, d), w1, w2)
        block = pl.BlockSpec((rows // 8, d), lambda i: (i, 0))
        return pl.pallas_call(
            _put,
            name="put",
            out_shape=hbm((rows, d), BF16),
            grid=(8,),
            in_specs=[block],
            out_specs=block,
        )(outs[0])

    return jax.shard_map(
        body,
        mesh=mesh,
        in_specs=(P(("fsdp", "tp"), None), P(None), P("fsdp", "tp"), P("tp", "fsdp")),
        out_specs=P(("fsdp", "tp"), None),
        check_vma=False,
    )
```

```python
import jax
import jax.numpy as jnp
from jax import lax
from jax.experimental import pallas as pl
from jax.experimental.pallas import tpu as pltpu
from jax.sharding import PartitionSpec as P

EPS = 1e-6
F32 = jnp.float32
BF16 = jnp.bfloat16
MESH = pl.DeviceIdType.MESH

N1 = 12
NR = N1 - 1
N2 = 6
NX = 8
AHEAD = 3

STEPS1 = (
    ((0, 4), (0, 2)),
    ((0, 4), (2, 1)),
    ((4, 2), (0, 3)),
    ((0, 3), (3, 1)),
    ((6, 1), (0, 3)),
    ((3, 4), (3, 1)),
    ((7, 1), (2, 2)),
    ((0, 8), (4, 1)),
    ((7, 1), (0, 2)),
    ((8, 2), (2, 3)),
    ((8, 5), (0, 2)),
)
BREAK1 = 10

REM, OWN, END = 0, 1, 2
R, A, B = ((lambda k, t=t: (t, k)) for t in (REM, OWN, END))
VISITS = (
    R(1), R(2), R(3), R(4),
    R(5), A(0), A(1), R(6), A(2), B(0), B(1), A(3), R(7), B(2), A(4), A(5), R(8), B(3), A(6), A(7), B(4), B(5),
    R(9), A(8), B(6), A(9), B(7), R(10), B(8), A(10), R(11), A(11), B(9), B(10), B(11),
)
BREAK2 = 4
PASS_F = {A(1): 0, B(1): 1, A(5): 2, B(5): 3, B(7): 4, R(11): 5}
PASS_G = {B(4): 0, A(11): 1}
SEND_F = {R(2): (2,), R(5): (3, 4), R(7): (5,)}
SEND_G = {R(2): 0, R(7): 1}


def _where(cond, a, b):
    return jnp.where(cond, jnp.int32(a), jnp.int32(b))


def _bounds1():
    at, out = 0, []
    for (_, nj), (_, nt) in STEPS1:
        out.append(at)
        at += nj * 2 * nt
    return out, at


def _step1(s):
    starts, _ = _bounds1()
    rows = [(at, j0, nt, t0) for at, ((j0, _), (t0, nt)) in zip(starts, STEPS1)]
    start, j0, nt, t0 = (jnp.int32(v) for v in rows[0])
    for row in rows[1:]:
        late = s >= row[0]
        start, j0, nt, t0 = (_where(late, new, old) for new, old in zip(row, (start, j0, nt, t0)))
    u = s - start
    pair = u // nt
    return j0 + pair // 2, pair % 2, t0 + u % nt


def _first_tile(j):
    return _where(j < 7, 0, _where(j < NR - 1, 2, _where(j == NR - 1, 9, 0)))


def _visit(v):
    code = jnp.int32(0)
    for n, (t, k) in enumerate(VISITS):
        code = _where(v == n, t * 16 + k, code)
    return code // 16, code % 16


def _kernel(
    x, gamma, w1, w2,
    y, xn, w1e, w1far, w1so, w1sf, w2e, w2far, w2so, w2sf, h, psend, pown, precv,
    act, wb, hout, pout, pin, pback, xin, yout, gam,
    act_sem, w_sem, h_sem, io_sem, out_sem, in_sem, tail_sem,
    xn_s, xn_r, e_s, e_r, w1y_s, w1y_r, w1c_s, w1c_r, w1f_s, w1f_r,
    w2y_s, w2y_r, w2c_s, w2c_r, w2f_s, w2f_r, p_s, p_r,
):
    a = lax.axis_index("fsdp")
    b = lax.axis_index("tp")
    to_y = {"fsdp": 1 - a}
    to_x = {"tp": lax.rem(b + 2, 4)}
    to_c = {"tp": b + 1 - 2 * lax.rem(b, 2)}
    rows, d = x.shape
    half, fq = w1.shape
    sub = rows // 4
    c1 = fq // N1
    c2 = half // N2
    cb = c1 // 2
    fr = NR * c1
    t0 = fr - c1
    kr = 2 * fr
    ke = 4 * c1
    wide = half // 2
    piece = rows // NX
    near = pl.multiple_of(a * half, half)
    away = pl.multiple_of((1 - a) * half, half)
    everything = slice(None)

    def remote(src, dst, ssem, rsem, to):
        return pltpu.make_async_remote_copy(
            src_ref=src, dst_ref=dst, send_sem=ssem, recv_sem=rsem, device_id=to, device_id_type=MESH
        )

    def cols1(j):
        return (everything, pl.ds(pl.multiple_of(j * c1, c1), c1))

    def cols2(k):
        return pl.ds(pl.multiple_of(k * c2, c2), c2)

    def w1_y(j):
        return remote(w1.at[cols1(j)], w1far.at[cols1(j)], w1y_s.at[j], w1y_r.at[j], to_y)

    def w1_ye():
        return remote(w1e, w1far.at[cols1(N1)], w1y_s.at[N1], w1y_r.at[N1], to_y)

    def w1_yr(j):
        return remote(w1far.at[cols1(j)], w1far.at[cols1(j)], w1y_s.at[j], w1y_r.at[j], to_y)

    def w1_c(j):
        return remote(w1.at[cols1(j)], w1so.at[cols1(j)], w1c_s.at[j], w1c_r.at[j], to_c)

    def w1_ce():
        return remote(w1e, w1so.at[cols1(N1)], w1c_s.at[N1], w1c_r.at[N1], to_c)

    def w1_cr(j):
        return remote(w1so.at[cols1(j)], w1so.at[cols1(j)], w1c_s.at[j], w1c_r.at[j], to_c)

    def w1_f(j):
        return remote(w1far.at[cols1(j)], w1sf.at[cols1(j)], w1f_s.at[j], w1f_r.at[j], to_c)

    def cols_t(t):
        return (everything, pl.ds(t0 + t * cb, cb))

    def tail_at(t):
        return NR - 1 if t == 0 else N1 + 1

    def w1_yt(t):
        return remote(w1.at[cols_t(t)], w1far.at[cols_t(t)], w1y_s.at[tail_at(t)], w1y_r.at[tail_at(t)], to_y)

    def w1_ft(t):
        return remote(w1far.at[cols_t(t)], w1sf.at[cols_t(t)], w1f_s.at[tail_at(t)], w1f_r.at[tail_at(t)], to_c)

    def w1_e():
        return remote(w1.at[cols1(N1 - 1)], w1e, e_s.at[0], e_r.at[0], to_x)

    def w2_e():
        return remote(w2.at[fr:fq], w2e, e_s.at[1], e_r.at[1], to_x)

    def w2_yf(k):
        at = (pl.ds(0, fr), cols2(k))
        return remote(w2.at[at], w2far.at[at], w2y_s.at[k], w2y_r.at[k], to_y)

    def w2_yg(g):
        at = (pl.ds(fr, c1), pl.ds(g * wide, wide))
        to = (pl.ds(fq, c1), pl.ds(g * wide, wide))
        return (
            remote(w2.at[at], w2far.at[at], w2y_s.at[N2 + 2 * g], w2y_r.at[N2 + 2 * g], to_y),
            remote(
                w2e.at[:, pl.ds(g * wide, wide)], w2far.at[to], w2y_s.at[N2 + 2 * g + 1], w2y_r.at[N2 + 2 * g + 1], to_y
            ),
        )

    def w2_c(k):
        at = (everything, cols2(k))
        return remote(w2.at[at], w2so.at[pl.ds(0, fq), cols2(k)], w2c_s.at[k], w2c_r.at[k], to_c)

    def w2_ce():
        return remote(w2e, w2so.at[fq : fq + c1], w2c_s.at[N2], w2c_r.at[N2], to_c)

    def w2_ff(k):
        at = (pl.ds(0, fr), cols2(k))
        return remote(w2far.at[at], w2sf.at[at], w2f_s.at[k], w2f_r.at[k], to_c)

    def w2_fg(g):
        at = (pl.ds(fr, 2 * c1), pl.ds(g * wide, wide))
        return remote(w2far.at[at], w2sf.at[at], w2f_s.at[N2 + g], w2f_r.at[N2 + g], to_c)

    def xrows(t):
        return pl.ds(pl.multiple_of(t * piece, piece), piece)

    def xn_x(t):
        return remote(xn.at[xrows(t)], xn.at[xrows(t + NX)], xn_s.at[t], xn_r.at[t], to_x)

    def p_x(i, k):
        at = (pl.ds(pl.multiple_of(i * sub, sub), sub), cols2(k))
        return remote(psend.at[at], precv.at[at], p_s.at[k * 4 + i], p_r.at[k * 4 + i], to_x)

    barrier = pltpu.get_barrier_semaphore()
    for to in (to_y, to_x, to_c):
        pl.semaphore_signal(barrier, inc=1, device_id=to, device_id_type=MESH)
    pl.semaphore_wait(barrier, 3)

    for j in range(AHEAD):
        w1_y(j).start()

    @pl.loop(0, N1)
    def _(j):
        w1_c(j).start()

    def gam_in():
        return [
            pltpu.make_async_copy(gamma.at[:, pl.ds(off, half)], gam.at[:, i * half : (i + 1) * half], io_sem.at[i])
            for i, off in enumerate((near, away))
        ]

    def x_in(t, slot):
        return [
            pltpu.make_async_copy(
                x.at[xrows(t), pl.ds(off, half)],
                act.at[slot, 0:piece, i * half : (i + 1) * half],
                act_sem.at[slot, i],
            )
            for i, off in enumerate((near, away))
        ]

    for c in gam_in():
        c.start()
    for c in x_in(0, 0):
        c.start()
    for c in gam_in():
        c.wait()

    @pl.loop(0, NX)
    def _(t):
        slot = t % 2

        @pl.when(t + 1 < NX)
        def _():
            for c in x_in(t + 1, 1 - slot):
                c.start()

        for c in x_in(t, slot):
            c.wait()

        @pl.loop(0, piece // 16)
        def _(r):
            at = pl.multiple_of(r * 16, 16)
            xs = act[slot, pl.ds(at, 16), 0:d].astype(F32)
            xc = xs - jnp.mean(xs, axis=1, keepdims=True)
            var = jnp.mean(xc * xc, axis=1, keepdims=True)
            act[slot, pl.ds(piece + at, 16), 0:d] = (xc * lax.rsqrt(var + EPS) * gam[...]).astype(BF16)

        out = pltpu.make_async_copy(act.at[slot, piece : 2 * piece, 0:d], xn.at[xrows(t)], io_sem.at[2])
        out.start()
        out.wait()

        @pl.when(t < NX // 2)
        def _():
            xn_x(t).start()

    def hcol(j, q):
        return pl.multiple_of(_where(j < NR, q * fr + j * c1, kr + (j - NR) * 2 * c1 + q * c1), c1)

    def tile_rows(m):
        return _where(m < 3, 2 * m, 3 + m), m < 3

    def hrows(r):
        return pl.ds(pl.multiple_of(r * sub, sub), sub)

    def a1_in(m, slot, go):
        r0, two = tile_rows(m)

        def one(i):
            c = pltpu.make_async_copy(
                xn.at[hrows(r0 + i)], act.at[slot, :, i * d : (i + 1) * d], act_sem.at[slot, i]
            )
            c.start() if go else c.wait()

        one(0)
        pl.when(two)(lambda: one(1))

    def w1_in(j, q, slot, go):
        def load(i, ref, at):
            c = pltpu.make_async_copy(ref.at[at], wb.at[slot, i * half : (i + 1) * half], w_sem.at[slot, i])
            c.start() if go else c.wait()

        if not go:
            for i in range(2):
                load(i, w1far, cols1(j))
            return
        pl.when((q == 0) & (j < N1))(lambda: load(0, w1, cols1(j)))
        pl.when((q == 0) & (j == N1))(lambda: load(0, w1e, (everything, everything)))
        pl.when(q == 0)(lambda: load(1, w1far, cols1(j)))

        @pl.when(q == 1)
        def _():
            load(0, w1so, cols1(j))
            load(1, w1sf, cols1(j))

    starts1, total1 = _bounds1()
    first2, first3, first4 = (
        next(at for at, (_, (m0, nm)) in zip(starts1, STEPS1) if m0 == m) for m in (2, 3, 4)
    )

    def arrive1(s):
        j, q, m = _step1(s)
        first = m == _first_tile(j)

        @pl.when(first & (q == 0))
        def _():
            w1_yr(j).wait_recv()
            w1_f(j).start()

            @pl.when(j + AHEAD < NR - 1)
            def _():
                w1_y(j + AHEAD).start()

            @pl.when(j + AHEAD == NR - 1)
            def _():
                w1_yt(0).start()
                w1_yt(1).start()
                w1_e().start()
                w2_e().start()

            @pl.when(j == 2)
            def _():
                for t in range(NX // 2, NX):
                    xn_x(t).start()

            @pl.when(j == 4)
            def _():
                for k in range(N2):
                    w2_c(k).start()

        @pl.when(first & (q == 1))
        def _():
            w1_cr(j).wait_recv()
            w1_f(j).wait_recv()

        for at, lo, hi in ((first2, 0, 4), (first3, 4, 6), (first4, 6, 8)):

            @pl.when(s == at)
            def _():
                for t in range(lo, hi):
                    xn_x(t).wait_recv()

    def load1(s, aslot, wslot, a_new, w_new):
        j, q, m = _step1(s)
        pl.when(a_new)(lambda: a1_in(m, aslot, True))
        pl.when(w_new)(lambda: w1_in(j, q, wslot, True))

    def h_out(s, i):
        j, q, m = _step1(s)
        r0, _ = tile_rows(m)
        return pltpu.make_async_copy(
            hout.at[s % 2, pl.ds(pl.multiple_of(i * sub, sub), sub)],
            h.at[hrows(r0 + i), pl.ds(hcol(j, q), c1)],
            h_sem.at[s % 2, i],
        )

    def h_done(s):
        _, two = tile_rows(_step1(s)[2])
        h_out(s, 0).wait()
        pl.when(two)(lambda: h_out(s, 1).wait())

    def first_product(lo, hi):
        arrive1(lo)
        load1(lo, 0, 0, True, True)

        def step(s, carry):
            aslot, wslot, a_fresh, w_fresh = carry
            j, q, m = _step1(s)
            nj, nq, nm = _step1(s + 1)
            more = s + 1 < hi
            a_new = more & (nm != m)
            w_new = more & ((nj != j) | (nq != q))
            na = _where(a_new, 1 - aslot, aslot)
            nw = _where(w_new, 1 - wslot, wslot)
            pl.when(more)(lambda: arrive1(s + 1))
            load1(s + 1, na, nw, a_new, w_new)
            pl.when(a_fresh == 1)(lambda: a1_in(m, aslot, False))
            pl.when(w_fresh == 1)(lambda: w1_in(j, q, wslot, False))
            pl.when(s >= lo + 2)(lambda: h_done(s - 2))
            _, two = tile_rows(m)

            @pl.loop(0, _where(two, 2, 1))
            def _(i):
                u = jnp.dot(
                    act[aslot, :, pl.ds(pl.multiple_of(i * d, d), d)], wb[wslot, 0:d], preferred_element_type=F32
                )
                hout[s % 2, pl.ds(pl.multiple_of(i * sub, sub), sub)] = jax.nn.gelu(u, approximate=True).astype(BF16)
                h_out(s, i).start()

            return na, nw, _where(a_new, 1, 0), _where(w_new, 1, 0)

        one, nil = jnp.int32(1), jnp.int32(0)
        lax.fori_loop(lo, hi, step, (nil, nil, one, one))
        h_done(hi - 2)
        h_done(hi - 1)

    def a2_in(typ, k, i, slot, go):
        r = _where(typ == REM, 4, 0) + i

        def wait_or_start(c):
            c.start() if go else c.wait()

        @pl.when(typ != END)
        def _():
            wait_or_start(pltpu.make_async_copy(h.at[hrows(r), 0:kr], act.at[slot, :, 0:kr], act_sem.at[slot, 0]))

        @pl.when(typ == END)
        def _():
            wait_or_start(
                pltpu.make_async_copy(h.at[hrows(r), kr : kr + ke], act.at[slot, :, 0:ke], act_sem.at[slot, 0])
            )
            ycol = pl.multiple_of(_where(k < N2, near, away) + (k % N2) * c2, c2)
            wait_or_start(pltpu.make_async_copy(pown.at[hrows(i), cols2(k)], pback.at[slot], in_sem.at[slot, 0]))
            wait_or_start(pltpu.make_async_copy(x.at[hrows(i), pl.ds(ycol, c2)], xin.at[slot], in_sem.at[slot, 1]))

    def w2_in(typ, k, slot, go):
        def load(n, at, rows_, ref, from_, kk):
            c = pltpu.make_async_copy(
                ref.at[pl.ds(from_, rows_), cols2(kk)], wb.at[slot, at : at + rows_], w_sem.at[slot, n]
            )
            c.start() if go else c.wait()

        def main(own, sib, kk):
            load(0, 0, fr, own, 0, kk)
            load(1, fr, fr, sib, 0, kk)

        def rest(own, ext, ext_at, sib, kk):
            load(0, 0, c1, own, fr, kk)
            load(1, c1, c1, sib, fr, kk)
            load(2, 2 * c1, c1, ext, ext_at, kk)
            load(3, 3 * c1, c1, sib, fq, kk)

        def both(side, kk, own, ext, ext_at, sib):
            pl.when(side & (typ != END))(lambda: main(own, sib, kk))
            pl.when(side & (typ == END))(lambda: rest(own, ext, ext_at, sib, kk))

        if not go:
            pl.when(typ != END)(lambda: main(w2far, w2sf, 0))
            pl.when(typ == END)(lambda: rest(w2far, w2far, fq, w2sf, 0))
            return
        both(k < N2, k, w2, w2e, 0, w2so)
        both(k >= N2, k - N2, w2far, w2far, fq, w2sf)

    def arrive2(v):
        at = {visit: n for n, visit in enumerate(VISITS)}
        for n in range(len(VISITS)):
            visit = VISITS[n]
            todo = []
            for u in SEND_F.get(visit, ()):
                todo.append(lambda u=u: w2_yf(u).start())
            if visit in SEND_G:
                todo.append(lambda g=SEND_G[visit]: [c.start() for c in w2_yg(g)])
            if visit in PASS_F:
                u = PASS_F[visit]
                todo.append(lambda u=u: (w2_yf(u).wait_recv(), w2_ff(u).start()))
            if visit in PASS_G:
                g = PASS_G[visit]
                todo.append(lambda g=g: ([c.wait_recv() for c in w2_yg(g)], w2_fg(g).start()))
            if visit[0] == REM:
                k = visit[1]
                todo.append(lambda k=k: w2_c(k).wait_recv() if k < N2 else w2_ff(k - N2).wait_recv())
            if n == min(at[B(k)] for k in range(N2)):
                todo.append(lambda: w2_ce().wait_recv())
            for g in range(2):
                if n == min(at[B(N2 + 3 * g + k)] for k in range(3)):
                    todo.append(lambda g=g: w2_fg(g).wait_recv())
            if todo:

                @pl.when(v == n)
                def _(todo=todo):
                    for f in todo:
                        f()

    def p_out(to, k, i, slot):
        return pltpu.make_async_copy(pout.at[slot], to.at[hrows(i), cols2(k)], out_sem.at[slot])

    def y_out(k, i, slot):
        ycol = pl.multiple_of(_where(k < N2, near, away) + (k % N2) * c2, c2)
        return pltpu.make_async_copy(yout.at[slot], y.at[hrows(i), pl.ds(ycol, c2)], out_sem.at[2 + slot])

    def finish(typ, k, i, slot):
        @pl.when((typ == REM) | (typ == OWN))
        def _():
            p_out(pown, k, i, slot).wait()

        @pl.when(typ == REM)
        def _():
            p_x(i, k).start()

        @pl.when(typ == END)
        def _():
            y_out(k, i, slot).wait()

    def second_product(lo, hi):
        arrive2(lo)
        typ0, k0 = _visit(lo)
        w2_in(typ0, k0, 0, True)
        a2_in(typ0, k0, jnp.int32(0), 0, True)

        def visit(v, carry):
            typ, k, ptyp, pk = carry
            more = v + 1 < hi
            ntyp, nk = _visit(v + 1)
            wslot = (v - lo) % 2

            def tile(i, before):
                btyp, bk, bi = before
                slot = i % 2
                last = i == 3

                @pl.when(last & more)
                def _():
                    arrive2(v + 1)
                    w2_in(ntyp, nk, 1 - wslot, True)

                @pl.when(more | (i < 3))
                def _():
                    a2_in(_where(last, ntyp, typ), _where(last, nk, k), _where(last, 0, i + 1), 1 - slot, True)

                a2_in(typ, k, i, slot, False)
                pl.when(i == 0)(lambda: w2_in(typ, k, wslot, False))

                @pl.when(typ != END)
                def _():
                    pout[slot] = jnp.dot(act[slot, :, 0:kr], wb[wslot, 0:kr], preferred_element_type=F32)

                @pl.when(typ == END)
                def _():
                    pout[slot] = jnp.dot(act[slot, :, 0:ke], wb[wslot, 0:ke], preferred_element_type=F32)

                finish(btyp, bk, bi, 1 - slot)
                pl.when(typ == OWN)(lambda: p_out(pown, k, i, slot).start())
                pl.when(typ == REM)(lambda: p_out(psend, k, i, slot).start())

                @pl.when(typ == END)
                def _():
                    p_x(i, k).wait_recv()
                    got = pltpu.make_async_copy(precv.at[hrows(i), cols2(k)], pin, io_sem.at[0])
                    got.start()
                    got.wait()
                    total = (pback[slot] + pout[slot]) + pin[...]
                    yout[slot] = (xin[slot].astype(F32) + total).astype(BF16)
                    y_out(k, i, slot).start()

                return typ, k, i

            ptyp, pk, _ = lax.fori_loop(0, 4, tile, (ptyp, pk, jnp.int32(3)))
            return ntyp, nk, ptyp, pk

        _, _, ptyp, pk = lax.fori_loop(lo, hi, visit, (typ0, k0, jnp.int32(3), jnp.int32(0)))
        finish(ptyp, pk, jnp.int32(3), 1)

    def junction():
        def w_tail(t, part):
            refs = ((w1, w1so), (w1far, w1sf))[part]
            return [
                pltpu.make_async_copy(
                    refs[q].at[cols_t(t)],
                    wb.at[0, t * d + part * half : t * d + (part + 1) * half, q * cb : (q + 1) * cb],
                    tail_sem.at[t, part, q],
                )
                for q in range(2)
            ]

        def xn_in(i):
            return pltpu.make_async_copy(xn.at[hrows(4 + i)], act.at[1, :, 0:d], act_sem.at[1, 0])

        def h_at(i, q, col, width):
            return h.at[hrows(4 + i), q * fr + col : q * fr + col + width]

        def h_in(i):
            return [
                pltpu.make_async_copy(h_at(i, q, 0, t0), act.at[0, :, q * fr : q * fr + t0], act_sem.at[0, q])
                for q in range(2)
            ]

        def arrive(t):
            w1_yt(t).wait_recv()
            w1_ft(t).start()
            if t == 1:
                w1_y(N1 - 1).start()
                w1_e().wait_recv()
                w1_ye().start()
                w2_yf(0).start()
                w2_yf(1).start()
                w2_e().wait_recv()
            w1_ft(t).wait_recv()
            for c in w_tail(t, 1):
                c.start()
            if t == 1:
                w1_ce().start()
                w2_ce().start()
            for part in range(2):
                for c in w_tail(t, part):
                    c.wait()

        w1_c(NR - 1).wait_recv()
        for t in range(2):
            for c in w_tail(t, 0):
                c.start()
        xn_in(0).start()
        for c in h_in(0):
            c.start()
        w2_c(0).wait_recv()
        rem, zero = jnp.int32(REM), jnp.int32(0)
        w2_in(rem, zero, 1, True)
        arrive(0)
        w2_in(rem, zero, 1, False)

        def tile_(i, carry):
            xn_in(i).wait()
            u = jnp.dot(act[1, :, 0:d], wb[0, 0:d], preferred_element_type=F32)
            g = jax.nn.gelu(u, approximate=True).astype(BF16)
            for c in h_in(i):
                c.wait()
            first = []
            for q in range(2):
                at = q * fr + t0
                act[0, :, at : at + cb] = g[:, q * cb : (q + 1) * cb]
                first.append(pltpu.make_async_copy(act.at[0, :, at : at + cb], h_at(i, q, t0, cb), h_sem.at[0, q]))
                first[-1].start()
            n = fr - cb
            pout[0] = jnp.dot(act[0, :, 0:n], wb[1, 0:n], preferred_element_type=F32) + jnp.dot(
                act[0, :, fr : fr + n], wb[1, fr : fr + n], preferred_element_type=F32
            )
            for c in first:
                c.wait()

            @pl.when(i < 3)
            def _():
                for c in h_in(i + 1):
                    c.start()

            pl.when(i == 0)(lambda: arrive(1))
            u = jnp.dot(act[1, :, 0:d], wb[0, d : 2 * d], preferred_element_type=F32)
            hout[0, 0:sub] = jax.nn.gelu(u, approximate=True).astype(BF16)
            pl.when(i < 3)(lambda: xn_in(i + 1).start())
            second = []
            for q in range(2):
                second.append(
                    pltpu.make_async_copy(
                        hout.at[0, 0:sub, q * cb : (q + 1) * cb], h_at(i, q, t0 + cb, cb), h_sem.at[1, q]
                    )
                )
                second[-1].start()
            pout[0] += jnp.dot(hout[0, 0:sub, 0:cb], wb[1, n:fr], preferred_element_type=F32) + jnp.dot(
                hout[0, 0:sub, cb : 2 * cb], wb[1, fr + n : kr], preferred_element_type=F32
            )
            out = p_out(psend, zero, i, 0)
            out.start()
            out.wait()
            p_x(i, 0).start()
            for c in second:
                c.wait()
            return carry

        lax.fori_loop(0, 4, tile_, jnp.int32(0))

    @pl.loop(0, 2)
    def _(phase):
        early = phase == 0
        cut = starts1[BREAK1]
        first_product(_where(early, 0, cut), _where(early, cut, total1))
        pl.when(early)(junction)
        second_product(_where(early, 0, BREAK2), _where(early, BREAK2, len(VISITS)))

    @pl.loop(0, N1 + 1)
    def _(j):
        w1_cr(j).wait_send()

    @pl.loop(0, N1 + 1)
    def _(j):
        @pl.when(j != NR - 1)
        def _():
            w1_yr(j).wait_send()
            w1_f(j).wait_send()

    for t in range(2):
        w1_yt(t).wait_send()
        w1_ft(t).wait_send()

    @pl.loop(0, N2)
    def _(k):
        w2_yf(k).wait_send()
        w2_c(k).wait_send()
        w2_ff(k).wait_send()

    w1_e().wait_send()
    w2_e().wait_send()
    w2_ce().wait_send()
    for g in range(2):
        for c in w2_yg(g):
            c.wait_send()
        w2_fg(g).wait_send()

    @pl.loop(0, NX)
    def _(t):
        xn_x(t).wait_send()

    @pl.loop(0, 2 * N2 * 4)
    def _(s):
        p_x(s % 4, s // 4).wait_send()


PUTS = 16


def _put(src, dst, buf, sems_in, sems_out):
    n = src.shape[0] // PUTS

    def get(i):
        return pltpu.make_async_copy(src.at[i * n : (i + 1) * n], buf.at[i], sems_in.at[i])

    def put(i):
        return pltpu.make_async_copy(buf.at[i], dst.at[i * n : (i + 1) * n], sems_out.at[i])

    for i in range(PUTS):
        get(i).start()
    for i in range(PUTS):
        get(i).wait()
        put(i).start()
    for i in range(PUTS):
        put(i).wait()


def solution(mesh):
    def body(x, gamma, w1, w2):
        rows, d = x.shape
        half, fq = w1.shape
        sub = rows // 4
        c1, c2 = fq // N1, half // N2

        def hbm(*shape, dtype=BF16):
            return jax.ShapeDtypeStruct(shape, dtype)

        dma = pltpu.SemaphoreType.DMA
        outs = (
            hbm(rows, d),
            hbm(2 * rows, d),
            hbm(half, c1), hbm(half, fq + c1), hbm(half, fq + c1), hbm(half, fq + c1),
            hbm(c1, half), hbm(fq + c1, half), hbm(fq + c1, half), hbm(fq + c1, half),
            hbm(2 * rows, 2 * (fq + c1)),
            hbm(rows, d, dtype=F32), hbm(rows, d, dtype=F32), hbm(rows, d, dtype=F32),
        )
        out = pl.pallas_call(
            _kernel,
            name="mlp",
            out_shape=outs,
            in_specs=[pl.BlockSpec(memory_space=pl.ANY)] * 4,
            out_specs=tuple([pl.BlockSpec(memory_space=pl.ANY)] * len(outs)),
            scratch_shapes=[
                pltpu.VMEM((2, sub, 2 * d), BF16),
                pltpu.VMEM((2, 2 * fq, c2), BF16),
                pltpu.VMEM((2, 2 * sub, c1), BF16),
                pltpu.VMEM((2, sub, c2), F32),
                pltpu.VMEM((sub, c2), F32),
                pltpu.VMEM((2, sub, c2), F32),
                pltpu.VMEM((2, sub, c2), BF16),
                pltpu.VMEM((2, sub, c2), BF16),
                pltpu.VMEM((1, d), F32),
                dma((2, 2)), dma((2, 4)), dma((2, 2)), dma((3,)), dma((4,)), dma((2, 2)), dma((2, 2, 2)),
                dma((NX,)), dma((NX,)), dma((2,)), dma((2,)),
                dma((N1 + 2,)), dma((N1 + 2,)), dma((N1 + 1,)), dma((N1 + 1,)), dma((N1 + 2,)), dma((N1 + 2,)),
                dma((N2 + 4,)), dma((N2 + 4,)), dma((N2 + 1,)), dma((N2 + 1,)), dma((N2 + 2,)), dma((N2 + 2,)),
                dma((8 * N2,)), dma((8 * N2,)),
            ],
            compiler_params=pltpu.CompilerParams(
                collective_id=0, has_side_effects=True, vmem_limit_bytes=67_000_000
            ),
        )(x, gamma.reshape(1, d), w1, w2)
        return pl.pallas_call(
            _put,
            name="put",
            out_shape=hbm(rows, d),
            in_specs=[pl.BlockSpec(memory_space=pl.ANY)],
            out_specs=pl.BlockSpec(memory_space=pl.ANY),
            scratch_shapes=[pltpu.VMEM((PUTS, rows // PUTS, d), BF16), dma((PUTS,)), dma((PUTS,))],
            compiler_params=pltpu.CompilerParams(vmem_limit_bytes=40_000_000),
        )(out[0])

    return jax.shard_map(
        body,
        mesh=mesh,
        in_specs=(P(("fsdp", "tp"), None), P(None), P("fsdp", "tp"), P("tp", "fsdp")),
        out_specs=P(("fsdp", "tp"), None),
        check_vma=False,
    )
```

```python
import jax
import jax.numpy as jnp
from jax import lax
from jax.experimental import pallas as pl
from jax.experimental.pallas import tpu as pltpu
from jax.sharding import PartitionSpec as P

EPS = 1e-6
F32 = jnp.float32
BF16 = jnp.bfloat16
MESH = pl.DeviceIdType.MESH

N1 = 12
NR = N1 - 1
N2 = 6
NX = 8
AHEAD = 3

STEPS1 = (
    ((0, 4), (0, 2)),
    ((0, 4), (2, 1)),
    ((4, 2), (0, 3)),
    ((0, 3), (4, 1)),
    ((6, 1), (0, 3)),
    ((3, 4), (4, 1)),
    ((7, 1), (2, 1)),
    ((7, 1), (4, 1)),
    ((0, 8), (5, 1)),
    ((8, 2), (2, 2)),
    ((7, 6), (0, 2)),
)
BREAK1 = 10

REM, OWN, END = 0, 1, 2
LAST = 2 * N2 - 1
R, A, B = ((lambda k, t=t: (t, k)) for t in (REM, OWN, END))
VISITS = (
    R(1), R(2), R(3), R(4),
    R(5), A(0), A(1), R(6), A(2), B(0), B(1), A(3), R(7), B(2), A(4), A(5), R(8), B(3), A(6), A(7), B(4), B(5),
    R(9), A(8), B(6), A(9), B(7), R(10), B(8), A(10), R(11), A(11), B(9), B(10), B(11),
)
BREAK2 = 4
PASS_F = {A(1): 0, B(1): 1, A(5): 2, B(5): 3, B(7): 4, R(11): 5}
PASS_G = {B(4): 0, A(11): 1}
SEND_F = {R(2): (2,), R(5): (3, 4), R(7): (5,)}
SEND_G = {R(2): 0, R(7): 1}


def _tail(c1):
    return ((0, c1 // 2), (c1 // 2, c1 // 2))


def _where(cond, a, b):
    return jnp.where(cond, jnp.int32(a), jnp.int32(b))


def _bounds1():
    at, out = 0, []
    for (_, nj), (_, nt) in STEPS1:
        out.append(at)
        at += nj * 2 * nt
    return out, at


def _step1(s):
    starts, _ = _bounds1()
    rows = [(at, j0, nt, t0) for at, ((j0, _), (t0, nt)) in zip(starts, STEPS1)]
    start, j0, nt, t0 = (jnp.int32(v) for v in rows[0])
    for row in rows[1:]:
        late = s >= row[0]
        start, j0, nt, t0 = (_where(late, new, old) for new, old in zip(row, (start, j0, nt, t0)))
    u = s - start
    pair = u // nt
    return j0 + pair // 2, pair % 2, t0 + u % nt


def _first_tile(j):
    return _where(j < 7, 0, _where(j < NR - 1, 2, _where(j == NR - 1, 9, 0)))


def _visit(v):
    code = jnp.int32(0)
    for n, (t, k) in enumerate(VISITS):
        code = _where(v == n, t * 16 + k, code)
    return code // 16, code % 16


def _kernel(
    x, gamma, w1, w2,
    y, xn, w1e, w1far, w1so, w1sf, w2e, w2far, w2so, w2sf, h, psend, pown, precv,
    act, wb, hout, pout, pin, pback, xin, yout, gam,
    act_sem, w_sem, h_sem, io_sem, out_sem, in_sem, tail_sem,
    xn_s, xn_r, e_s, e_r, w1y_s, w1y_r, w1c_s, w1c_r, w1f_s, w1f_r,
    w2y_s, w2y_r, w2c_s, w2c_r, w2f_s, w2f_r, p_s, p_r,
):
    a = lax.axis_index("fsdp")
    b = lax.axis_index("tp")
    to_y = {"fsdp": 1 - a}
    to_x = {"tp": lax.rem(b + 2, 4)}
    to_c = {"tp": b + 1 - 2 * lax.rem(b, 2)}
    rows, d = x.shape
    half, fq = w1.shape
    sub = rows // 4
    c1 = fq // N1
    c2 = half // N2
    tail = _tail(c1)
    fr = NR * c1
    t0 = fr - c1
    kr = 2 * fr
    ke = 4 * c1
    wide = half // 2
    piece = rows // NX
    near = pl.multiple_of(a * half, half)
    away = pl.multiple_of((1 - a) * half, half)
    everything = slice(None)

    def remote(src, dst, ssem, rsem, to):
        return pltpu.make_async_remote_copy(
            src_ref=src, dst_ref=dst, send_sem=ssem, recv_sem=rsem, device_id=to, device_id_type=MESH
        )

    def cols1(j):
        return (everything, pl.ds(pl.multiple_of(j * c1, c1), c1))

    def cols2(k):
        return pl.ds(pl.multiple_of(k * c2, c2), c2)

    def w1_y(j):
        return remote(w1.at[cols1(j)], w1far.at[cols1(j)], w1y_s.at[j], w1y_r.at[j], to_y)

    def w1_ye():
        return remote(w1e, w1far.at[cols1(N1)], w1y_s.at[N1], w1y_r.at[N1], to_y)

    def w1_yr(j):
        return remote(w1far.at[cols1(j)], w1far.at[cols1(j)], w1y_s.at[j], w1y_r.at[j], to_y)

    def w1_c(j):
        return remote(w1.at[cols1(j)], w1so.at[cols1(j)], w1c_s.at[j], w1c_r.at[j], to_c)

    def w1_ce():
        return remote(w1e, w1so.at[cols1(N1)], w1c_s.at[N1], w1c_r.at[N1], to_c)

    def w1_cr(j):
        return remote(w1so.at[cols1(j)], w1so.at[cols1(j)], w1c_s.at[j], w1c_r.at[j], to_c)

    def w1_f(j):
        return remote(w1far.at[cols1(j)], w1sf.at[cols1(j)], w1f_s.at[j], w1f_r.at[j], to_c)

    def cols_t(t):
        return (everything, pl.ds(t0 + tail[t][0], tail[t][1]))

    def tail_at(t):
        return NR - 1 if t == 0 else N1 + t

    def w1_yt(t):
        return remote(w1.at[cols_t(t)], w1far.at[cols_t(t)], w1y_s.at[tail_at(t)], w1y_r.at[tail_at(t)], to_y)

    def w1_ft(t):
        return remote(w1far.at[cols_t(t)], w1sf.at[cols_t(t)], w1f_s.at[tail_at(t)], w1f_r.at[tail_at(t)], to_c)

    def w1_e():
        return remote(w1.at[cols1(N1 - 1)], w1e, e_s.at[0], e_r.at[0], to_x)

    def w2_e():
        return remote(w2.at[fr:fq], w2e, e_s.at[1], e_r.at[1], to_x)

    def w2_yf(k):
        at = (pl.ds(0, fr), cols2(k))
        return remote(w2.at[at], w2far.at[at], w2y_s.at[k], w2y_r.at[k], to_y)

    def w2_yg(g):
        at = (pl.ds(fr, c1), pl.ds(g * wide, wide))
        to = (pl.ds(fq, c1), pl.ds(g * wide, wide))
        return (
            remote(w2.at[at], w2far.at[at], w2y_s.at[N2 + 2 * g], w2y_r.at[N2 + 2 * g], to_y),
            remote(
                w2e.at[:, pl.ds(g * wide, wide)], w2far.at[to], w2y_s.at[N2 + 2 * g + 1], w2y_r.at[N2 + 2 * g + 1], to_y
            ),
        )

    def w2_c(k):
        at = (everything, cols2(k))
        return remote(w2.at[at], w2so.at[pl.ds(0, fq), cols2(k)], w2c_s.at[k], w2c_r.at[k], to_c)

    def w2_ce():
        return remote(w2e, w2so.at[fq : fq + c1], w2c_s.at[N2], w2c_r.at[N2], to_c)

    def w2_ff(k):
        at = (pl.ds(0, fr), cols2(k))
        return remote(w2far.at[at], w2sf.at[at], w2f_s.at[k], w2f_r.at[k], to_c)

    def w2_fg(g):
        at = (pl.ds(fr, 2 * c1), pl.ds(g * wide, wide))
        return remote(w2far.at[at], w2sf.at[at], w2f_s.at[N2 + g], w2f_r.at[N2 + g], to_c)

    def xrows(t):
        return pl.ds(pl.multiple_of(t * piece, piece), piece)

    def xn_x(t):
        return remote(xn.at[xrows(t)], xn.at[xrows(t + NX)], xn_s.at[t], xn_r.at[t], to_x)

    def p_x(i, k):
        at = (pl.ds(pl.multiple_of(i * sub, sub), sub), cols2(k))
        return remote(psend.at[at], precv.at[at], p_s.at[k * 4 + i], p_r.at[k * 4 + i], to_x)

    barrier = pltpu.get_barrier_semaphore()
    for to in (to_y, to_x, to_c):
        pl.semaphore_signal(barrier, inc=1, device_id=to, device_id_type=MESH)
    pl.semaphore_wait(barrier, 3)

    for j in range(AHEAD):
        w1_y(j).start()

    @pl.loop(0, N1)
    def _(j):
        w1_c(j).start()

    def gam_in():
        return [
            pltpu.make_async_copy(gamma.at[:, pl.ds(off, half)], gam.at[:, i * half : (i + 1) * half], io_sem.at[i])
            for i, off in enumerate((near, away))
        ]

    def x_in(t, slot):
        return [
            pltpu.make_async_copy(
                x.at[xrows(t), pl.ds(off, half)],
                act.at[slot, 0:piece, i * half : (i + 1) * half],
                act_sem.at[slot, i],
            )
            for i, off in enumerate((near, away))
        ]

    for c in gam_in():
        c.start()
    for c in x_in(0, 0):
        c.start()
    for c in gam_in():
        c.wait()

    @pl.loop(0, NX)
    def _(t):
        slot = t % 2

        @pl.when(t + 1 < NX)
        def _():
            for c in x_in(t + 1, 1 - slot):
                c.start()

        for c in x_in(t, slot):
            c.wait()

        @pl.loop(0, piece // 16)
        def _(r):
            at = pl.multiple_of(r * 16, 16)
            xs = act[slot, pl.ds(at, 16), 0:d].astype(F32)
            xc = xs - jnp.mean(xs, axis=1, keepdims=True)
            var = jnp.mean(xc * xc, axis=1, keepdims=True)
            act[slot, pl.ds(piece + at, 16), 0:d] = (xc * lax.rsqrt(var + EPS) * gam[...]).astype(BF16)

        out = pltpu.make_async_copy(act.at[slot, piece : 2 * piece, 0:d], xn.at[xrows(t)], io_sem.at[2])
        out.start()
        out.wait()

        @pl.when(t < NX // 2)
        def _():
            xn_x(t).start()

    def hcol(j, q):
        return pl.multiple_of(_where(j < NR, q * fr + j * c1, kr + (j - NR) * 2 * c1 + q * c1), c1)

    def tile_rows(m):
        return _where(m < 4, 2 * m, 2 + m), m < 4

    def hrows(r):
        return pl.ds(pl.multiple_of(r * sub, sub), sub)

    def a1_in(m, slot, go):
        r0, two = tile_rows(m)

        def one(i):
            c = pltpu.make_async_copy(
                xn.at[hrows(r0 + i)], act.at[slot, :, i * d : (i + 1) * d], act_sem.at[slot, i]
            )
            c.start() if go else c.wait()

        one(0)
        pl.when(two)(lambda: one(1))

    def w1_in(j, q, slot, go):
        def load(i, ref, at):
            c = pltpu.make_async_copy(ref.at[at], wb.at[slot, i * half : (i + 1) * half], w_sem.at[slot, i])
            c.start() if go else c.wait()

        if not go:
            for i in range(2):
                load(i, w1far, cols1(j))
            return
        pl.when((q == 0) & (j < N1))(lambda: load(0, w1, cols1(j)))
        pl.when((q == 0) & (j == N1))(lambda: load(0, w1e, (everything, everything)))
        pl.when(q == 0)(lambda: load(1, w1far, cols1(j)))

        @pl.when(q == 1)
        def _():
            load(0, w1so, cols1(j))
            load(1, w1sf, cols1(j))

    starts1, total1 = _bounds1()
    first2, first3, first4 = (
        next(at for at, (_, (m0, nm)) in zip(starts1, STEPS1) if m0 == m) for m in (2, 4, 5)
    )

    def arrive1(s):
        j, q, m = _step1(s)
        first = m == _first_tile(j)

        @pl.when(first & (q == 0))
        def _():
            w1_yr(j).wait_recv()
            w1_f(j).start()

            @pl.when(j + AHEAD < NR - 1)
            def _():
                w1_y(j + AHEAD).start()

            @pl.when(j + AHEAD == NR - 1)
            def _():
                for t in range(len(tail)):
                    w1_yt(t).start()
                w1_e().start()
                w2_e().start()

            @pl.when(j == 2)
            def _():
                for t in range(NX // 2, NX):
                    xn_x(t).start()

            @pl.when(j == 4)
            def _():
                for k in range(N2):
                    w2_c(k).start()

        @pl.when(first & (q == 1))
        def _():
            w1_cr(j).wait_recv()
            w1_f(j).wait_recv()

        for at, lo, hi in ((first2, 0, 4), (first3, 4, 6), (first4, 6, 8)):

            @pl.when(s == at)
            def _():
                for t in range(lo, hi):
                    xn_x(t).wait_recv()

    def load1(s, aslot, wslot, a_new, w_new):
        j, q, m = _step1(s)
        pl.when(a_new)(lambda: a1_in(m, aslot, True))
        pl.when(w_new)(lambda: w1_in(j, q, wslot, True))

    def h_out(s, i):
        j, q, m = _step1(s)
        r0, _ = tile_rows(m)
        return pltpu.make_async_copy(
            hout.at[s % 2, pl.ds(pl.multiple_of(i * sub, sub), sub)],
            h.at[hrows(r0 + i), pl.ds(hcol(j, q), c1)],
            h_sem.at[s % 2, i],
        )

    def h_done(s):
        _, two = tile_rows(_step1(s)[2])
        h_out(s, 0).wait()
        pl.when(two)(lambda: h_out(s, 1).wait())

    def first_product(lo, hi):
        arrive1(lo)
        load1(lo, 0, 0, True, True)

        def step(s, carry):
            aslot, wslot, a_fresh, w_fresh = carry
            j, q, m = _step1(s)
            nj, nq, nm = _step1(s + 1)
            more = s + 1 < hi
            a_new = more & (nm != m)
            w_new = more & ((nj != j) | (nq != q))
            na = _where(a_new, 1 - aslot, aslot)
            nw = _where(w_new, 1 - wslot, wslot)
            pl.when(more)(lambda: arrive1(s + 1))
            load1(s + 1, na, nw, a_new, w_new)
            pl.when(a_fresh == 1)(lambda: a1_in(m, aslot, False))
            pl.when(w_fresh == 1)(lambda: w1_in(j, q, wslot, False))
            pl.when(s >= lo + 2)(lambda: h_done(s - 2))
            _, two = tile_rows(m)

            @pl.loop(0, _where(two, 2, 1))
            def _(i):
                u = jnp.dot(
                    act[aslot, :, pl.ds(pl.multiple_of(i * d, d), d)], wb[wslot, 0:d], preferred_element_type=F32
                )
                hout[s % 2, pl.ds(pl.multiple_of(i * sub, sub), sub)] = jax.nn.gelu(u, approximate=True).astype(BF16)
                h_out(s, i).start()

            return na, nw, _where(a_new, 1, 0), _where(w_new, 1, 0)

        one, nil = jnp.int32(1), jnp.int32(0)
        lax.fori_loop(lo, hi, step, (nil, nil, one, one))
        h_done(hi - 2)
        h_done(hi - 1)

    def p_in(i, k, slot):
        return pltpu.make_async_copy(precv.at[hrows(i), cols2(k)], pin.at[slot], in_sem.at[slot, 2])

    def a2_in(typ, k, i, slot, go):
        r = _where(typ == REM, 4, 0) + i

        def wait_or_start(c):
            c.start() if go else c.wait()

        @pl.when(typ != END)
        def _():
            wait_or_start(pltpu.make_async_copy(h.at[hrows(r), 0:kr], act.at[slot, :, 0:kr], act_sem.at[slot, 0]))

        @pl.when(typ == END)
        def _():
            wait_or_start(
                pltpu.make_async_copy(h.at[hrows(r), kr : kr + ke], act.at[slot, :, 0:ke], act_sem.at[slot, 0])
            )
            ycol = pl.multiple_of(_where(k < N2, near, away) + (k % N2) * c2, c2)
            wait_or_start(pltpu.make_async_copy(pown.at[hrows(i), cols2(k)], pback.at[slot], in_sem.at[slot, 0]))
            wait_or_start(pltpu.make_async_copy(x.at[hrows(i), pl.ds(ycol, c2)], xin.at[slot], in_sem.at[slot, 1]))
            if go:

                @pl.when(k < LAST)
                def _():
                    p_x(i, k).wait_recv()
                    p_in(i, k, slot).start()

    def w2_in(typ, k, slot, go):
        def load(n, at, rows_, ref, from_, kk):
            c = pltpu.make_async_copy(
                ref.at[pl.ds(from_, rows_), cols2(kk)], wb.at[slot, at : at + rows_], w_sem.at[slot, n]
            )
            c.start() if go else c.wait()

        def main(own, sib, kk):
            load(0, 0, fr, own, 0, kk)
            load(1, fr, fr, sib, 0, kk)

        def rest(own, ext, ext_at, sib, kk):
            load(0, 0, c1, own, fr, kk)
            load(1, c1, c1, sib, fr, kk)
            load(2, 2 * c1, c1, ext, ext_at, kk)
            load(3, 3 * c1, c1, sib, fq, kk)

        def both(side, kk, own, ext, ext_at, sib):
            pl.when(side & (typ != END))(lambda: main(own, sib, kk))
            pl.when(side & (typ == END))(lambda: rest(own, ext, ext_at, sib, kk))

        if not go:
            pl.when(typ != END)(lambda: main(w2far, w2sf, 0))
            pl.when(typ == END)(lambda: rest(w2far, w2far, fq, w2sf, 0))
            return
        both(k < N2, k, w2, w2e, 0, w2so)
        both(k >= N2, k - N2, w2far, w2far, fq, w2sf)

    def arrive2(v):
        at = {visit: n for n, visit in enumerate(VISITS)}
        for n in range(len(VISITS)):
            visit = VISITS[n]
            todo = []
            for u in SEND_F.get(visit, ()):
                todo.append(lambda u=u: w2_yf(u).start())
            if visit in SEND_G:
                todo.append(lambda g=SEND_G[visit]: [c.start() for c in w2_yg(g)])
            if visit in PASS_F:
                u = PASS_F[visit]
                todo.append(lambda u=u: (w2_yf(u).wait_recv(), w2_ff(u).start()))
            if visit in PASS_G:
                g = PASS_G[visit]
                todo.append(lambda g=g: ([c.wait_recv() for c in w2_yg(g)], w2_fg(g).start()))
            if visit[0] == REM:
                k = visit[1]
                todo.append(lambda k=k: w2_c(k).wait_recv() if k < N2 else w2_ff(k - N2).wait_recv())
            if n == min(at[B(k)] for k in range(N2)):
                todo.append(lambda: w2_ce().wait_recv())
            for g in range(2):
                if n == min(at[B(N2 + 3 * g + k)] for k in range(3)):
                    todo.append(lambda g=g: w2_fg(g).wait_recv())
            if todo:

                @pl.when(v == n)
                def _(todo=todo):
                    for f in todo:
                        f()

    def p_out(to, k, i, slot):
        return pltpu.make_async_copy(pout.at[slot], to.at[hrows(i), cols2(k)], out_sem.at[slot])

    def y_out(k, i):
        ycol = pl.multiple_of(_where(k < N2, near, away) + (k % N2) * c2, c2)
        return pltpu.make_async_copy(yout, y.at[hrows(i), pl.ds(ycol, c2)], out_sem.at[2])

    def finish(typ, k, i, slot):
        @pl.when((typ == REM) | (typ == OWN))
        def _():
            p_out(pown, k, i, slot).wait()

        @pl.when(typ == REM)
        def _():
            p_x(i, k).start()

        @pl.when(typ == END)
        def _():
            y_out(k, i).wait()

    def second_product(lo, hi):
        arrive2(lo)
        typ0, k0 = _visit(lo)
        w2_in(typ0, k0, 0, True)
        a2_in(typ0, k0, jnp.int32(0), 0, True)

        def visit(v, carry):
            typ, k, ptyp, pk = carry
            more = v + 1 < hi
            ntyp, nk = _visit(v + 1)
            wslot = (v - lo) % 2

            def tile(i, before):
                btyp, bk, bi = before
                slot = i % 2
                last = i == 3

                @pl.when(last & more)
                def _():
                    arrive2(v + 1)
                    w2_in(ntyp, nk, 1 - wslot, True)

                @pl.when(more | (i < 3))
                def _():
                    a2_in(_where(last, ntyp, typ), _where(last, nk, k), _where(last, 0, i + 1), 1 - slot, True)

                a2_in(typ, k, i, slot, False)
                pl.when(i == 0)(lambda: w2_in(typ, k, wslot, False))

                @pl.when(typ != END)
                def _():
                    pout[slot] = jnp.dot(act[slot, :, 0:kr], wb[wslot, 0:kr], preferred_element_type=F32)

                @pl.when(typ == END)
                def _():
                    pout[slot] = jnp.dot(act[slot, :, 0:ke], wb[wslot, 0:ke], preferred_element_type=F32)

                finish(btyp, bk, bi, 1 - slot)
                pl.when(typ == OWN)(lambda: p_out(pown, k, i, slot).start())
                pl.when(typ == REM)(lambda: p_out(psend, k, i, slot).start())

                @pl.when(typ == END)
                def _():
                    @pl.when(k == LAST)
                    def _():
                        p_x(i, k).wait_recv()
                        p_in(i, k, slot).start()

                    p_in(i, k, slot).wait()
                    total = (pback[slot] + pout[slot]) + pin[slot]
                    yout[...] = (xin[slot].astype(F32) + total).astype(BF16)
                    y_out(k, i).start()

                return typ, k, i

            ptyp, pk, _ = lax.fori_loop(0, 4, tile, (ptyp, pk, jnp.int32(3)))
            return ntyp, nk, ptyp, pk

        _, _, ptyp, pk = lax.fori_loop(lo, hi, visit, (typ0, k0, jnp.int32(3), jnp.int32(0)))
        finish(ptyp, pk, jnp.int32(3), 1)

    def junction():
        final = len(tail) - 1

        def lanes(t):
            at = 0 if t < 2 else 2 * sum(w for _, w in tail[1:t])
            return (0 if t == 0 else d), at

        def w_tail(t, part):
            refs = ((w1, w1so), (w1far, w1sf))[part]
            r, at = lanes(t)
            w = tail[t][1]
            return [
                pltpu.make_async_copy(
                    refs[q].at[cols_t(t)],
                    wb.at[0, r + part * half : r + (part + 1) * half, at + q * w : at + (q + 1) * w],
                    tail_sem.at[t, part, q],
                )
                for q in range(2)
            ]

        def xn_in(i):
            return pltpu.make_async_copy(xn.at[hrows(4 + i)], act.at[1, :, 0:d], act_sem.at[1, 0])

        def h_at(i, q, col, width):
            return h.at[hrows(4 + i), q * fr + col : q * fr + col + width]

        def h_in(i):
            return [
                pltpu.make_async_copy(h_at(i, q, 0, t0), act.at[0, :, q * fr : q * fr + t0], act_sem.at[0, q])
                for q in range(2)
            ]

        def hidden(t):
            r, at = lanes(t)
            u = jnp.dot(act[1, :, 0:d], wb[0, r : r + d, at : at + 2 * tail[t][1]], preferred_element_type=F32)
            return jax.nn.gelu(u, approximate=True).astype(BF16)

        def arrive(t):
            w1_yt(t).wait_recv()
            w1_ft(t).start()
            if t == final:
                w1_y(N1 - 1).start()
                w1_e().wait_recv()
                w1_ye().start()
                w2_yf(0).start()
                w2_yf(1).start()
                w2_e().wait_recv()
            w1_ft(t).wait_recv()
            for c in w_tail(t, 1):
                c.start()
            if t == final:
                w1_ce().start()
                w2_ce().start()
            for part in range(2):
                for c in w_tail(t, part):
                    c.wait()

        w1_c(NR - 1).wait_recv()
        for t in range(len(tail)):
            for c in w_tail(t, 0):
                c.start()
        xn_in(0).start()
        for c in h_in(0):
            c.start()
        w2_c(0).wait_recv()
        rem, zero = jnp.int32(REM), jnp.int32(0)
        w2_in(rem, zero, 1, True)
        arrive(0)
        w2_in(rem, zero, 1, False)

        def tile_(i, carry):
            xn_in(i).wait()
            out = []
            for t in range(final):
                if t > 0:
                    pl.when(i == 0)(lambda t=t: arrive(t))
                g = hidden(t)
                if t == 0:
                    for c in h_in(i):
                        c.wait()
                off, w = tail[t]
                for q in range(2):
                    at = q * fr + t0 + off
                    act[0, :, at : at + w] = g[:, q * w : (q + 1) * w]
                    out.append(
                        pltpu.make_async_copy(act.at[0, :, at : at + w], h_at(i, q, t0 + off, w), h_sem.at[t, q])
                    )
                    out[-1].start()
            off, w = tail[final]
            n = fr - w
            pout[0] = jnp.dot(act[0, :, 0:n], wb[1, 0:n], preferred_element_type=F32) + jnp.dot(
                act[0, :, fr : fr + n], wb[1, fr : fr + n], preferred_element_type=F32
            )
            for c in out:
                c.wait()

            @pl.when(i < 3)
            def _():
                for c in h_in(i + 1):
                    c.start()

            pl.when(i == 0)(lambda: arrive(final))
            hout[0, 0:sub, 0 : 2 * w] = hidden(final)
            pl.when(i < 3)(lambda: xn_in(i + 1).start())
            out = []
            for q in range(2):
                out.append(
                    pltpu.make_async_copy(
                        hout.at[0, 0:sub, q * w : (q + 1) * w], h_at(i, q, t0 + off, w), h_sem.at[2, q]
                    )
                )
                out[-1].start()
            pout[0] += jnp.dot(hout[0, 0:sub, 0:w], wb[1, n:fr], preferred_element_type=F32) + jnp.dot(
                hout[0, 0:sub, w : 2 * w], wb[1, fr + n : kr], preferred_element_type=F32
            )
            sent = p_out(psend, zero, i, 0)
            sent.start()
            sent.wait()
            p_x(i, 0).start()
            for c in out:
                c.wait()
            return carry

        lax.fori_loop(0, 4, tile_, jnp.int32(0))

    @pl.loop(0, 2)
    def _(phase):
        early = phase == 0
        cut = starts1[BREAK1]
        first_product(_where(early, 0, cut), _where(early, cut, total1))
        pl.when(early)(junction)
        second_product(_where(early, 0, BREAK2), _where(early, BREAK2, len(VISITS)))

    @pl.loop(0, N1 + 1)
    def _(j):
        w1_cr(j).wait_send()

    @pl.loop(0, N1 + 1)
    def _(j):
        @pl.when(j != NR - 1)
        def _():
            w1_yr(j).wait_send()
            w1_f(j).wait_send()

    for t in range(len(tail)):
        w1_yt(t).wait_send()
        w1_ft(t).wait_send()

    @pl.loop(0, N2)
    def _(k):
        w2_yf(k).wait_send()
        w2_c(k).wait_send()
        w2_ff(k).wait_send()

    w1_e().wait_send()
    w2_e().wait_send()
    w2_ce().wait_send()
    for g in range(2):
        for c in w2_yg(g):
            c.wait_send()
        w2_fg(g).wait_send()

    @pl.loop(0, NX)
    def _(t):
        xn_x(t).wait_send()

    @pl.loop(0, 2 * N2 * 4)
    def _(s):
        p_x(s % 4, s // 4).wait_send()


PUTS = 16


def _put(src, dst, buf, sems_in, sems_out):
    n = src.shape[0] // PUTS

    def get(i):
        return pltpu.make_async_copy(src.at[i * n : (i + 1) * n], buf.at[i], sems_in.at[i])

    def put(i):
        return pltpu.make_async_copy(buf.at[i], dst.at[i * n : (i + 1) * n], sems_out.at[i])

    for i in range(PUTS):
        get(i).start()
    for i in range(PUTS):
        get(i).wait()
        put(i).start()
    for i in range(PUTS):
        put(i).wait()


def solution(mesh):
    def body(x, gamma, w1, w2):
        rows, d = x.shape
        half, fq = w1.shape
        sub = rows // 4
        c1, c2 = fq // N1, half // N2

        def hbm(*shape, dtype=BF16):
            return jax.ShapeDtypeStruct(shape, dtype)

        dma = pltpu.SemaphoreType.DMA
        outs = (
            hbm(rows, d),
            hbm(2 * rows, d),
            hbm(half, c1), hbm(half, fq + c1), hbm(half, fq + c1), hbm(half, fq + c1),
            hbm(c1, half), hbm(fq + c1, half), hbm(fq + c1, half), hbm(fq + c1, half),
            hbm(2 * rows, 2 * (fq + c1)),
            hbm(rows, d, dtype=F32), hbm(rows, d, dtype=F32), hbm(rows, d, dtype=F32),
        )
        out = pl.pallas_call(
            _kernel,
            name="mlp",
            out_shape=outs,
            in_specs=[pl.BlockSpec(memory_space=pl.ANY)] * 4,
            out_specs=tuple([pl.BlockSpec(memory_space=pl.ANY)] * len(outs)),
            scratch_shapes=[
                pltpu.VMEM((2, sub, 2 * d), BF16),
                pltpu.VMEM((2, 2 * fq, c2), BF16),
                pltpu.VMEM((2, 2 * sub, c1), BF16),
                pltpu.VMEM((2, sub, c2), F32),
                pltpu.VMEM((2, sub, c2), F32),
                pltpu.VMEM((2, sub, c2), F32),
                pltpu.VMEM((2, sub, c2), BF16),
                pltpu.VMEM((sub, c2), BF16),
                pltpu.VMEM((1, d), F32),
                dma((2, 2)), dma((2, 4)), dma((3, 2)), dma((3,)), dma((3,)), dma((2, 3)), dma((3, 2, 2)),
                dma((NX,)), dma((NX,)), dma((2,)), dma((2,)),
                dma((N1 + 3,)), dma((N1 + 3,)), dma((N1 + 1,)), dma((N1 + 1,)), dma((N1 + 3,)), dma((N1 + 3,)),
                dma((N2 + 4,)), dma((N2 + 4,)), dma((N2 + 1,)), dma((N2 + 1,)), dma((N2 + 2,)), dma((N2 + 2,)),
                dma((8 * N2,)), dma((8 * N2,)),
            ],
            compiler_params=pltpu.CompilerParams(
                collective_id=0, has_side_effects=True, vmem_limit_bytes=67_000_000
            ),
        )(x, gamma.reshape(1, d), w1, w2)
        return pl.pallas_call(
            _put,
            name="put",
            out_shape=hbm(rows, d),
            in_specs=[pl.BlockSpec(memory_space=pl.ANY)],
            out_specs=pl.BlockSpec(memory_space=pl.ANY),
            scratch_shapes=[pltpu.VMEM((PUTS, rows // PUTS, d), BF16), dma((PUTS,)), dma((PUTS,))],
            compiler_params=pltpu.CompilerParams(vmem_limit_bytes=40_000_000),
        )(out[0])

    return jax.shard_map(
        body,
        mesh=mesh,
        in_specs=(P(("fsdp", "tp"), None), P(None), P("fsdp", "tp"), P("tp", "fsdp")),
        out_specs=P(("fsdp", "tp"), None),
        check_vma=False,
    )
```

```python
import jax
import jax.numpy as jnp
from jax import lax
from jax.experimental import pallas as pl
from jax.experimental.pallas import tpu as pltpu
from jax.sharding import PartitionSpec as P

EPS = 1e-6
F32 = jnp.float32
BF16 = jnp.bfloat16
MESH = pl.DeviceIdType.MESH

N1 = 12
NR = N1 - 1
N2 = 6
NX = 8
BOTH = range(2)
AHEAD = 3

STEPS1 = (
    ((0, 4), (0, 2)),
    ((0, 4), (2, 1)),
    ((4, 2), (0, 3)),
    ((0, 3), (4, 1)),
    ((6, 1), (0, 3)),
    ((3, 4), (4, 1)),
    ((7, 1), (2, 1)),
    ((7, 1), (4, 1)),
    ((0, 8), (5, 1)),
    ((8, 2), (2, 2)),
    ((7, 6), (0, 2)),
)
BREAK1 = 10

REM, OWN, END = 0, 1, 2
LAST = 2 * N2 - 1
R, A, B = ((lambda k, t=t: (t, k)) for t in (REM, OWN, END))
VISITS = (
    *map(R, range(1, 6)),
    A(0), A(1), R(6), A(2), B(0), B(1), A(3), R(7), B(2), A(4), A(5), R(8), B(3), A(6), A(7), B(4), B(5),
    R(9), A(8), B(6), A(9), B(7), R(10), B(8), A(10), R(11), A(11), B(9), B(10), B(11),
)
BREAK2 = 4
PASS_F = {A(1): 0, B(1): 1, A(5): 2, B(5): 3, B(7): 4, R(11): 5}
PASS_G = {B(4): 0, A(11): 1}
SEND_F = {R(2): (2,), R(5): (3, 4), R(7): (5,)}
SEND_G = {R(2): 0, R(7): 1}


def _tail(c1):
    w = c1 // 2
    return ((0, w), (w, w))


def _where(cond, a, b):
    return jnp.where(cond, jnp.int32(a), jnp.int32(b))


def _bounds1():
    at, out = 0, []
    for (_, nj), (_, nt) in STEPS1:
        out.append(at)
        at += nj * 2 * nt
    return out, at


def _step1(s):
    starts, _ = _bounds1()
    rows = [(at, j0, nt, t0) for at, ((j0, _), (t0, nt)) in zip(starts, STEPS1)]
    start, j0, nt, t0 = (jnp.int32(v) for v in rows[0])
    for row in rows[1:]:
        late = s >= row[0]
        start, j0, nt, t0 = (_where(late, new, old) for new, old in zip(row, (start, j0, nt, t0)))
    u = s - start
    pair = u // nt
    return j0 + pair // 2, pair % 2, t0 + u % nt


def _first_tile(j):
    return _where(j < 7, 0, _where(j < NR - 1, 2, _where(j == NR - 1, 9, 0)))


def _visit(v):
    code = jnp.int32(0)
    for n, (t, k) in enumerate(VISITS):
        code = _where(v == n, t * 16 + k, code)
    return code // 16, code % 16


def _kernel(
    x, gamma, w1, w2,
    y, xlast, olast, xn, w1e, w1far, w1so, w1sf, w2e, w2far, w2so, w2sf, h, psend, pown, precv,
    act, wb, hout, pout, pin, pback, xin, yout, gam,
    act_sem, w_sem, h_sem, io_sem, out_sem, in_sem, tail_sem,
    xn_s, xn_r, e_s, e_r, w1y_s, w1y_r, w1c_s, w1c_r, w1f_s, w1f_r,
    w2y_s, w2y_r, w2c_s, w2c_r, w2f_s, w2f_r, p_s, p_r,
):
    a = lax.axis_index("fsdp")
    b = lax.axis_index("tp")
    to_y = {"fsdp": 1 - a}
    to_x = {"tp": lax.rem(b + 2, 4)}
    to_c = {"tp": b + 1 - 2 * lax.rem(b, 2)}
    rows, d = x.shape
    half, fq = w1.shape
    sub = rows // 4
    c1 = fq // N1
    c2 = half // N2
    tail = _tail(c1)
    fr = NR * c1
    t0 = fr - c1
    kr = 2 * fr
    ke = 4 * c1
    wide = half // 2
    piece = rows // NX
    near = pl.multiple_of(a * half, half)
    away = pl.multiple_of((1 - a) * half, half)
    everything = slice(None)

    def remote(src, dst, ssem, rsem, to):
        return pltpu.make_async_remote_copy(
            src_ref=src, dst_ref=dst, send_sem=ssem, recv_sem=rsem, device_id=to, device_id_type=MESH
        )

    def cols1(j):
        return (everything, pl.ds(pl.multiple_of(j * c1, c1), c1))

    def cols2(k):
        return pl.ds(pl.multiple_of(k * c2, c2), c2)

    def w1_y(j):
        return remote(w1.at[cols1(j)], w1far.at[cols1(j)], w1y_s.at[j], w1y_r.at[j], to_y)

    def w1_ye():
        return remote(w1e, w1far.at[cols1(N1)], w1y_s.at[N1], w1y_r.at[N1], to_y)

    def w1_yr(j):
        return remote(w1far.at[cols1(j)], w1far.at[cols1(j)], w1y_s.at[j], w1y_r.at[j], to_y)

    def w1_c(j):
        return remote(w1.at[cols1(j)], w1so.at[cols1(j)], w1c_s.at[j], w1c_r.at[j], to_c)

    def w1_ce():
        return remote(w1e, w1so.at[cols1(N1)], w1c_s.at[N1], w1c_r.at[N1], to_c)

    def w1_cr(j):
        return remote(w1so.at[cols1(j)], w1so.at[cols1(j)], w1c_s.at[j], w1c_r.at[j], to_c)

    def w1_f(j):
        return remote(w1far.at[cols1(j)], w1sf.at[cols1(j)], w1f_s.at[j], w1f_r.at[j], to_c)

    def cols_t(t):
        return (everything, pl.ds(t0 + tail[t][0], tail[t][1]))

    def tail_at(t):
        return NR - 1 if t == 0 else N1 + t

    def w1_yt(t):
        return remote(w1.at[cols_t(t)], w1far.at[cols_t(t)], w1y_s.at[tail_at(t)], w1y_r.at[tail_at(t)], to_y)

    def w1_ft(t):
        return remote(w1far.at[cols_t(t)], w1sf.at[cols_t(t)], w1f_s.at[tail_at(t)], w1f_r.at[tail_at(t)], to_c)

    def w1_e():
        return remote(w1.at[cols1(N1 - 1)], w1e, e_s.at[0], e_r.at[0], to_x)

    def w2_e():
        return remote(w2.at[fr:fq], w2e, e_s.at[1], e_r.at[1], to_x)

    def w2_yf(k):
        at = (pl.ds(0, fr), cols2(k))
        return remote(w2.at[at], w2far.at[at], w2y_s.at[k], w2y_r.at[k], to_y)

    def w2_yg(g):
        at = (pl.ds(fr, c1), pl.ds(g * wide, wide))
        to = (pl.ds(fq, c1), pl.ds(g * wide, wide))
        return (
            remote(w2.at[at], w2far.at[at], w2y_s.at[N2 + 2 * g], w2y_r.at[N2 + 2 * g], to_y),
            remote(
                w2e.at[:, pl.ds(g * wide, wide)], w2far.at[to], w2y_s.at[N2 + 2 * g + 1], w2y_r.at[N2 + 2 * g + 1], to_y
            ),
        )

    def w2_c(k):
        at = (everything, cols2(k))
        return remote(w2.at[at], w2so.at[pl.ds(0, fq), cols2(k)], w2c_s.at[k], w2c_r.at[k], to_c)

    def w2_ce():
        return remote(w2e, w2so.at[fq : fq + c1], w2c_s.at[N2], w2c_r.at[N2], to_c)

    def w2_ff(k):
        at = (pl.ds(0, fr), cols2(k))
        return remote(w2far.at[at], w2sf.at[at], w2f_s.at[k], w2f_r.at[k], to_c)

    def w2_fg(g):
        at = (pl.ds(fr, 2 * c1), pl.ds(g * wide, wide))
        return remote(w2far.at[at], w2sf.at[at], w2f_s.at[N2 + g], w2f_r.at[N2 + g], to_c)

    def xrows(t):
        return pl.ds(pl.multiple_of(t * piece, piece), piece)

    def xn_x(t):
        return remote(xn.at[xrows(t)], xn.at[xrows(t + NX)], xn_s.at[t], xn_r.at[t], to_x)

    def p_x(i, k):
        at = (pl.ds(pl.multiple_of(i * sub, sub), sub), cols2(k))
        return remote(psend.at[at], precv.at[at], p_s.at[k * 4 + i], p_r.at[k * 4 + i], to_x)

    barrier = pltpu.get_barrier_semaphore()
    for to in (to_y, to_x, to_c):
        pl.semaphore_signal(barrier, inc=1, device_id=to, device_id_type=MESH)
    pl.semaphore_wait(barrier, 3)

    for j in range(AHEAD):
        w1_y(j).start()

    @pl.loop(0, N1)
    def _(j):
        w1_c(j).start()

    def gam_in():
        return [
            pltpu.make_async_copy(gamma.at[:, pl.ds(off, half)], gam.at[:, i * half : (i + 1) * half], io_sem.at[i])
            for i, off in enumerate((near, away))
        ]

    def x_in(t, slot):
        return [
            pltpu.make_async_copy(
                x.at[xrows(t), pl.ds(off, half)],
                act.at[slot, 0:piece, i * half : (i + 1) * half],
                act_sem.at[slot, i],
            )
            for i, off in enumerate((near, away))
        ]

    for c in gam_in():
        c.start()
    for c in x_in(0, 0):
        c.start()
    for c in gam_in():
        c.wait()

    @pl.loop(0, NX)
    def _(t):
        slot = t % 2

        @pl.when(t + 1 < NX)
        def _():
            for c in x_in(t + 1, 1 - slot):
                c.start()

        for c in x_in(t, slot):
            c.wait()

        @pl.loop(0, piece // 16)
        def _(r):
            at = pl.multiple_of(r * 16, 16)
            xs = act[slot, pl.ds(at, 16), 0:d].astype(F32)
            xc = xs - jnp.mean(xs, axis=1, keepdims=True)
            var = jnp.mean(xc * xc, axis=1, keepdims=True)
            act[slot, pl.ds(piece + at, 16), 0:d] = (xc * lax.rsqrt(var + EPS) * gam[...]).astype(BF16)

        out = pltpu.make_async_copy(act.at[slot, piece : 2 * piece, 0:d], xn.at[xrows(t)], io_sem.at[2])
        out.start()
        out.wait()

        @pl.when(t < NX // 2)
        def _():
            xn_x(t).start()

    def hcol(j, q):
        return pl.multiple_of(_where(j < NR, q * fr + j * c1, kr + (j - NR) * 2 * c1 + q * c1), c1)

    def tile_rows(m):
        return _where(m < 4, 2 * m, 2 + m), m < 4

    def hrows(r):
        return pl.ds(pl.multiple_of(r * sub, sub), sub)

    def a1_in(m, slot, go):
        r0, two = tile_rows(m)

        def one(i):
            c = pltpu.make_async_copy(
                xn.at[hrows(r0 + i)], act.at[slot, :, i * d : (i + 1) * d], act_sem.at[slot, i]
            )
            c.start() if go else c.wait()

        one(0)
        pl.when(two)(lambda: one(1))

    def w1_in(j, q, slot, go):
        def load(i, ref, at):
            c = pltpu.make_async_copy(ref.at[at], wb.at[slot, i * half : (i + 1) * half], w_sem.at[slot, i])
            c.start() if go else c.wait()

        if not go:
            for i in BOTH:
                load(i, w1far, cols1(j))
            return
        pl.when((q == 0) & (j < N1))(lambda: load(0, w1, cols1(j)))
        pl.when((q == 0) & (j == N1))(lambda: load(0, w1e, (everything, everything)))
        pl.when(q == 0)(lambda: load(1, w1far, cols1(j)))

        @pl.when(q == 1)
        def _():
            load(0, w1so, cols1(j))
            load(1, w1sf, cols1(j))

    starts1, total1 = _bounds1()
    first2, first3, first4 = (
        next(at for at, (_, (m0, nm)) in zip(starts1, STEPS1) if m0 == m) for m in (2, 4, 5)
    )

    def arrive1(s):
        j, q, m = _step1(s)
        first = m == _first_tile(j)

        @pl.when(first & (q == 0))
        def _():
            w1_yr(j).wait_recv()
            w1_f(j).start()

            @pl.when(j + AHEAD < NR - 1)
            def _():
                w1_y(j + AHEAD).start()

            @pl.when(j + AHEAD == NR - 1)
            def _():
                for t in range(len(tail)):
                    w1_yt(t).start()
                w1_e().start()
                w2_e().start()

            @pl.when(j == 2)
            def _():
                for t in range(NX // 2, NX):
                    xn_x(t).start()

            @pl.when(j == 4)
            def _():
                for k in range(N2):
                    w2_c(k).start()

        @pl.when(first & (q == 1))
        def _():
            w1_cr(j).wait_recv()
            w1_f(j).wait_recv()

        for at, lo, hi in ((first2, 0, 4), (first3, 4, 6), (first4, 6, 8)):

            @pl.when(s == at)
            def _():
                for t in range(lo, hi):
                    xn_x(t).wait_recv()

    def load1(s, aslot, wslot, a_new, w_new):
        j, q, m = _step1(s)
        pl.when(a_new)(lambda: a1_in(m, aslot, True))
        pl.when(w_new)(lambda: w1_in(j, q, wslot, True))

    def h_out(s, i):
        j, q, m = _step1(s)
        r0, _ = tile_rows(m)
        return pltpu.make_async_copy(
            hout.at[s % 2, pl.ds(pl.multiple_of(i * sub, sub), sub)],
            h.at[hrows(r0 + i), pl.ds(hcol(j, q), c1)],
            h_sem.at[s % 2, i],
        )

    def h_done(s):
        _, two = tile_rows(_step1(s)[2])
        h_out(s, 0).wait()
        pl.when(two)(lambda: h_out(s, 1).wait())

    def first_product(lo, hi):
        arrive1(lo)
        load1(lo, 0, 0, True, True)

        def step(s, carry):
            aslot, wslot, a_fresh, w_fresh = carry
            j, q, m = _step1(s)
            nj, nq, nm = _step1(s + 1)
            more = s + 1 < hi
            a_new = more & (nm != m)
            w_new = more & ((nj != j) | (nq != q))
            na = _where(a_new, 1 - aslot, aslot)
            nw = _where(w_new, 1 - wslot, wslot)
            pl.when(more)(lambda: arrive1(s + 1))
            load1(s + 1, na, nw, a_new, w_new)
            pl.when(a_fresh == 1)(lambda: a1_in(m, aslot, False))
            pl.when(w_fresh == 1)(lambda: w1_in(j, q, wslot, False))
            pl.when(s >= lo + 2)(lambda: h_done(s - 2))
            _, two = tile_rows(m)

            @pl.loop(0, _where(two, 2, 1))
            def _(i):
                u = jnp.dot(
                    act[aslot, :, pl.ds(pl.multiple_of(i * d, d), d)], wb[wslot, 0:d], preferred_element_type=F32
                )
                hout[s % 2, pl.ds(pl.multiple_of(i * sub, sub), sub)] = jax.nn.gelu(u, approximate=True).astype(BF16)
                h_out(s, i).start()

            return na, nw, _where(a_new, 1, 0), _where(w_new, 1, 0)

        one, nil = jnp.int32(1), jnp.int32(0)
        lax.fori_loop(lo, hi, step, (nil, nil, one, one))
        h_done(hi - 2)
        h_done(hi - 1)

    def p_in(i, k, slot):
        return pltpu.make_async_copy(precv.at[hrows(i), cols2(k)], pin.at[slot], in_sem.at[slot, 2])

    def a2_in(typ, k, i, slot, go):
        r = _where(typ == REM, 4, 0) + i

        def wait_or_start(c):
            c.start() if go else c.wait()

        @pl.when(typ != END)
        def _():
            wait_or_start(pltpu.make_async_copy(h.at[hrows(r), 0:kr], act.at[slot, :, 0:kr], act_sem.at[slot, 0]))

        @pl.when(typ == END)
        def _():
            wait_or_start(
                pltpu.make_async_copy(h.at[hrows(r), kr : kr + ke], act.at[slot, :, 0:ke], act_sem.at[slot, 0])
            )
            ycol = pl.multiple_of(_where(k < N2, near, away) + (k % N2) * c2, c2)
            wait_or_start(pltpu.make_async_copy(pown.at[hrows(i), cols2(k)], pback.at[slot], in_sem.at[slot, 0]))
            wait_or_start(pltpu.make_async_copy(x.at[hrows(i), pl.ds(ycol, c2)], xin.at[slot], in_sem.at[slot, 1]))
            if go:

                @pl.when(k < LAST)
                def _():
                    p_x(i, k).wait_recv()
                    p_in(i, k, slot).start()

    def w2_in(typ, k, slot, go):
        def load(n, at, rows_, ref, from_, kk):
            c = pltpu.make_async_copy(
                ref.at[pl.ds(from_, rows_), cols2(kk)], wb.at[slot, at : at + rows_], w_sem.at[slot, n]
            )
            c.start() if go else c.wait()

        def main(own, sib, kk):
            load(0, 0, fr, own, 0, kk)
            load(1, fr, fr, sib, 0, kk)

        def rest(own, ext, ext_at, sib, kk):
            load(0, 0, c1, own, fr, kk)
            load(1, c1, c1, sib, fr, kk)
            load(2, 2 * c1, c1, ext, ext_at, kk)
            load(3, 3 * c1, c1, sib, fq, kk)

        def both(side, kk, own, ext, ext_at, sib):
            pl.when(side & (typ != END))(lambda: main(own, sib, kk))
            pl.when(side & (typ == END))(lambda: rest(own, ext, ext_at, sib, kk))

        if not go:
            pl.when(typ != END)(lambda: main(w2far, w2sf, 0))
            pl.when(typ == END)(lambda: rest(w2far, w2far, fq, w2sf, 0))
            return
        both(k < N2, k, w2, w2e, 0, w2so)
        both(k >= N2, k - N2, w2far, w2far, fq, w2sf)

    def arrive2(v):
        at = {visit: n for n, visit in enumerate(VISITS)}
        for n in range(len(VISITS)):
            visit = VISITS[n]
            todo = []
            for u in SEND_F.get(visit, ()):
                todo.append(lambda u=u: w2_yf(u).start())
            if visit in SEND_G:
                todo.append(lambda g=SEND_G[visit]: [c.start() for c in w2_yg(g)])
            if visit in PASS_F:
                u = PASS_F[visit]
                todo.append(lambda u=u: (w2_yf(u).wait_recv(), w2_ff(u).start()))
            if visit in PASS_G:
                g = PASS_G[visit]
                todo.append(lambda g=g: ([c.wait_recv() for c in w2_yg(g)], w2_fg(g).start()))
            if visit[0] == REM:
                k = visit[1]
                todo.append(lambda k=k: w2_c(k).wait_recv() if k < N2 else w2_ff(k - N2).wait_recv())
            if n == min(at[B(k)] for k in range(N2)):
                todo.append(lambda: w2_ce().wait_recv())
            for g in BOTH:
                if n == min(at[B(N2 + 3 * g + k)] for k in range(3)):
                    todo.append(lambda g=g: w2_fg(g).wait_recv())
            if todo:

                @pl.when(v == n)
                def _(todo=todo):
                    for f in todo:
                        f()

    def p_out(to, k, i, slot):
        return pltpu.make_async_copy(pout.at[slot], to.at[hrows(i), cols2(k)], out_sem.at[slot])

    def y_out(k, i):
        ycol = pl.multiple_of(_where(k < N2, near, away) + (k % N2) * c2, c2)
        return pltpu.make_async_copy(yout, y.at[hrows(i), pl.ds(ycol, c2)], out_sem.at[2])

    def last_out(to, slot):
        return pltpu.make_async_copy(pout.at[slot], to, out_sem.at[slot])

    def finish(typ, k, i, slot):
        outside = (k == LAST) & (i == 3)

        @pl.when((typ == REM) | (typ == OWN) | ((typ == END) & outside))
        def _():
            p_out(pown, k, i, slot).wait()

        @pl.when((typ == REM) & jnp.logical_not(outside))
        def _():
            p_x(i, k).start()

        @pl.when((typ == END) & jnp.logical_not(outside))
        def _():
            y_out(k, i).wait()

    def second_product(lo, hi):
        arrive2(lo)
        typ0, k0 = _visit(lo)
        w2_in(typ0, k0, 0, True)
        a2_in(typ0, k0, jnp.int32(0), 0, True)

        def visit(v, carry):
            typ, k, ptyp, pk = carry
            more = v + 1 < hi
            ntyp, nk = _visit(v + 1)
            wslot = (v - lo) % 2

            def tile(i, before):
                btyp, bk, bi = before
                slot = i % 2
                last = i == 3

                @pl.when(last & more)
                def _():
                    arrive2(v + 1)
                    w2_in(ntyp, nk, 1 - wslot, True)

                @pl.when(more | (i < 3))
                def _():
                    a2_in(_where(last, ntyp, typ), _where(last, nk, k), _where(last, 0, i + 1), 1 - slot, True)

                a2_in(typ, k, i, slot, False)
                pl.when(i == 0)(lambda: w2_in(typ, k, wslot, False))

                @pl.when(typ != END)
                def _():
                    pout[slot] = jnp.dot(act[slot, :, 0:kr], wb[wslot, 0:kr], preferred_element_type=F32)

                @pl.when(typ == END)
                def _():
                    pout[slot] = jnp.dot(act[slot, :, 0:ke], wb[wslot, 0:ke], preferred_element_type=F32)

                finish(btyp, bk, bi, 1 - slot)
                pl.when(typ == OWN)(lambda: p_out(pown, k, i, slot).start())
                outside = (k == LAST) & last
                inside = jnp.logical_not(outside)
                pl.when((typ == REM) & inside)(lambda: p_out(psend, k, i, slot).start())
                pl.when((typ == REM) & outside)(lambda: last_out(xlast, slot).start())

                @pl.when((typ == END) & outside)
                def _():
                    pout[slot] = pback[slot] + pout[slot]
                    last_out(olast, slot).start()

                @pl.when((typ == END) & inside)
                def _():
                    @pl.when(k == LAST)
                    def _():
                        p_x(i, k).wait_recv()
                        p_in(i, k, slot).start()

                    p_in(i, k, slot).wait()
                    total = (pback[slot] + pout[slot]) + pin[slot]
                    yout[...] = (xin[slot].astype(F32) + total).astype(BF16)
                    y_out(k, i).start()

                return typ, k, i

            ptyp, pk, _ = lax.fori_loop(0, 4, tile, (ptyp, pk, jnp.int32(3)))
            return ntyp, nk, ptyp, pk

        _, _, ptyp, pk = lax.fori_loop(lo, hi, visit, (typ0, k0, jnp.int32(3), jnp.int32(0)))
        finish(ptyp, pk, jnp.int32(3), 1)

    def junction():
        final = len(tail) - 1

        def lanes(t):
            at = 0 if t < 2 else 2 * sum(w for _, w in tail[1:t])
            return (0 if t == 0 else d), at

        def w_tail(t, part):
            refs = ((w1, w1so), (w1far, w1sf))[part]
            r, at = lanes(t)
            w = tail[t][1]
            return [
                pltpu.make_async_copy(
                    refs[q].at[cols_t(t)],
                    wb.at[0, r + part * half : r + (part + 1) * half, at + q * w : at + (q + 1) * w],
                    tail_sem.at[t, part, q],
                )
                for q in BOTH
            ]

        def xn_in(i):
            return pltpu.make_async_copy(xn.at[hrows(4 + i)], act.at[1, :, 0:d], act_sem.at[1, 0])

        def h_at(i, q, col, width):
            return h.at[hrows(4 + i), q * fr + col : q * fr + col + width]

        def h_in(i):
            return [
                pltpu.make_async_copy(h_at(i, q, 0, t0), act.at[0, :, q * fr : q * fr + t0], act_sem.at[0, q])
                for q in BOTH
            ]

        def first_sum(block):
            return remote(pout.at[0, block], precv.at[block, 0:c2], p_s.at[0], p_r.at[0], to_x)

        def hidden(t, block=everything):
            r, at = lanes(t)
            u = jnp.dot(act[1, block, 0:d], wb[0, r : r + d, at : at + 2 * tail[t][1]], preferred_element_type=F32)
            return jax.nn.gelu(u, approximate=True).astype(BF16)

        def arrive(t):
            w1_yt(t).wait_recv()
            w1_ft(t).start()
            w_tail(t, 1)[0].start()
            if t == final:
                w1_y(N1 - 1).start()
                w1_e().wait_recv()
                w1_ye().start()
                w2_yf(0).start()
                w2_yf(1).start()
                w2_e().wait_recv()
            w1_ft(t).wait_recv()
            w_tail(t, 1)[1].start()
            if t == final:
                w1_ce().start()
                w2_ce().start()
            for part in BOTH:
                for c in w_tail(t, part):
                    c.wait()

        w1_c(NR - 1).wait_recv()
        for t in range(len(tail)):
            for c in w_tail(t, 0):
                c.start()
        xn_in(0).start()
        for c in h_in(0):
            c.start()
        w2_c(0).wait_recv()
        rem, zero = jnp.int32(REM), jnp.int32(0)
        w2_in(rem, zero, 1, True)
        arrive(0)
        w2_in(rem, zero, 1, False)

        def tile_(i, carry):
            xn_in(i).wait()
            out = []
            for t in range(final):
                if t > 0:
                    pl.when(i == 0)(lambda t=t: arrive(t))
                g = hidden(t)
                if t == 0:
                    for c in h_in(i):
                        c.wait()
                off, w = tail[t]
                for q in BOTH:
                    at = q * fr + t0 + off
                    act[0, :, at : at + w] = g[:, q * w : (q + 1) * w]
                    out.append(
                        pltpu.make_async_copy(act.at[0, :, at : at + w], h_at(i, q, t0 + off, w), h_sem.at[t, q])
                    )
                    out[-1].start()
            off, w = tail[final]
            n = fr - w
            slot = _where(i == 0, 0, 1)
            pout[slot] = jnp.dot(act[0, :, 0:n], wb[1, 0:n], preferred_element_type=F32) + jnp.dot(
                act[0, :, fr : fr + n], wb[1, fr : fr + n], preferred_element_type=F32
            )
            for c in out:
                c.wait()

            @pl.when(i < 3)
            def _():
                for c in h_in(i + 1):
                    c.start()

            pl.when(i == 0)(lambda: arrive(final))
            block = sub // 2

            @pl.loop(0, 2)
            def _(m):
                at = pl.ds(pl.multiple_of(m * block, block), block)
                g = hidden(final, at)
                hout[0, at, 0 : 2 * w] = g
                pout[slot, at] += jnp.dot(g[:, 0:w], wb[1, n:fr], preferred_element_type=F32) + jnp.dot(
                    g[:, w : 2 * w], wb[1, fr + n : kr], preferred_element_type=F32
                )
                pl.when(i == 0)(lambda: first_sum(at).start())

            pl.when(i < 3)(lambda: xn_in(i + 1).start())
            out = []
            for q in BOTH:
                out.append(
                    pltpu.make_async_copy(
                        hout.at[0, 0:sub, q * w : (q + 1) * w], h_at(i, q, t0 + off, w), h_sem.at[2, q]
                    )
                )
                out[-1].start()

            @pl.when(i > 0)
            def _():
                sent = p_out(psend, zero, i, 1)
                sent.start()
                sent.wait()
                p_x(i, 0).start()

            for c in out:
                c.wait()
            return carry

        lax.fori_loop(0, 4, tile_, jnp.int32(0))
        p_x(0, 0).wait_send()

    @pl.loop(0, 2)
    def _(phase):
        early = phase == 0
        cut = starts1[BREAK1]
        first_product(_where(early, 0, cut), _where(early, cut, total1))
        pl.when(early)(junction)
        second_product(_where(early, 0, BREAK2), _where(early, BREAK2, len(VISITS)))

    @pl.loop(0, N1 + 1)
    def _(j):
        w1_cr(j).wait_send()

    @pl.loop(0, N1 + 1)
    def _(j):
        @pl.when(j != NR - 1)
        def _():
            w1_yr(j).wait_send()
            w1_f(j).wait_send()

    for t in range(len(tail)):
        w1_yt(t).wait_send()
        w1_ft(t).wait_send()

    @pl.loop(0, N2)
    def _(k):
        w2_yf(k).wait_send()
        w2_c(k).wait_send()
        w2_ff(k).wait_send()

    w1_e().wait_send()
    w2_e().wait_send()
    w2_ce().wait_send()
    for g in BOTH:
        for c in w2_yg(g):
            c.wait_send()
        w2_fg(g).wait_send()

    @pl.loop(0, NX)
    def _(t):
        xn_x(t).wait_send()

    @pl.loop(1, 2 * N2 * 4 - 1)
    def _(s):
        p_x(s % 4, s // 4).wait_send()


PUTS = 16


def _put(src, dst, buf, sems_in, sems_out):
    n = src.shape[0] // PUTS

    def get(i):
        return pltpu.make_async_copy(src.at[i * n : (i + 1) * n], buf.at[i], sems_in.at[i])

    def put(i):
        return pltpu.make_async_copy(buf.at[i], dst.at[i * n : (i + 1) * n], sems_out.at[i])

    for i in range(PUTS):
        get(i).start()
    for i in range(PUTS):
        get(i).wait()
        put(i).start()
    for i in range(PUTS):
        put(i).wait()


def solution(mesh):
    def body(x, gamma, w1, w2):
        rows, d = x.shape
        half, fq = w1.shape
        sub = rows // 4
        c1, c2 = fq // N1, half // N2

        def hbm(*shape, dtype=BF16):
            return jax.ShapeDtypeStruct(shape, dtype)

        dma = pltpu.SemaphoreType.DMA
        outs = (
            hbm(rows, d),
            hbm(sub, c2, dtype=F32),
            hbm(sub, c2, dtype=F32),
            hbm(2 * rows, d),
            hbm(half, c1), hbm(half, fq + c1), hbm(half, fq + c1), hbm(half, fq + c1),
            hbm(c1, half), hbm(fq + c1, half), hbm(fq + c1, half), hbm(fq + c1, half),
            hbm(2 * rows, 2 * (fq + c1)),
            hbm(rows, d, dtype=F32), hbm(rows, d, dtype=F32), hbm(rows, d, dtype=F32),
        )
        sent = (NX, 2, N1 + 3, N1 + 1, N1 + 3, N2 + 4, N2 + 1, N2 + 2, 8 * N2)
        out = pl.pallas_call(
            _kernel,
            name="mlp",
            out_shape=outs,
            in_specs=[pl.BlockSpec(memory_space=pl.ANY)] * 4,
            out_specs=tuple([pl.BlockSpec(memory_space=pl.ANY)] * len(outs)),
            scratch_shapes=[
                pltpu.VMEM((2, sub, 2 * d), BF16),
                pltpu.VMEM((2, 2 * fq, c2), BF16),
                pltpu.VMEM((2, 2 * sub, c1), BF16),
                pltpu.VMEM((2, sub, c2), F32),
                pltpu.VMEM((2, sub, c2), F32),
                pltpu.VMEM((2, sub, c2), F32),
                pltpu.VMEM((2, sub, c2), BF16),
                pltpu.VMEM((sub, c2), BF16),
                pltpu.VMEM((1, d), F32),
                *(dma(n) for n in ((2, 2), (2, 4), (3, 2), (3,), (3,), (2, 3), (2, 2, 2))),
                *(dma((n,)) for n in sent for _ in BOTH),
            ],
            compiler_params=pltpu.CompilerParams(
                collective_id=0, has_side_effects=True, vmem_limit_bytes=67_000_000
            ),
        )(x, gamma.reshape(1, d), w1, w2)
        got = lax.ppermute(out[1], "tp", [(i, (i + 2) % 4) for i in range(4)])
        y = pl.pallas_call(
            _put,
            name="put",
            out_shape=hbm(rows, d),
            in_specs=[pl.BlockSpec(memory_space=pl.ANY)],
            out_specs=pl.BlockSpec(memory_space=pl.ANY),
            scratch_shapes=[pltpu.VMEM((PUTS, rows // PUTS, d), BF16), dma((PUTS,)), dma((PUTS,))],
            compiler_params=pltpu.CompilerParams(vmem_limit_bytes=40_000_000),
            cost_estimate=pl.CostEstimate(flops=30_000_000_000, bytes_accessed=4 * rows * d, transcendentals=0),
        )(out[0])
        at = (3 * sub, (1 - lax.axis_index("fsdp")) * half + (N2 - 1) * c2)
        tile = lax.dynamic_slice(x, at, (sub, c2)).astype(F32) + (out[2] + got)
        return lax.dynamic_update_slice(y, tile.astype(BF16), at)

    return jax.shard_map(
        body,
        mesh=mesh,
        in_specs=(P(("fsdp", "tp"), None), P(None), P("fsdp", "tp"), P("tp", "fsdp")),
        out_specs=P(("fsdp", "tp"), None),
        check_vma=False,
    )
```

```python
import jax
import jax.numpy as jnp
from jax import lax
from jax.experimental import pallas as pl
from jax.experimental.pallas import tpu as pltpu
from jax.sharding import PartitionSpec as P

EPS = 1e-6
F32 = jnp.float32
BF16 = jnp.bfloat16
MESH = pl.DeviceIdType.MESH

N1 = 12
NR = N1 - 1
N2 = 6
NX = 8
BOTH = range(2)
AHEAD = 3

STEPS1 = (
    ((0, 4), (0, 2)),
    ((0, 4), (2, 1)),
    ((4, 2), (0, 3)),
    ((0, 3), (4, 1)),
    ((6, 1), (0, 3)),
    ((3, 4), (4, 1)),
    ((7, 1), (2, 1)),
    ((7, 1), (4, 1)),
    ((0, 8), (5, 1)),
    ((8, 2), (2, 2)),
    ((7, 6), (0, 2)),
)
BREAK1 = 10

REM, OWN, END = 0, 1, 2
LAST = 2 * N2 - 1
R, A, B = ((lambda k, t=t: (t, k)) for t in (REM, OWN, END))
VISITS = (
    *map(R, range(1, 6)),
    A(0), A(1), R(6), A(2), B(0), B(1), A(3), R(7), B(2), A(4), A(5), R(8), B(3), A(6), A(7), B(4), B(5),
    R(9), A(8), B(6), A(9), B(7), R(10), B(8), A(10), R(11), A(11), B(9), B(10), B(11),
)
BREAK2 = 4
PASS_F = {A(1): 0, B(1): 1, A(5): 2, B(5): 3, B(7): 4, R(11): 5}
PASS_G = {B(4): 0, A(11): 1, B(9): 2, B(10): 3}
SEND_F = {R(2): (2,), R(5): (3, 4), R(7): (5,)}
SEND_G = {R(2): (0,), R(7): (1, 2, 3)}
PARTS_G = ((0, 3), (3, 1), (4, 1), (5, 1))


def _tail(c1):
    w = c1 // 2
    return ((0, w), (w, w))


def _where(cond, a, b):
    return jnp.where(cond, jnp.int32(a), jnp.int32(b))


def _bounds1():
    at, out = 0, []
    for (_, nj), (_, nt) in STEPS1:
        out.append(at)
        at += nj * 2 * nt
    return out, at


def _step1(s):
    starts, _ = _bounds1()
    rows = [(at, j0, nt, t0) for at, ((j0, _), (t0, nt)) in zip(starts, STEPS1)]
    start, j0, nt, t0 = (jnp.int32(v) for v in rows[0])
    for row in rows[1:]:
        late = s >= row[0]
        start, j0, nt, t0 = (_where(late, new, old) for new, old in zip(row, (start, j0, nt, t0)))
    u = s - start
    pair = u // nt
    return j0 + pair // 2, pair % 2, t0 + u % nt


def _first_tile(j):
    return _where(j < 7, 0, _where(j < NR - 1, 2, _where(j == NR - 1, 9, 0)))


def _visit(v):
    code = jnp.int32(0)
    for n, (t, k) in enumerate(VISITS):
        code = _where(v == n, t * 16 + k, code)
    return code // 16, code % 16


def _kernel(
    x, gamma, w1, w2,
    y, xlast, olast, xn, w1e, w1far, w1so, w1sf, w2e, w2far, w2so, w2sf, h, psend, pown, precv,
    act, wb, hout, pout, pin, pback, xin, yout, gam,
    act_sem, w_sem, h_sem, io_sem, out_sem, in_sem, tail_sem,
    xn_s, xn_r, e_s, e_r, w1y_s, w1y_r, w1c_s, w1c_r, w1f_s, w1f_r,
    w2y_s, w2y_r, w2c_s, w2c_r, w2f_s, w2f_r, p_s, p_r,
):
    a = lax.axis_index("fsdp")
    b = lax.axis_index("tp")
    to_y = {"fsdp": 1 - a}
    to_x = {"tp": lax.rem(b + 2, 4)}
    to_c = {"tp": b + 1 - 2 * lax.rem(b, 2)}
    rows, d = x.shape
    half, fq = w1.shape
    sub = rows // 4
    c1 = fq // N1
    c2 = half // N2
    tail = _tail(c1)
    fr = NR * c1
    t0 = fr - c1
    kr = 2 * fr
    ke = 4 * c1
    piece = rows // NX
    near = pl.multiple_of(a * half, half)
    away = pl.multiple_of((1 - a) * half, half)
    everything = slice(None)

    def remote(src, dst, ssem, rsem, to):
        return pltpu.make_async_remote_copy(
            src_ref=src, dst_ref=dst, send_sem=ssem, recv_sem=rsem, device_id=to, device_id_type=MESH
        )

    def cols1(j):
        return (everything, pl.ds(pl.multiple_of(j * c1, c1), c1))

    def cols2(k):
        return pl.ds(pl.multiple_of(k * c2, c2), c2)

    def w1_y(j):
        return remote(w1.at[cols1(j)], w1far.at[cols1(j)], w1y_s.at[j], w1y_r.at[j], to_y)

    def w1_ye():
        return remote(w1e, w1far.at[cols1(N1)], w1y_s.at[N1], w1y_r.at[N1], to_y)

    def w1_yr(j):
        return remote(w1far.at[cols1(j)], w1far.at[cols1(j)], w1y_s.at[j], w1y_r.at[j], to_y)

    def w1_c(j):
        return remote(w1.at[cols1(j)], w1so.at[cols1(j)], w1c_s.at[j], w1c_r.at[j], to_c)

    def w1_ce():
        return remote(w1e, w1so.at[cols1(N1)], w1c_s.at[N1], w1c_r.at[N1], to_c)

    def w1_cr(j):
        return remote(w1so.at[cols1(j)], w1so.at[cols1(j)], w1c_s.at[j], w1c_r.at[j], to_c)

    def w1_f(j):
        return remote(w1far.at[cols1(j)], w1sf.at[cols1(j)], w1f_s.at[j], w1f_r.at[j], to_c)

    def cols_t(t):
        return (everything, pl.ds(t0 + tail[t][0], tail[t][1]))

    def tail_at(t):
        return NR - 1 if t == 0 else N1 + t

    def w1_yt(t):
        return remote(w1.at[cols_t(t)], w1far.at[cols_t(t)], w1y_s.at[tail_at(t)], w1y_r.at[tail_at(t)], to_y)

    def w1_ft(t):
        return remote(w1far.at[cols_t(t)], w1sf.at[cols_t(t)], w1f_s.at[tail_at(t)], w1f_r.at[tail_at(t)], to_c)

    def w1_e():
        return remote(w1.at[cols1(N1 - 1)], w1e, e_s.at[0], e_r.at[0], to_x)

    def w2_e():
        return remote(w2.at[fr:fq], w2e, e_s.at[1], e_r.at[1], to_x)

    def w2_yf(k):
        at = (pl.ds(0, fr), cols2(k))
        return remote(w2.at[at], w2far.at[at], w2y_s.at[k], w2y_r.at[k], to_y)

    def cols_g(g):
        k, n = PARTS_G[g]
        return pl.ds(k * c2, n * c2)

    def w2_yg(g):
        at, to, n = (pl.ds(fr, c1), cols_g(g)), (pl.ds(fq, c1), cols_g(g)), N2 + g + g
        return (
            remote(w2.at[at], w2far.at[at], w2y_s.at[n], w2y_r.at[n], to_y),
            remote(w2e.at[:, cols_g(g)], w2far.at[to], w2y_s.at[n + 1], w2y_r.at[n + 1], to_y),
        )

    def w2_c(k):
        at = (everything, cols2(k))
        return remote(w2.at[at], w2so.at[pl.ds(0, fq), cols2(k)], w2c_s.at[k], w2c_r.at[k], to_c)

    def w2_ce():
        return remote(w2e, w2so.at[fq : fq + c1], w2c_s.at[N2], w2c_r.at[N2], to_c)

    def w2_ff(k):
        at = (pl.ds(0, fr), cols2(k))
        return remote(w2far.at[at], w2sf.at[at], w2f_s.at[k], w2f_r.at[k], to_c)

    def w2_fg(g):
        at = (pl.ds(fr, 2 * c1), cols_g(g))
        return remote(w2far.at[at], w2sf.at[at], w2f_s.at[N2 + g], w2f_r.at[N2 + g], to_c)

    def xrows(t):
        return pl.ds(pl.multiple_of(t * piece, piece), piece)

    def xn_x(t):
        return remote(xn.at[xrows(t)], xn.at[xrows(t + NX)], xn_s.at[t], xn_r.at[t], to_x)

    def p_x(i, k):
        at = (pl.ds(pl.multiple_of(i * sub, sub), sub), cols2(k))
        return remote(psend.at[at], precv.at[at], p_s.at[k * 4 + i], p_r.at[k * 4 + i], to_x)

    barrier = pltpu.get_barrier_semaphore()
    for to in (to_y, to_x, to_c):
        pl.semaphore_signal(barrier, inc=1, device_id=to, device_id_type=MESH)
    pl.semaphore_wait(barrier, 3)

    for j in range(AHEAD):
        w1_y(j).start()

    @pl.loop(0, N1)
    def _(j):
        w1_c(j).start()

    def gam_in():
        return [
            pltpu.make_async_copy(gamma.at[:, pl.ds(off, half)], gam.at[:, i * half : (i + 1) * half], io_sem.at[i])
            for i, off in enumerate((near, away))
        ]

    def x_in(t, slot):
        return [
            pltpu.make_async_copy(
                x.at[xrows(t), pl.ds(off, half)],
                act.at[slot, :piece, i * half : (i + 1) * half],
                act_sem.at[slot, i],
            )
            for i, off in enumerate((near, away))
        ]

    for c in gam_in():
        c.start()
    for c in x_in(0, 0):
        c.start()
    for c in gam_in():
        c.wait()

    @pl.loop(0, NX)
    def _(t):
        slot = t % 2

        @pl.when(t + 1 < NX)
        def _():
            for c in x_in(t + 1, 1 - slot):
                c.start()

        for c in x_in(t, slot):
            c.wait()

        @pl.loop(0, piece // 16)
        def _(r):
            at = pl.multiple_of(r * 16, 16)
            xs = act[slot, pl.ds(at, 16), :d].astype(F32)
            xc = xs - jnp.mean(xs, axis=1, keepdims=True)
            var = jnp.mean(xc * xc, axis=1, keepdims=True)
            act[slot, pl.ds(piece + at, 16), :d] = (xc * lax.rsqrt(var + EPS) * gam[...]).astype(BF16)

        out = pltpu.make_async_copy(act.at[slot, piece : 2 * piece, :d], xn.at[xrows(t)], io_sem.at[2])
        out.start()
        out.wait()

        @pl.when(t < NX // 2)
        def _():
            xn_x(t).start()

    def hcol(j, q):
        return pl.multiple_of(_where(j < NR, q * fr + j * c1, kr + (j - NR) * 2 * c1 + q * c1), c1)

    def tile_rows(m):
        return _where(m < 4, 2 * m, 2 + m), m < 4

    def hrows(r):
        return pl.ds(pl.multiple_of(r * sub, sub), sub)

    def a1_in(m, slot, go):
        r0, two = tile_rows(m)

        def one(i):
            c = pltpu.make_async_copy(
                xn.at[hrows(r0 + i)], act.at[slot, :, i * d : (i + 1) * d], act_sem.at[slot, i]
            )
            c.start() if go else c.wait()

        one(0)
        pl.when(two)(lambda: one(1))

    def w1_in(j, q, slot, go):
        def load(i, ref, at):
            c = pltpu.make_async_copy(ref.at[at], wb.at[slot, i * half : (i + 1) * half], w_sem.at[slot, i])
            c.start() if go else c.wait()

        if not go:
            for i in BOTH:
                load(i, w1far, cols1(j))
            return
        pl.when((q == 0) & (j < N1))(lambda: load(0, w1, cols1(j)))
        pl.when((q == 0) & (j == N1))(lambda: load(0, w1e, (everything, everything)))
        pl.when(q == 0)(lambda: load(1, w1far, cols1(j)))

        @pl.when(q == 1)
        def _():
            load(0, w1so, cols1(j))
            load(1, w1sf, cols1(j))

    starts1, total1 = _bounds1()
    first2, first3, first4 = (
        next(at for at, (_, (m0, nm)) in zip(starts1, STEPS1) if m0 == m) for m in (2, 4, 5)
    )

    def arrive1(s):
        j, q, m = _step1(s)
        first = m == _first_tile(j)

        @pl.when(first & (q == 0))
        def _():
            w1_yr(j).wait_recv()
            w1_f(j).start()

            @pl.when(j + AHEAD < NR - 1)
            def _():
                w1_y(j + AHEAD).start()

            @pl.when(j + AHEAD == NR - 1)
            def _():
                for t in range(len(tail)):
                    w1_yt(t).start()
                w1_e().start()
                w2_e().start()

            @pl.when(j == 2)
            def _():
                for t in range(NX // 2, NX):
                    xn_x(t).start()

            @pl.when(j == 4)
            def _():
                for k in range(N2):
                    w2_c(k).start()

        @pl.when(first & (q == 1))
        def _():
            w1_cr(j).wait_recv()
            w1_f(j).wait_recv()

        for at, lo, hi in ((first2, 0, 4), (first3, 4, 6), (first4, 6, 8)):

            @pl.when(s == at)
            def _():
                for t in range(lo, hi):
                    xn_x(t).wait_recv()

    def load1(s, aslot, wslot, a_new, w_new):
        j, q, m = _step1(s)
        pl.when(a_new)(lambda: a1_in(m, aslot, True))
        pl.when(w_new)(lambda: w1_in(j, q, wslot, True))

    def h_out(s, i):
        j, q, m = _step1(s)
        r0, _ = tile_rows(m)
        return pltpu.make_async_copy(
            hout.at[s % 2, pl.ds(pl.multiple_of(i * sub, sub), sub)],
            h.at[hrows(r0 + i), pl.ds(hcol(j, q), c1)],
            h_sem.at[s % 2, i],
        )

    def h_done(s):
        _, two = tile_rows(_step1(s)[2])
        h_out(s, 0).wait()
        pl.when(two)(lambda: h_out(s, 1).wait())

    def first_product(lo, hi):
        arrive1(lo)
        load1(lo, 0, 0, True, True)

        def step(s, carry):
            aslot, wslot, a_fresh, w_fresh = carry
            j, q, m = _step1(s)
            nj, nq, nm = _step1(s + 1)
            more = s + 1 < hi
            a_new = more & (nm != m)
            w_new = more & ((nj != j) | (nq != q))
            na = _where(a_new, 1 - aslot, aslot)
            nw = _where(w_new, 1 - wslot, wslot)
            pl.when(more)(lambda: arrive1(s + 1))
            load1(s + 1, na, nw, a_new, w_new)
            pl.when(a_fresh == 1)(lambda: a1_in(m, aslot, False))
            pl.when(w_fresh == 1)(lambda: w1_in(j, q, wslot, False))
            pl.when(s >= lo + 2)(lambda: h_done(s - 2))
            _, two = tile_rows(m)

            @pl.loop(0, _where(two, 2, 1))
            def _(i):
                u = jnp.dot(
                    act[aslot, :, pl.ds(pl.multiple_of(i * d, d), d)], wb[wslot, :d], preferred_element_type=F32
                )
                hout[s % 2, pl.ds(pl.multiple_of(i * sub, sub), sub)] = jax.nn.gelu(u, approximate=True).astype(BF16)
                h_out(s, i).start()

            return na, nw, _where(a_new, 1, 0), _where(w_new, 1, 0)

        one, nil = jnp.int32(1), jnp.int32(0)
        lax.fori_loop(lo, hi, step, (nil, nil, one, one))
        h_done(hi - 2)
        h_done(hi - 1)

    def p_in(i, k, slot):
        return pltpu.make_async_copy(precv.at[hrows(i), cols2(k)], pin.at[slot], in_sem.at[slot, 2])

    def a2_in(typ, k, i, slot, go):
        r = _where(typ == REM, 4, 0) + i

        def wait_or_start(c):
            c.start() if go else c.wait()

        @pl.when(typ != END)
        def _():
            wait_or_start(pltpu.make_async_copy(h.at[hrows(r), :kr], act.at[slot, :, :kr], act_sem.at[slot, 0]))

        @pl.when(typ == END)
        def _():
            wait_or_start(
                pltpu.make_async_copy(h.at[hrows(r), kr : kr + ke], act.at[slot, :, :ke], act_sem.at[slot, 0])
            )
            ycol = pl.multiple_of(_where(k < N2, near, away) + (k % N2) * c2, c2)
            wait_or_start(pltpu.make_async_copy(pown.at[hrows(i), cols2(k)], pback.at[slot], in_sem.at[slot, 0]))
            wait_or_start(pltpu.make_async_copy(x.at[hrows(i), pl.ds(ycol, c2)], xin.at[slot], in_sem.at[slot, 1]))
            if go:

                @pl.when(k < LAST)
                def _():
                    p_x(i, k).wait_recv()
                    p_in(i, k, slot).start()

    def w2_in(typ, k, slot, go):
        def load(n, at, rows_, ref, from_, kk):
            c = pltpu.make_async_copy(
                ref.at[pl.ds(from_, rows_), cols2(kk)], wb.at[slot, at : at + rows_], w_sem.at[slot, n]
            )
            c.start() if go else c.wait()

        def main(own, sib, kk):
            load(0, 0, fr, own, 0, kk)
            load(1, fr, fr, sib, 0, kk)

        def rest(own, ext, ext_at, sib, kk):
            load(0, 0, c1, own, fr, kk)
            load(1, c1, c1, sib, fr, kk)
            load(2, 2 * c1, c1, ext, ext_at, kk)
            load(3, 3 * c1, c1, sib, fq, kk)

        def both(side, kk, own, ext, ext_at, sib):
            pl.when(side & (typ != END))(lambda: main(own, sib, kk))
            pl.when(side & (typ == END))(lambda: rest(own, ext, ext_at, sib, kk))

        if not go:
            pl.when(typ != END)(lambda: main(w2far, w2sf, 0))
            pl.when(typ == END)(lambda: rest(w2far, w2far, fq, w2sf, 0))
            return
        both(k < N2, k, w2, w2e, 0, w2so)
        both(k >= N2, k - N2, w2far, w2far, fq, w2sf)

    def arrive2(v):
        at = {visit: n for n, visit in enumerate(VISITS)}
        for n in range(len(VISITS)):
            visit = VISITS[n]
            todo = []
            for u in SEND_F.get(visit, ()):
                todo.append(lambda u=u: w2_yf(u).start())
            for g in SEND_G.get(visit, ()):
                todo.append(lambda g=g: [c.start() for c in w2_yg(g)])
            if visit in PASS_F:
                u = PASS_F[visit]
                todo.append(lambda u=u: (w2_yf(u).wait_recv(), w2_ff(u).start()))
            if visit in PASS_G:
                g = PASS_G[visit]
                todo.append(lambda g=g: ([c.wait_recv() for c in w2_yg(g)], w2_fg(g).start()))
            if visit[0] == REM:
                k = visit[1]
                todo.append(lambda k=k: w2_c(k).wait_recv() if k < N2 else w2_ff(k - N2).wait_recv())
            if n == min(at[B(k)] for k in range(N2)):
                todo.append(lambda: w2_ce().wait_recv())
            for g, (k0, nk) in enumerate(PARTS_G):
                if n == min(at[B(N2 + k)] for k in range(k0, k0 + nk)):
                    todo.append(lambda g=g: w2_fg(g).wait_recv())
            if todo:

                @pl.when(v == n)
                def _(todo=todo):
                    for f in todo:
                        f()

    def p_out(to, k, i, slot):
        return pltpu.make_async_copy(pout.at[slot], to.at[hrows(i), cols2(k)], out_sem.at[slot])

    def y_out(k, i):
        ycol = pl.multiple_of(_where(k < N2, near, away) + (k % N2) * c2, c2)
        return pltpu.make_async_copy(yout, y.at[hrows(i), pl.ds(ycol, c2)], out_sem.at[2])

    def last_out(to, slot):
        return pltpu.make_async_copy(pout.at[slot], to, out_sem.at[slot])

    def finish(typ, k, i, slot):
        outside = (k == LAST) & (i == 3)

        @pl.when((typ == REM) | (typ == OWN) | ((typ == END) & outside))
        def _():
            p_out(pown, k, i, slot).wait()

        @pl.when((typ == REM) & jnp.logical_not(outside))
        def _():
            p_x(i, k).start()

        @pl.when((typ == END) & jnp.logical_not(outside))
        def _():
            y_out(k, i).wait()

    def second_product(lo, hi):
        arrive2(lo)
        typ0, k0 = _visit(lo)
        w2_in(typ0, k0, 0, True)
        a2_in(typ0, k0, jnp.int32(0), 0, True)

        def visit(v, carry):
            typ, k, ptyp, pk = carry
            more = v + 1 < hi
            ntyp, nk = _visit(v + 1)
            wslot = (v - lo) % 2

            def tile(i, before):
                btyp, bk, bi = before
                slot = i % 2
                last = i == 3

                @pl.when(last & more)
                def _():
                    arrive2(v + 1)
                    w2_in(ntyp, nk, 1 - wslot, True)

                @pl.when(more | (i < 3))
                def _():
                    a2_in(_where(last, ntyp, typ), _where(last, nk, k), _where(last, 0, i + 1), 1 - slot, True)

                a2_in(typ, k, i, slot, False)
                pl.when(i == 0)(lambda: w2_in(typ, k, wslot, False))

                @pl.when(typ != END)
                def _():
                    pout[slot] = jnp.dot(act[slot, :, :kr], wb[wslot, :kr], preferred_element_type=F32)

                @pl.when(typ == END)
                def _():
                    pout[slot] = jnp.dot(act[slot, :, :ke], wb[wslot, :ke], preferred_element_type=F32)

                finish(btyp, bk, bi, 1 - slot)
                pl.when(typ == OWN)(lambda: p_out(pown, k, i, slot).start())
                outside = (k == LAST) & last
                inside = jnp.logical_not(outside)
                pl.when((typ == REM) & inside)(lambda: p_out(psend, k, i, slot).start())
                pl.when((typ == REM) & outside)(lambda: last_out(xlast, slot).start())

                @pl.when((typ == END) & outside)
                def _():
                    pout[slot] = pback[slot] + pout[slot]
                    last_out(olast, slot).start()

                @pl.when((typ == END) & inside)
                def _():
                    @pl.when(k == LAST)
                    def _():
                        p_x(i, k).wait_recv()
                        p_in(i, k, slot).start()

                    p_in(i, k, slot).wait()
                    total = (pback[slot] + pout[slot]) + pin[slot]
                    yout[...] = (xin[slot].astype(F32) + total).astype(BF16)
                    y_out(k, i).start()

                return typ, k, i

            ptyp, pk, _ = lax.fori_loop(0, 4, tile, (ptyp, pk, jnp.int32(3)))
            return ntyp, nk, ptyp, pk

        _, _, ptyp, pk = lax.fori_loop(lo, hi, visit, (typ0, k0, jnp.int32(3), jnp.int32(0)))
        finish(ptyp, pk, jnp.int32(3), 1)

    def junction():
        final = len(tail) - 1

        def lanes(t):
            at = 0 if t < 2 else 2 * sum(w for _, w in tail[1:t])
            return (0 if t == 0 else d), at

        def w_tail(t, part):
            refs = ((w1, w1so), (w1far, w1sf))[part]
            r, at = lanes(t)
            w = tail[t][1]
            return [
                pltpu.make_async_copy(
                    refs[q].at[cols_t(t)],
                    wb.at[0, r + part * half : r + (part + 1) * half, at + q * w : at + (q + 1) * w],
                    tail_sem.at[t, part, q],
                )
                for q in BOTH
            ]

        def xn_in(i):
            return pltpu.make_async_copy(xn.at[hrows(4 + i)], act.at[1, :, :d], act_sem.at[1, 0])

        def h_at(i, q, col, width):
            return h.at[hrows(4 + i), q * fr + col : q * fr + col + width]

        def h_in(i):
            return [
                pltpu.make_async_copy(h_at(i, q, 0, t0), act.at[0, :, q * fr : q * fr + t0], act_sem.at[0, q])
                for q in BOTH
            ]

        def first_sum(block):
            return remote(pout.at[0, block], precv.at[block, :c2], p_s.at[0], p_r.at[0], to_x)

        def hidden(t, block=everything):
            r, at = lanes(t)
            u = jnp.dot(act[1, block, :d], wb[0, r : r + d, at : at + 2 * tail[t][1]], preferred_element_type=F32)
            return jax.nn.gelu(u, approximate=True).astype(BF16)

        def arrive(t):
            w1_yt(t).wait_recv()
            w1_ft(t).start()
            w_tail(t, 1)[0].start()
            if t == final:
                w1_y(N1 - 1).start()
                w1_e().wait_recv()
                w1_ye().start()
                w2_yf(0).start()
                w2_yf(1).start()
                w2_e().wait_recv()
            w1_ft(t).wait_recv()
            w_tail(t, 1)[1].start()
            if t == final:
                w1_ce().start()
                w2_ce().start()
            for part in BOTH:
                for c in w_tail(t, part):
                    c.wait()

        w1_c(NR - 1).wait_recv()
        for t in range(len(tail)):
            for c in w_tail(t, 0):
                c.start()
        xn_in(0).start()
        for c in h_in(0):
            c.start()
        w2_c(0).wait_recv()
        rem, zero = jnp.int32(REM), jnp.int32(0)
        w2_in(rem, zero, 1, True)
        arrive(0)
        w2_in(rem, zero, 1, False)

        def tile_(i, carry):
            xn_in(i).wait()
            out = []
            for t in range(final):
                if t > 0:
                    pl.when(i == 0)(lambda t=t: arrive(t))
                g = hidden(t)
                if t == 0:
                    for c in h_in(i):
                        c.wait()
                off, w = tail[t]
                for q in BOTH:
                    at = q * fr + t0 + off
                    act[0, :, at : at + w] = g[:, q * w : (q + 1) * w]
                    out.append(
                        pltpu.make_async_copy(act.at[0, :, at : at + w], h_at(i, q, t0 + off, w), h_sem.at[t, q])
                    )
                    out[-1].start()
            off, w = tail[final]
            n = fr - w
            slot = _where(i == 0, 0, 1)
            pout[slot] = jnp.dot(act[0, :, :n], wb[1, :n], preferred_element_type=F32) + jnp.dot(
                act[0, :, fr : fr + n], wb[1, fr : fr + n], preferred_element_type=F32
            )
            for c in out:
                c.wait()

            @pl.when(i < 3)
            def _():
                for c in h_in(i + 1):
                    c.start()

            pl.when(i == 0)(lambda: arrive(final))
            block = sub // 2

            @pl.loop(0, 2)
            def _(m):
                at = pl.ds(pl.multiple_of(m * block, block), block)
                g = hidden(final, at)
                hout[0, at, :2 * w] = g
                pout[slot, at] += jnp.dot(g[:, :w], wb[1, n:fr], preferred_element_type=F32) + jnp.dot(
                    g[:, w : 2 * w], wb[1, fr + n : kr], preferred_element_type=F32
                )
                pl.when(i == 0)(lambda: first_sum(at).start())

            pl.when(i < 3)(lambda: xn_in(i + 1).start())
            out = []
            for q in BOTH:
                out.append(
                    pltpu.make_async_copy(
                        hout.at[0, :sub, q * w : (q + 1) * w], h_at(i, q, t0 + off, w), h_sem.at[2, q]
                    )
                )
                out[-1].start()

            @pl.when(i > 0)
            def _():
                sent = p_out(psend, zero, i, 1)
                sent.start()
                sent.wait()
                p_x(i, 0).start()

            for c in out:
                c.wait()
            return carry

        lax.fori_loop(0, 4, tile_, jnp.int32(0))
        p_x(0, 0).wait_send()

    @pl.loop(0, 2)
    def _(phase):
        early = phase == 0
        cut = starts1[BREAK1]
        first_product(_where(early, 0, cut), _where(early, cut, total1))
        pl.when(early)(junction)
        second_product(_where(early, 0, BREAK2), _where(early, BREAK2, len(VISITS)))

    @pl.loop(0, N1 + 1)
    def _(j):
        w1_cr(j).wait_send()

    @pl.loop(0, N1 + 1)
    def _(j):
        @pl.when(j != NR - 1)
        def _():
            w1_yr(j).wait_send()
            w1_f(j).wait_send()

    for t in range(len(tail)):
        w1_yt(t).wait_send()
        w1_ft(t).wait_send()

    @pl.loop(0, N2)
    def _(k):
        w2_yf(k).wait_send()
        w2_c(k).wait_send()
        w2_ff(k).wait_send()

    w1_e().wait_send()
    w2_e().wait_send()
    w2_ce().wait_send()
    for g in range(len(PARTS_G)):
        for c in w2_yg(g):
            c.wait_send()
        w2_fg(g).wait_send()

    @pl.loop(0, NX)
    def _(t):
        xn_x(t).wait_send()

    @pl.loop(1, 2 * N2 * 4 - 1)
    def _(s):
        p_x(s % 4, s // 4).wait_send()


PUTS = 16


def _put(src, dst, buf, sems_in, sems_out):
    n = src.shape[0] // PUTS

    def get(i):
        return pltpu.make_async_copy(src.at[i * n : (i + 1) * n], buf.at[i], sems_in.at[i])

    def put(i):
        return pltpu.make_async_copy(buf.at[i], dst.at[i * n : (i + 1) * n], sems_out.at[i])

    for i in range(PUTS):
        get(i).start()
    for i in range(PUTS):
        get(i).wait()
        put(i).start()
    for i in range(PUTS):
        put(i).wait()


def solution(mesh):
    def body(x, gamma, w1, w2):
        rows, d = x.shape
        half, fq = w1.shape
        sub = rows // 4
        c1, c2 = fq // N1, half // N2

        def hbm(*shape, dtype=BF16):
            return jax.ShapeDtypeStruct(shape, dtype)

        dma = pltpu.SemaphoreType.DMA
        outs = (
            hbm(rows, d),
            hbm(sub, c2, dtype=F32),
            hbm(sub, c2, dtype=F32),
            hbm(2 * rows, d),
            hbm(half, c1), hbm(half, fq + c1), hbm(half, fq + c1), hbm(half, fq + c1),
            hbm(c1, half), hbm(fq + c1, half), hbm(fq + c1, half), hbm(fq + c1, half),
            hbm(2 * rows, 2 * (fq + c1)),
            hbm(rows, d, dtype=F32), hbm(rows, d, dtype=F32), hbm(rows, d, dtype=F32),
        )
        sent = (NX, 2, N1 + 3, N1 + 1, N1 + 3, 3 * N2, N2 + 1, 2 * N2, 8 * N2)
        out = pl.pallas_call(
            _kernel,
            name="mlp",
            out_shape=outs,
            in_specs=[pl.BlockSpec(memory_space=pl.ANY)] * 4,
            out_specs=tuple([pl.BlockSpec(memory_space=pl.ANY)] * len(outs)),
            scratch_shapes=[
                pltpu.VMEM((2, sub, 2 * d), BF16),
                pltpu.VMEM((2, 2 * fq, c2), BF16),
                pltpu.VMEM((2, 2 * sub, c1), BF16),
                pltpu.VMEM((2, sub, c2), F32),
                pltpu.VMEM((2, sub, c2), F32),
                pltpu.VMEM((2, sub, c2), F32),
                pltpu.VMEM((2, sub, c2), BF16),
                pltpu.VMEM((sub, c2), BF16),
                pltpu.VMEM((1, d), F32),
                *(dma(n) for n in ((2, 2), (2, 4), (3, 2), (3,), (3,), (2, 3), (2, 2, 2))),
                *(dma((n,)) for n in sent for _ in BOTH),
            ],
            compiler_params=pltpu.CompilerParams(
                collective_id=0, has_side_effects=True, vmem_limit_bytes=67_000_000
            ),
        )(x, gamma.reshape(1, d), w1, w2)
        got = lax.ppermute(out[1], "tp", [(i, (i + 2) % 4) for i in range(4)])
        y = pl.pallas_call(
            _put,
            name="put",
            out_shape=hbm(rows, d),
            in_specs=[pl.BlockSpec(memory_space=pl.ANY)],
            out_specs=pl.BlockSpec(memory_space=pl.ANY),
            scratch_shapes=[pltpu.VMEM((PUTS, rows // PUTS, d), BF16), dma((PUTS,)), dma((PUTS,))],
            compiler_params=pltpu.CompilerParams(vmem_limit_bytes=40_000_000),
            cost_estimate=pl.CostEstimate(flops=30_000_000_000, bytes_accessed=4 * rows * d, transcendentals=0),
        )(out[0])
        at = (3 * sub, (1 - lax.axis_index("fsdp")) * half + (N2 - 1) * c2)
        tile = lax.dynamic_slice(x, at, (sub, c2)).astype(F32) + (out[2] + got)
        return lax.dynamic_update_slice(y, tile.astype(BF16), at)

    return jax.shard_map(
        body,
        mesh=mesh,
        in_specs=(P(("fsdp", "tp"), None), P(None), P("fsdp", "tp"), P("tp", "fsdp")),
        out_specs=P(("fsdp", "tp"), None),
        check_vma=False,
    )
```

```python
import jax
import jax.numpy as jnp
from jax import lax
from jax.experimental import pallas as pl
from jax.experimental.pallas import tpu as pltpu
from jax.sharding import PartitionSpec as P

EPS = 1e-6
F32 = jnp.float32
BF16 = jnp.bfloat16
MESH = pl.DeviceIdType.MESH

N1 = 12
NR = N1 - 1
NT = NR - 1
N2 = 6
NX = 8
BOTH = range(2)
AHEAD = 3

STEPS1 = (
    ((0, 4), (0, 2)),
    ((0, 4), (2, 1)),
    ((4, 2), (0, 3)),
    ((0, 3), (4, 1)),
    ((6, 1), (0, 3)),
    ((3, 4), (4, 1)),
    ((7, 1), (2, 1)),
    ((7, 1), (4, 1)),
    ((0, 8), (5, 1)),
    ((8, 2), (2, 2)),
    ((7, 7), (0, 2)),
)
BREAK1 = 10

REM, OWN, END = 0, 1, 2
LAST = 2 * N2 - 1
R, A, B = ((lambda k, t=t: (t, k)) for t in (REM, OWN, END))
VISITS = (
    *map(R, range(1, 6)),
    A(0), A(1), R(6), A(2), B(0), B(1), A(3), R(7), B(2), A(4), A(5), R(8), B(3), A(6), A(7), B(4), B(5),
    R(9), A(8), B(6), A(9), B(7), R(10), B(8), A(10), R(11), A(11), B(9), B(10), B(11),
)
BREAK2 = 4
PASS_F = {A(1): 0, B(1): 1, A(5): 2, B(5): 3, B(7): 4, R(11): 5}
PASS_G = {B(4): 0, A(11): 1, B(9): 2, B(10): 3}
SEND_F = {R(2): (2,), R(5): (3, 4), R(7): (5,)}
SEND_G = {R(2): (0,), R(7): (1, 2, 3)}
PARTS_G = ((0, 3), (3, 1), (4, 1), (5, 1))


def _tail(c1):
    w = c1 // 2
    return ((0, w), (w, w // 2))


def _where(cond, a, b):
    return jnp.where(cond, jnp.int32(a), jnp.int32(b))


def _bounds1():
    at, out = 0, []
    for (_, nj), (_, nt) in STEPS1:
        out.append(at)
        at += nj * 2 * nt
    return out, at


def _step1(s):
    starts, _ = _bounds1()
    rows = [(at, j0, nt, t0) for at, ((j0, _), (t0, nt)) in zip(starts, STEPS1)]
    start, j0, nt, t0 = (jnp.int32(v) for v in rows[0])
    for row in rows[1:]:
        late = s >= row[0]
        start, j0, nt, t0 = (_where(late, new, old) for new, old in zip(row, (start, j0, nt, t0)))
    u = s - start
    pair = u // nt
    return j0 + pair // 2, pair % 2, t0 + u % nt


def _first_tile(j):
    return _where((j >= 7) & (j < NT), 2, 0)


def _visit(v):
    code = jnp.int32(0)
    for n, (t, k) in enumerate(VISITS):
        code = _where(v == n, t * 16 + k, code)
    return code // 16, code % 16


def _kernel(
    x, gamma, w1, w2,
    y, xlast, olast, xn, w1e, w1far, w1so, w1sf, w2e, w2far, w2so, w2sf, h, psend, pown, precv,
    act, wb, hout, pout, pin, pback, xin, yout, gam,
    act_sem, w_sem, h_sem, io_sem, out_sem, in_sem, tail_sem,
    xn_s, xn_r, e_s, e_r, w1y_s, w1y_r, w1c_s, w1c_r, w1f_s, w1f_r,
    w2y_s, w2y_r, w2c_s, w2c_r, w2f_s, w2f_r, p_s, p_r,
):
    a = lax.axis_index("fsdp")
    b = lax.axis_index("tp")
    to_y = {"fsdp": 1 - a}
    to_x = {"tp": lax.rem(b + 2, 4)}
    to_c = {"tp": b + 1 - 2 * lax.rem(b, 2)}
    rows, d = x.shape
    half, fq = w1.shape
    sub = rows // 4
    c1 = fq // N1
    c2 = half // N2
    tail = _tail(c1)
    t0 = NT * c1
    fr = t0 + sum(w for _, w in tail)
    ce = fq - fr
    kr = 2 * fr
    ke = 4 * ce
    piece = rows // NX
    near = pl.multiple_of(a * half, half)
    away = pl.multiple_of((1 - a) * half, half)
    everything = slice(None)

    def remote(src, dst, ssem, rsem, to):
        return pltpu.make_async_remote_copy(
            src_ref=src, dst_ref=dst, send_sem=ssem, recv_sem=rsem, device_id=to, device_id_type=MESH
        )

    def cols1(j):
        return (everything, pl.ds(pl.multiple_of(j * c1, c1), c1))

    def cols2(k):
        return pl.ds(pl.multiple_of(k * c2, c2), c2)

    own_e = (everything, pl.ds(fr, ce))
    ext_e = (everything, pl.ds(fq, ce))

    def w1_y(j):
        return remote(w1.at[cols1(j)], w1far.at[cols1(j)], w1y_s.at[j], w1y_r.at[j], to_y)

    def w1_yo():
        return remote(w1.at[own_e], w1far.at[own_e], w1y_s.at[NR], w1y_r.at[NR], to_y)

    def w1_ye():
        return remote(w1e.at[:, :ce], w1far.at[ext_e], w1y_s.at[N1], w1y_r.at[N1], to_y)

    def w1_c(j):
        return remote(w1.at[cols1(j)], w1so.at[cols1(j)], w1c_s.at[j], w1c_r.at[j], to_c)

    def w1_ce():
        return remote(w1e.at[:, :ce], w1so.at[ext_e], w1c_s.at[N1], w1c_r.at[N1], to_c)

    def w1_f(j):
        return remote(w1far.at[cols1(j)], w1sf.at[cols1(j)], w1f_s.at[j], w1f_r.at[j], to_c)

    def w1_fo():
        return remote(w1far.at[own_e], w1sf.at[own_e], w1f_s.at[NR], w1f_r.at[NR], to_c)

    def w1_fe():
        return remote(w1far.at[ext_e], w1sf.at[ext_e], w1f_s.at[N1], w1f_r.at[N1], to_c)

    def cols_t(t):
        return (everything, pl.ds(t0 + tail[t][0], tail[t][1]))

    def tail_at(t):
        return NT if t == 0 else N1 + t

    def w1_yt(t):
        return remote(w1.at[cols_t(t)], w1far.at[cols_t(t)], w1y_s.at[tail_at(t)], w1y_r.at[tail_at(t)], to_y)

    def w1_ft(t):
        return remote(w1far.at[cols_t(t)], w1sf.at[cols_t(t)], w1f_s.at[tail_at(t)], w1f_r.at[tail_at(t)], to_c)

    def w1_e():
        return remote(w1.at[own_e], w1e.at[:, :ce], e_s.at[0], e_r.at[0], to_x)

    def w2_e():
        return remote(w2.at[fr:fq], w2e, e_s.at[1], e_r.at[1], to_x)

    def w2_yf(k):
        at = (pl.ds(0, fr), cols2(k))
        return remote(w2.at[at], w2far.at[at], w2y_s.at[k], w2y_r.at[k], to_y)

    def cols_g(g):
        k, n = PARTS_G[g]
        return pl.ds(k * c2, n * c2)

    def w2_yg(g):
        at, to, n = (pl.ds(fr, ce), cols_g(g)), (pl.ds(fq, ce), cols_g(g)), N2 + g + g
        return (
            remote(w2.at[at], w2far.at[at], w2y_s.at[n], w2y_r.at[n], to_y),
            remote(w2e.at[:, cols_g(g)], w2far.at[to], w2y_s.at[n + 1], w2y_r.at[n + 1], to_y),
        )

    def w2_c(k):
        at = (everything, cols2(k))
        return remote(w2.at[at], w2so.at[pl.ds(0, fq), cols2(k)], w2c_s.at[k], w2c_r.at[k], to_c)

    def w2_ce():
        return remote(w2e, w2so.at[fq : fq + ce], w2c_s.at[N2], w2c_r.at[N2], to_c)

    def w2_ff(k):
        at = (pl.ds(0, fr), cols2(k))
        return remote(w2far.at[at], w2sf.at[at], w2f_s.at[k], w2f_r.at[k], to_c)

    def w2_fg(g):
        at = (pl.ds(fr, 2 * ce), cols_g(g))
        return remote(w2far.at[at], w2sf.at[at], w2f_s.at[N2 + g], w2f_r.at[N2 + g], to_c)

    def xrows(t):
        return pl.ds(pl.multiple_of(t * piece, piece), piece)

    def xn_x(t):
        return remote(xn.at[xrows(t)], xn.at[xrows(t + NX)], xn_s.at[t], xn_r.at[t], to_x)

    def p_x(i, k):
        at = (pl.ds(pl.multiple_of(i * sub, sub), sub), cols2(k))
        return remote(psend.at[at], precv.at[at], p_s.at[k * 4 + i], p_r.at[k * 4 + i], to_x)

    barrier = pltpu.get_barrier_semaphore()
    for to in (to_y, to_x, to_c):
        pl.semaphore_signal(barrier, inc=1, device_id=to, device_id_type=MESH)
    pl.semaphore_wait(barrier, 3)

    for j in range(AHEAD):
        w1_y(j).start()

    @pl.loop(0, N1)
    def _(j):
        w1_c(j).start()

    def gam_in():
        return [
            pltpu.make_async_copy(gamma.at[:, pl.ds(off, half)], gam.at[:, i * half : (i + 1) * half], io_sem.at[i])
            for i, off in enumerate((near, away))
        ]

    def x_in(t, slot):
        return [
            pltpu.make_async_copy(
                x.at[xrows(t), pl.ds(off, half)],
                act.at[slot, :piece, i * half : (i + 1) * half],
                act_sem.at[slot, i],
            )
            for i, off in enumerate((near, away))
        ]

    for c in gam_in():
        c.start()
    for c in x_in(0, 0):
        c.start()
    for c in gam_in():
        c.wait()

    @pl.loop(0, NX)
    def _(t):
        slot = t % 2

        @pl.when(t + 1 < NX)
        def _():
            for c in x_in(t + 1, 1 - slot):
                c.start()

        for c in x_in(t, slot):
            c.wait()

        @pl.loop(0, piece // 16)
        def _(r):
            at = pl.multiple_of(r * 16, 16)
            xs = act[slot, pl.ds(at, 16), :d].astype(F32)
            xc = xs - jnp.mean(xs, axis=1, keepdims=True)
            var = jnp.mean(xc * xc, axis=1, keepdims=True)
            act[slot, pl.ds(piece + at, 16), :d] = (xc * lax.rsqrt(var + EPS) * gam[...]).astype(BF16)

        out = pltpu.make_async_copy(act.at[slot, piece : 2 * piece, :d], xn.at[xrows(t)], io_sem.at[2])
        out.start()
        out.wait()

        @pl.when(t < NX // 2)
        def _():
            xn_x(t).start()

    def tile_rows(m):
        return _where(m < 4, 2 * m, 2 + m), m < 4

    def hrows(r):
        return pl.ds(pl.multiple_of(r * sub, sub), sub)

    def a1_in(m, slot, go):
        r0, two = tile_rows(m)

        def one(i):
            c = pltpu.make_async_copy(
                xn.at[hrows(r0 + i)], act.at[slot, :, i * d : (i + 1) * d], act_sem.at[slot, i]
            )
            c.start() if go else c.wait()

        one(0)
        pl.when(two)(lambda: one(1))

    def w1_in(j, q, slot, go):
        def load(i, ref, at):
            c = pltpu.make_async_copy(ref.at[at], wb.at[slot, i * half : (i + 1) * half], w_sem.at[slot, i])
            c.start() if go else c.wait()

        if not go:
            for i in BOTH:
                load(i, w1far, cols1(j))
            return
        pl.when((q == 0) & (j < N1))(lambda: load(0, w1, cols1(j)))
        pl.when((q == 0) & (j >= N1))(lambda: load(0, w1e, cols1(j - N1)))
        pl.when(q == 0)(lambda: load(1, w1far, cols1(j)))

        @pl.when(q == 1)
        def _():
            load(0, w1so, cols1(j))
            load(1, w1sf, cols1(j))

    starts1, total1 = _bounds1()
    first2, first3, first4 = (
        next(at for at, (_, (m0, nm)) in zip(starts1, STEPS1) if m0 == m) for m in (2, 4, 5)
    )

    def arrive1(s):
        j, q, m = _step1(s)
        first = (m == _first_tile(j)) & (j < NT)

        @pl.when((m == 0) & (q == 0))
        def _():
            pl.when(j == NT)(lambda: (w1_yo().wait_recv(), w1_fo().start()) and None)
            pl.when(j == N1)(lambda: (w1_ye().wait_recv(), w1_fe().start()) and None)

        @pl.when((m == 0) & (q == 1))
        def _():
            pl.when(j == NT)(lambda: w1_fo().wait_recv())
            pl.when(j == NR)(lambda: w1_c(j).wait_recv())
            pl.when(j == N1)(lambda: (w1_ce().wait_recv(), w1_fe().wait_recv()) and None)

        @pl.when(first & (q == 0))
        def _():
            w1_y(j).wait_recv()
            w1_f(j).start()

            @pl.when(j + AHEAD < NT)
            def _():
                w1_y(j + AHEAD).start()

            @pl.when(j + AHEAD == NT)
            def _():
                for t in range(len(tail)):
                    w1_yt(t).start()
                w1_e().start()
                w2_e().start()

            @pl.when(j == 2)
            def _():
                for t in range(NX // 2, NX):
                    xn_x(t).start()

            @pl.when(j == 4)
            def _():
                for k in range(N2):
                    w2_c(k).start()

        @pl.when(first & (q == 1))
        def _():
            w1_c(j).wait_recv()
            w1_f(j).wait_recv()

        for at, lo, hi in ((first2, 0, 4), (first3, 4, 6), (first4, 6, 8)):

            @pl.when(s == at)
            def _():
                for t in range(lo, hi):
                    xn_x(t).wait_recv()

    def load1(s, aslot, wslot, a_new, w_new):
        j, q, m = _step1(s)
        pl.when(a_new)(lambda: a1_in(m, aslot, True))
        pl.when(w_new)(lambda: w1_in(j, q, wslot, True))

    def h_out(s, i, go):
        j, q, m = _step1(s)
        r0, _ = tile_rows(m)
        slot = s % 2
        full = fr - t0

        def part(at, w, col, sem):
            c = pltpu.make_async_copy(
                hout.at[slot, pl.ds(pl.multiple_of(i * sub, sub), sub), at : at + w],
                h.at[hrows(r0 + i), pl.ds(pl.multiple_of(col, c1 - full), w)],
                h_sem.at[sem, i],
            )
            c.start() if go else c.wait()

        own, ext = kr + q * ce, kr + (2 + q) * ce
        pl.when(j < NT)(lambda: part(0, c1, q * fr + j * c1, slot))

        @pl.when(j == NT)
        def _():
            part(0, full, q * fr + t0, slot)
            part(full, c1 - full, own, 2 + slot)

        pl.when(j == NR)(lambda: part(0, c1, own + c1 - full, slot))
        pl.when(j == N1)(lambda: part(0, c1, ext, slot))
        pl.when(j > N1)(lambda: part(0, ce - c1, ext + c1, slot))

    def h_done(s):
        _, two = tile_rows(_step1(s)[2])
        h_out(s, 0, False)
        pl.when(two)(lambda: h_out(s, 1, False))

    def first_product(lo, hi):
        arrive1(lo)
        load1(lo, 0, 0, True, True)

        def step(s, carry):
            aslot, wslot, a_fresh, w_fresh = carry
            j, q, m = _step1(s)
            nj, nq, nm = _step1(s + 1)
            more = s + 1 < hi
            a_new = more & (nm != m)
            w_new = more & ((nj != j) | (nq != q))
            na = _where(a_new, 1 - aslot, aslot)
            nw = _where(w_new, 1 - wslot, wslot)
            pl.when(more)(lambda: arrive1(s + 1))
            load1(s + 1, na, nw, a_new, w_new)
            pl.when(a_fresh == 1)(lambda: a1_in(m, aslot, False))
            pl.when(w_fresh == 1)(lambda: w1_in(j, q, wslot, False))
            pl.when(s >= lo + 2)(lambda: h_done(s - 2))
            _, two = tile_rows(m)

            @pl.loop(0, _where(two, 2, 1))
            def _(i):
                u = jnp.dot(
                    act[aslot, :, pl.ds(pl.multiple_of(i * d, d), d)], wb[wslot, :d], preferred_element_type=F32
                )
                hout[s % 2, pl.ds(pl.multiple_of(i * sub, sub), sub)] = jax.nn.gelu(u, approximate=True).astype(BF16)
                h_out(s, i, True)

            return na, nw, _where(a_new, 1, 0), _where(w_new, 1, 0)

        one, nil = jnp.int32(1), jnp.int32(0)
        lax.fori_loop(lo, hi, step, (nil, nil, one, one))
        h_done(hi - 2)
        h_done(hi - 1)

    def p_in(i, k, slot):
        return pltpu.make_async_copy(precv.at[hrows(i), cols2(k)], pin.at[slot], in_sem.at[slot, 2])

    def a2_in(typ, k, i, slot, go):
        r = _where(typ == REM, 4, 0) + i

        def wait_or_start(c):
            c.start() if go else c.wait()

        @pl.when(typ != END)
        def _():
            wait_or_start(pltpu.make_async_copy(h.at[hrows(r), :kr], act.at[slot, :, :kr], act_sem.at[slot, 0]))

        @pl.when(typ == END)
        def _():
            wait_or_start(
                pltpu.make_async_copy(h.at[hrows(r), kr : kr + ke], act.at[slot, :, :ke], act_sem.at[slot, 0])
            )
            ycol = pl.multiple_of(_where(k < N2, near, away) + (k % N2) * c2, c2)
            wait_or_start(pltpu.make_async_copy(pown.at[hrows(i), cols2(k)], pback.at[slot], in_sem.at[slot, 0]))
            wait_or_start(pltpu.make_async_copy(x.at[hrows(i), pl.ds(ycol, c2)], xin.at[slot], in_sem.at[slot, 1]))
            if go:

                @pl.when(k < LAST)
                def _():
                    p_x(i, k).wait_recv()
                    p_in(i, k, slot).start()

    def w2_in(typ, k, slot, go):
        def load(n, at, rows_, ref, from_, kk):
            c = pltpu.make_async_copy(
                ref.at[pl.ds(from_, rows_), cols2(kk)], wb.at[slot, at : at + rows_], w_sem.at[slot, n]
            )
            c.start() if go else c.wait()

        def main(own, sib, kk):
            load(0, 0, fr, own, 0, kk)
            load(1, fr, fr, sib, 0, kk)

        def rest(own, ext, ext_at, sib, kk):
            for n, (ref, from_) in enumerate(((own, fr), (sib, fr), (ext, ext_at), (sib, fq))):
                load(n, n * ce, ce, ref, from_, kk)

        def both(side, kk, own, ext, ext_at, sib):
            pl.when(side & (typ != END))(lambda: main(own, sib, kk))
            pl.when(side & (typ == END))(lambda: rest(own, ext, ext_at, sib, kk))

        if not go:
            pl.when(typ != END)(lambda: main(w2far, w2sf, 0))
            pl.when(typ == END)(lambda: rest(w2far, w2far, fq, w2sf, 0))
            return
        both(k < N2, k, w2, w2e, 0, w2so)
        both(k >= N2, k - N2, w2far, w2far, fq, w2sf)

    def arrive2(v):
        at = {visit: n for n, visit in enumerate(VISITS)}
        for n in range(len(VISITS)):
            visit = VISITS[n]
            todo = []
            for u in SEND_F.get(visit, ()):
                todo.append(lambda u=u: w2_yf(u).start())
            for g in SEND_G.get(visit, ()):
                todo.append(lambda g=g: [c.start() for c in w2_yg(g)])
            if visit in PASS_F:
                u = PASS_F[visit]
                todo.append(lambda u=u: (w2_yf(u).wait_recv(), w2_ff(u).start()))
            if visit in PASS_G:
                g = PASS_G[visit]
                todo.append(lambda g=g: ([c.wait_recv() for c in w2_yg(g)], w2_fg(g).start()))
            if visit[0] == REM:
                k = visit[1]
                todo.append(lambda k=k: w2_c(k).wait_recv() if k < N2 else w2_ff(k - N2).wait_recv())
            if n == min(at[B(k)] for k in range(N2)):
                todo.append(lambda: w2_ce().wait_recv())
            for g, (k0, nk) in enumerate(PARTS_G):
                if n == min(at[B(N2 + k)] for k in range(k0, k0 + nk)):
                    todo.append(lambda g=g: w2_fg(g).wait_recv())
            if todo:

                @pl.when(v == n)
                def _(todo=todo):
                    for f in todo:
                        f()

    def p_out(to, k, i, slot):
        return pltpu.make_async_copy(pout.at[slot], to.at[hrows(i), cols2(k)], out_sem.at[slot])

    def y_out(k, i):
        ycol = pl.multiple_of(_where(k < N2, near, away) + (k % N2) * c2, c2)
        return pltpu.make_async_copy(yout, y.at[hrows(i), pl.ds(ycol, c2)], out_sem.at[2])

    def last_out(to, slot):
        return pltpu.make_async_copy(pout.at[slot], to, out_sem.at[slot])

    def finish(typ, k, i, slot):
        outside = (k == LAST) & (i >= 2)

        @pl.when((typ == REM) | (typ == OWN) | ((typ == END) & outside))
        def _():
            p_out(pown, k, i, slot).wait()

        @pl.when((typ == REM) & ((k < LAST) | (i < 3)))
        def _():
            p_x(i, k).start()

        @pl.when((typ == END) & jnp.logical_not(outside))
        def _():
            y_out(k, i).wait()

    def second_product(lo, hi):
        arrive2(lo)
        typ0, k0 = _visit(lo)
        w2_in(typ0, k0, 0, True)
        a2_in(typ0, k0, jnp.int32(0), 0, True)

        def visit(v, carry):
            typ, k, ptyp, pk = carry
            more = v + 1 < hi
            ntyp, nk = _visit(v + 1)
            wslot = (v - lo) % 2

            def tile(i, before):
                btyp, bk, bi = before
                slot = i % 2
                last = i == 3

                @pl.when(last & more)
                def _():
                    arrive2(v + 1)
                    w2_in(ntyp, nk, 1 - wslot, True)

                @pl.when(more | (i < 3))
                def _():
                    a2_in(_where(last, ntyp, typ), _where(last, nk, k), _where(last, 0, i + 1), 1 - slot, True)

                a2_in(typ, k, i, slot, False)
                pl.when(i == 0)(lambda: w2_in(typ, k, wslot, False))

                @pl.when(typ != END)
                def _():
                    pout[slot] = jnp.dot(act[slot, :, :kr], wb[wslot, :kr], preferred_element_type=F32)

                @pl.when(typ == END)
                def _():
                    pout[slot] = jnp.dot(act[slot, :, :ke], wb[wslot, :ke], preferred_element_type=F32)

                finish(btyp, bk, bi, 1 - slot)
                pl.when(typ == OWN)(lambda: p_out(pown, k, i, slot).start())
                outside = (k == LAST) & (i >= 2)
                inside = jnp.logical_not(outside)
                final = (k == LAST) & last
                pl.when((typ == REM) & jnp.logical_not(final))(lambda: p_out(psend, k, i, slot).start())
                pl.when((typ == REM) & final)(lambda: last_out(xlast, slot).start())

                @pl.when((typ == END) & outside)
                def _():
                    pout[slot] = pback[slot] + pout[slot]
                    last_out(olast.at[pl.ds(pl.multiple_of((i - 2) * sub, sub), sub)], slot).start()

                @pl.when((typ == END) & inside)
                def _():
                    @pl.when(k == LAST)
                    def _():
                        p_x(i, k).wait_recv()
                        p_in(i, k, slot).start()

                    p_in(i, k, slot).wait()
                    total = (pback[slot] + pout[slot]) + pin[slot]
                    yout[...] = (xin[slot].astype(F32) + total).astype(BF16)
                    y_out(k, i).start()

                return typ, k, i

            ptyp, pk, _ = lax.fori_loop(0, 4, tile, (ptyp, pk, jnp.int32(3)))
            return ntyp, nk, ptyp, pk

        _, _, ptyp, pk = lax.fori_loop(lo, hi, visit, (typ0, k0, jnp.int32(3), jnp.int32(0)))
        finish(ptyp, pk, jnp.int32(3), 1)

    def junction():
        final = len(tail) - 1

        def lanes(t):
            at = 0 if t < 2 else 2 * sum(w for _, w in tail[1:t])
            return (0 if t == 0 else d), at

        def w_tail(t, part):
            refs = ((w1, w1so), (w1far, w1sf))[part]
            r, at = lanes(t)
            w = tail[t][1]
            return [
                pltpu.make_async_copy(
                    refs[q].at[cols_t(t)],
                    wb.at[0, r + part * half : r + (part + 1) * half, at + q * w : at + (q + 1) * w],
                    tail_sem.at[t, part, q],
                )
                for q in BOTH
            ]

        def xn_in(i):
            return pltpu.make_async_copy(xn.at[hrows(4 + i)], act.at[1, :, :d], act_sem.at[1, 0])

        def h_at(i, q, col, width):
            return h.at[hrows(4 + i), q * fr + col : q * fr + col + width]

        def h_in(i):
            return [
                pltpu.make_async_copy(h_at(i, q, 0, t0), act.at[0, :, q * fr : q * fr + t0], act_sem.at[0, q])
                for q in BOTH
            ]

        def first_sum(block):
            return remote(pout.at[0, block], precv.at[block, :c2], p_s.at[0], p_r.at[0], to_x)

        def hidden(t, block=everything):
            r, at = lanes(t)
            u = jnp.dot(act[1, block, :d], wb[0, r : r + d, at : at + 2 * tail[t][1]], preferred_element_type=F32)
            return jax.nn.gelu(u, approximate=True).astype(BF16)

        def arrive(t, meanwhile=lambda: None):
            w1_yt(t).wait_recv()
            w1_ft(t).start()
            w_tail(t, 1)[0].start()
            meanwhile()
            if t == final:
                w1_yo().start()
                w1_e().wait_recv()
                w1_ye().start()
                w2_yf(0).start()
                w2_yf(1).start()
                w2_e().wait_recv()
            w1_ft(t).wait_recv()
            w_tail(t, 1)[1].start()
            if t == final:
                w1_ce().start()
                w2_ce().start()
            for part in BOTH:
                for c in w_tail(t, part):
                    c.wait()

        w1_c(NT).wait_recv()
        for t in range(len(tail)):
            for c in w_tail(t, 0):
                c.start()
        xn_in(0).start()
        rem, zero = jnp.int32(REM), jnp.int32(0)

        def rest():
            for c in h_in(0):
                c.start()
            w2_c(0).wait_recv()
            w2_in(rem, zero, 1, True)

        arrive(0, rest)

        def tile_(i, carry):
            xn_in(i).wait()
            out = []
            for t in range(final):
                if t > 0:
                    pl.when(i == 0)(lambda t=t: arrive(t))
                g = hidden(t)
                if t == 0:
                    for c in h_in(i):
                        c.wait()
                off, w = tail[t]
                for q in BOTH:
                    at = q * fr + t0 + off
                    act[0, :, at : at + w] = g[:, q * w : (q + 1) * w]
                    out.append(
                        pltpu.make_async_copy(act.at[0, :, at : at + w], h_at(i, q, t0 + off, w), h_sem.at[t, q])
                    )
                    out[-1].start()
            pl.when(i == 0)(lambda: w2_in(rem, zero, 1, False))
            off, w = tail[final]
            n = fr - w
            slot = _where(i == 0, 0, 1)
            pout[slot] = jnp.dot(act[0, :, :n], wb[1, :n], preferred_element_type=F32) + jnp.dot(
                act[0, :, fr : fr + n], wb[1, fr : fr + n], preferred_element_type=F32
            )
            for c in out:
                c.wait()

            @pl.when(i < 3)
            def _():
                for c in h_in(i + 1):
                    c.start()

            pl.when(i == 0)(lambda: arrive(final))
            block = sub // 2

            @pl.loop(0, 2)
            def _(m):
                at = pl.ds(pl.multiple_of(m * block, block), block)
                g = hidden(final, at)
                hout[0, at, :2 * w] = g
                pout[slot, at] += jnp.dot(g[:, :w], wb[1, n:fr], preferred_element_type=F32) + jnp.dot(
                    g[:, w : 2 * w], wb[1, fr + n : kr], preferred_element_type=F32
                )
                pl.when(i == 0)(lambda: first_sum(at).start())

            pl.when(i < 3)(lambda: xn_in(i + 1).start())
            out = []
            for q in BOTH:
                out.append(
                    pltpu.make_async_copy(
                        hout.at[0, :sub, q * w : (q + 1) * w], h_at(i, q, t0 + off, w), h_sem.at[2, q]
                    )
                )
                out[-1].start()

            @pl.when(i > 0)
            def _():
                sent = p_out(psend, zero, i, 1)
                sent.start()
                sent.wait()
                p_x(i, 0).start()

            for c in out:
                c.wait()
            return carry

        lax.fori_loop(0, 4, tile_, jnp.int32(0))
        p_x(0, 0).wait_send()

    @pl.loop(0, 2)
    def _(phase):
        early = phase == 0
        cut = starts1[BREAK1]
        first_product(_where(early, 0, cut), _where(early, cut, total1))
        pl.when(early)(junction)
        second_product(_where(early, 0, BREAK2), _where(early, BREAK2, len(VISITS)))

    p_x(2, LAST).wait_recv()

    @pl.loop(0, N1)
    def _(j):
        w1_c(j).wait_send()

    @pl.loop(0, NT)
    def _(j):
        w1_y(j).wait_send()
        w1_f(j).wait_send()

    for c in (w1_yo(), w1_ye(), w1_fo(), w1_fe(), w1_ce()):
        c.wait_send()

    for t in range(len(tail)):
        w1_yt(t).wait_send()
        w1_ft(t).wait_send()

    @pl.loop(0, N2)
    def _(k):
        w2_yf(k).wait_send()
        w2_c(k).wait_send()
        w2_ff(k).wait_send()

    w1_e().wait_send()
    w2_e().wait_send()
    w2_ce().wait_send()
    for g in range(len(PARTS_G)):
        for c in w2_yg(g):
            c.wait_send()
        w2_fg(g).wait_send()

    @pl.loop(0, NX)
    def _(t):
        xn_x(t).wait_send()

    @pl.loop(1, 2 * N2 * 4 - 1)
    def _(s):
        p_x(s % 4, s // 4).wait_send()


PUTS = 16


def _put(src, dst, buf, sems_in, sems_out):
    n = src.shape[0] // PUTS

    def get(i):
        return pltpu.make_async_copy(src.at[i * n : (i + 1) * n], buf.at[i], sems_in.at[i])

    def put(i):
        return pltpu.make_async_copy(buf.at[i], dst.at[i * n : (i + 1) * n], sems_out.at[i])

    for i in range(PUTS):
        get(i).start()
    for i in range(PUTS):
        get(i).wait()
        put(i).start()
    for i in range(PUTS):
        put(i).wait()


def solution(mesh):
    def body(x, gamma, w1, w2):
        rows, d = x.shape
        half, fq = w1.shape
        sub = rows // 4
        c1, c2 = fq // N1, half // N2
        ce = fq - NT * c1 - sum(w for _, w in _tail(c1))

        def hbm(*shape, dtype=BF16):
            return jax.ShapeDtypeStruct(shape, dtype)

        dma = pltpu.SemaphoreType.DMA
        outs = (
            hbm(rows, d),
            hbm(sub, c2, dtype=F32),
            hbm(2 * sub, c2, dtype=F32),
            hbm(2 * rows, d),
            hbm(half, 2 * c1), *[hbm(half, fq + 2 * c1) for _ in range(3)],
            hbm(ce, half), *[hbm(fq + ce, half) for _ in range(3)],
            hbm(2 * rows, 2 * (fq + ce)),
            hbm(rows, d, dtype=F32), hbm(rows, d, dtype=F32), hbm(rows, d, dtype=F32),
        )
        sent = (NX, 2, N1 + 3, N1 + 1, N1 + 3, 3 * N2, N2 + 1, 2 * N2, 8 * N2)
        out = pl.pallas_call(
            _kernel,
            name="mlp",
            out_shape=outs,
            in_specs=[pl.BlockSpec(memory_space=pl.ANY)] * 4,
            out_specs=tuple([pl.BlockSpec(memory_space=pl.ANY)] * len(outs)),
            scratch_shapes=[
                pltpu.VMEM((2, sub, 2 * d), BF16),
                pltpu.VMEM((2, 2 * fq, c2), BF16),
                pltpu.VMEM((2, 2 * sub, c1), BF16),
                pltpu.VMEM((2, sub, c2), F32),
                pltpu.VMEM((2, sub, c2), F32),
                pltpu.VMEM((2, sub, c2), F32),
                pltpu.VMEM((2, sub, c2), BF16),
                pltpu.VMEM((sub, c2), BF16),
                pltpu.VMEM((1, d), F32),
                *(dma(n) for n in ((2, 2), (2, 4), (4, 2), (3,), (3,), (2, 3), (2, 2, 2))),
                *(dma((n,)) for n in sent for _ in BOTH),
            ],
            compiler_params=pltpu.CompilerParams(
                collective_id=0, has_side_effects=True, vmem_limit_bytes=67_000_000
            ),
        )(x, gamma.reshape(1, d), w1, w2)
        got = lax.ppermute(out[1], "tp", [(i, (i + 2) % 4) for i in range(4)])
        y = pl.pallas_call(
            _put,
            name="put",
            out_shape=hbm(rows, d),
            in_specs=[pl.BlockSpec(memory_space=pl.ANY)],
            out_specs=pl.BlockSpec(memory_space=pl.ANY),
            scratch_shapes=[pltpu.VMEM((PUTS, rows // PUTS, d), BF16), dma((PUTS,)), dma((PUTS,))],
            compiler_params=pltpu.CompilerParams(vmem_limit_bytes=40_000_000),
            cost_estimate=pl.CostEstimate(flops=30_000_000_000, bytes_accessed=4 * rows * d, transcendentals=0),
        )(out[0])
        col = (1 - lax.axis_index("fsdp")) * half + (N2 - 1) * c2
        recv = (out[-1][2 * sub : 3 * sub, LAST * c2 :], got)
        for i in BOTH:
            at = ((2 + i) * sub, col)
            total = out[2][i * sub : (i + 1) * sub] + recv[i]
            y = lax.dynamic_update_slice(y, (lax.dynamic_slice(x, at, (sub, c2)).astype(F32) + total).astype(BF16), at)
        return y

    return jax.shard_map(
        body,
        mesh=mesh,
        in_specs=(P(("fsdp", "tp"), None), P(None), P("fsdp", "tp"), P("tp", "fsdp")),
        out_specs=P(("fsdp", "tp"), None),
        check_vma=False,
    )
```

```python
import jax
import jax.numpy as jnp
from jax import lax
from jax.experimental import pallas as pl
from jax.experimental.pallas import tpu as pltpu
from jax.sharding import PartitionSpec as P

EPS = 1e-6
F32 = jnp.float32
BF16 = jnp.bfloat16
MESH = pl.DeviceIdType.MESH

N1 = 12
NR = N1 - 1
NT = NR - 1
N2 = 6
NX = 8
BOTH = range(2)
AHEAD = 3

STEPS1 = (
    ((0, 4), (0, 2)),
    ((0, 4), (2, 1)),
    ((4, 2), (0, 3)),
    ((0, 3), (4, 1)),
    ((6, 1), (0, 3)),
    ((3, 4), (4, 1)),
    ((7, 1), (2, 1)),
    ((7, 1), (4, 1)),
    ((0, 8), (5, 1)),
    ((8, 2), (2, 2)),
    ((7, 7), (0, 2)),
)
BREAK1 = 10

REM, OWN, END = 0, 1, 2
LAST = 2 * N2 - 1
R, A, B = ((lambda k, t=t: (t, k)) for t in (REM, OWN, END))
VISITS = (
    *map(R, range(1, 6)),
    A(0), A(1), R(6), A(2), B(0), B(1), A(3), R(7), B(2), A(4), A(5), R(8), B(3), A(6), A(7), B(4), B(5),
    R(9), A(8), A(9), R(10), A(10), R(11), A(11), *map(B, range(N2, N2 + N2)),
)
BREAK2 = 4
PASS_F = {A(1): 0, B(1): 1, A(5): 2, B(5): 3, A(9): 4, R(11): 5}
PASS_G = {A(11): 0, B(6): 1, B(7): 2, B(9): 3, B(10): 4, B(11): 5}
SEND_F = {R(2): (2,), R(5): (3, 4), R(7): (5,)}
SEND_G = {R(7): range(N2)}


def _tail(c1):
    w = c1 // 2
    return ((0, w), (w, w // 2))


def _where(cond, a, b):
    return jnp.where(cond, jnp.int32(a), jnp.int32(b))


def _bounds1():
    at, out = 0, []
    for (_, nj), (_, nt) in STEPS1:
        out.append(at)
        at += nj * 2 * nt
    return out, at


def _step1(s):
    starts, _ = _bounds1()
    rows = [(at, j0, nt, t0) for at, ((j0, _), (t0, nt)) in zip(starts, STEPS1)]
    start, j0, nt, t0 = (jnp.int32(v) for v in rows[0])
    for row in rows[1:]:
        late = s >= row[0]
        start, j0, nt, t0 = (_where(late, new, old) for new, old in zip(row, (start, j0, nt, t0)))
    u = s - start
    pair = u // nt
    return j0 + pair // 2, pair % 2, t0 + u % nt


def _first_tile(j):
    return _where((j >= 7) & (j < NT), 2, 0)


def _visit(v):
    code = jnp.int32(0)
    for n, (t, k) in enumerate(VISITS):
        code = _where(v == n, t * 16 + k, code)
    return code // 16, code % 16


def _kernel(
    x, gamma, w1, w2,
    y, xlast, olast, xn, w1e, w1far, w1so, w1sf, w2e, w2far, w2so, w2sf, h, psend, pown, precv,
    act, wb, hout, pout, pin, pback, xin, yout, gam,
    act_sem, w_sem, h_sem, io_sem, out_sem, in_sem, tail_sem,
    xn_s, xn_r, e_s, e_r, w1y_s, w1y_r, w1c_s, w1c_r, w1f_s, w1f_r,
    w2y_s, w2y_r, w2c_s, w2c_r, w2f_s, w2f_r, p_s, p_r,
):
    a = lax.axis_index("fsdp")
    b = lax.axis_index("tp")
    to_y = {"fsdp": 1 - a}
    to_x = {"tp": lax.rem(b + 2, 4)}
    to_c = {"tp": b + 1 - 2 * lax.rem(b, 2)}
    rows, d = x.shape
    half, fq = w1.shape
    sub = rows // 4
    c1 = fq // N1
    c2 = half // N2
    tail = _tail(c1)
    t0 = NT * c1
    fr = t0 + sum(w for _, w in tail)
    ce = fq - fr
    kr = 2 * fr
    ke = 4 * ce
    piece = rows // NX
    near = pl.multiple_of(a * half, half)
    away = pl.multiple_of((1 - a) * half, half)
    everything = slice(None)

    def remote(src, dst, ssem, rsem, to):
        return pltpu.make_async_remote_copy(
            src_ref=src, dst_ref=dst, send_sem=ssem, recv_sem=rsem, device_id=to, device_id_type=MESH
        )

    def cols1(j):
        return (everything, pl.ds(pl.multiple_of(j * c1, c1), c1))

    def cols2(k):
        return pl.ds(pl.multiple_of(k * c2, c2), c2)

    own_e = (everything, pl.ds(fr, ce))
    ext_e = (everything, pl.ds(fq, ce))

    def w1_y(j):
        return remote(w1.at[cols1(j)], w1far.at[cols1(j)], w1y_s.at[j], w1y_r.at[j], to_y)

    def w1_yo():
        return remote(w1.at[own_e], w1far.at[own_e], w1y_s.at[NR], w1y_r.at[NR], to_y)

    def w1_ye():
        return remote(w1e.at[:, :ce], w1far.at[ext_e], w1y_s.at[N1], w1y_r.at[N1], to_y)

    def w1_c(j):
        return remote(w1.at[cols1(j)], w1so.at[cols1(j)], w1c_s.at[j], w1c_r.at[j], to_c)

    def w1_ce():
        return remote(w1e.at[:, :ce], w1so.at[ext_e], w1c_s.at[N1], w1c_r.at[N1], to_c)

    def w1_f(j):
        return remote(w1far.at[cols1(j)], w1sf.at[cols1(j)], w1f_s.at[j], w1f_r.at[j], to_c)

    def w1_fo():
        return remote(w1far.at[own_e], w1sf.at[own_e], w1f_s.at[NR], w1f_r.at[NR], to_c)

    def w1_fe():
        return remote(w1far.at[ext_e], w1sf.at[ext_e], w1f_s.at[N1], w1f_r.at[N1], to_c)

    def cols_t(t):
        return (everything, pl.ds(t0 + tail[t][0], tail[t][1]))

    def tail_at(t):
        return NT if t == 0 else N1 + t

    def w1_yt(t):
        return remote(w1.at[cols_t(t)], w1far.at[cols_t(t)], w1y_s.at[tail_at(t)], w1y_r.at[tail_at(t)], to_y)

    def w1_ft(t):
        return remote(w1far.at[cols_t(t)], w1sf.at[cols_t(t)], w1f_s.at[tail_at(t)], w1f_r.at[tail_at(t)], to_c)

    def w1_e():
        return remote(w1.at[own_e], w1e.at[:, :ce], e_s.at[0], e_r.at[0], to_x)

    def w2_e():
        return remote(w2.at[fr:fq], w2e, e_s.at[1], e_r.at[1], to_x)

    def w2_yf(k):
        at = (pl.ds(0, fr), cols2(k))
        return remote(w2.at[at], w2far.at[at], w2y_s.at[k], w2y_r.at[k], to_y)

    def w2_yg(g):
        at, to, n = (pl.ds(fr, ce), cols2(g)), (pl.ds(fq, ce), cols2(g)), N2 + g + g
        return (
            remote(w2.at[at], w2far.at[at], w2y_s.at[n], w2y_r.at[n], to_y),
            remote(w2e.at[:, cols2(g)], w2far.at[to], w2y_s.at[n + 1], w2y_r.at[n + 1], to_y),
        )

    def w2_c(k):
        at = (everything, cols2(k))
        return remote(w2.at[at], w2so.at[pl.ds(0, fq), cols2(k)], w2c_s.at[k], w2c_r.at[k], to_c)

    def w2_ce():
        return remote(w2e, w2so.at[fq : fq + ce], w2c_s.at[N2], w2c_r.at[N2], to_c)

    def w2_ff(k):
        at = (pl.ds(0, fr), cols2(k))
        return remote(w2far.at[at], w2sf.at[at], w2f_s.at[k], w2f_r.at[k], to_c)

    def w2_fg(g):
        at = (pl.ds(fr, 2 * ce), cols2(g))
        return remote(w2far.at[at], w2sf.at[at], w2f_s.at[N2 + g], w2f_r.at[N2 + g], to_c)

    def xrows(t):
        return pl.ds(pl.multiple_of(t * piece, piece), piece)

    def xn_x(t):
        return remote(xn.at[xrows(t)], xn.at[xrows(t + NX)], xn_s.at[t], xn_r.at[t], to_x)

    def p_x(i, k):
        at = (pl.ds(pl.multiple_of(i * sub, sub), sub), cols2(k))
        return remote(psend.at[at], precv.at[at], p_s.at[k * 4 + i], p_r.at[k * 4 + i], to_x)

    barrier = pltpu.get_barrier_semaphore()
    for to in (to_y, to_x, to_c):
        pl.semaphore_signal(barrier, inc=1, device_id=to, device_id_type=MESH)
    pl.semaphore_wait(barrier, 3)

    for j in range(AHEAD):
        w1_y(j).start()

    @pl.loop(0, N1)
    def _(j):
        w1_c(j).start()

    def gam_in():
        return [
            pltpu.make_async_copy(gamma.at[:, pl.ds(off, half)], gam.at[:, i * half : (i + 1) * half], io_sem.at[i])
            for i, off in enumerate((near, away))
        ]

    def x_in(t, slot):
        return [
            pltpu.make_async_copy(
                x.at[xrows(t), pl.ds(off, half)],
                act.at[slot, :piece, i * half : (i + 1) * half],
                act_sem.at[slot, i],
            )
            for i, off in enumerate((near, away))
        ]

    for c in gam_in():
        c.start()
    for c in x_in(0, 0):
        c.start()
    for c in gam_in():
        c.wait()

    @pl.loop(0, NX)
    def _(t):
        slot = t % 2

        @pl.when(t + 1 < NX)
        def _():
            for c in x_in(t + 1, 1 - slot):
                c.start()

        for c in x_in(t, slot):
            c.wait()

        @pl.loop(0, piece // 16)
        def _(r):
            at = pl.multiple_of(r * 16, 16)
            xs = act[slot, pl.ds(at, 16), :d].astype(F32)
            xc = xs - jnp.mean(xs, axis=1, keepdims=True)
            var = jnp.mean(xc * xc, axis=1, keepdims=True)
            act[slot, pl.ds(piece + at, 16), :d] = (xc * lax.rsqrt(var + EPS) * gam[...]).astype(BF16)

        out = pltpu.make_async_copy(act.at[slot, piece : 2 * piece, :d], xn.at[xrows(t)], io_sem.at[2])
        out.start()
        out.wait()

        @pl.when(t < NX // 2)
        def _():
            xn_x(t).start()

    def tile_rows(m):
        return _where(m < 4, 2 * m, 2 + m), m < 4

    def hrows(r):
        return pl.ds(pl.multiple_of(r * sub, sub), sub)

    def a1_in(m, slot, go):
        r0, two = tile_rows(m)

        def one(i):
            c = pltpu.make_async_copy(
                xn.at[hrows(r0 + i)], act.at[slot, :, i * d : (i + 1) * d], act_sem.at[slot, i]
            )
            c.start() if go else c.wait()

        one(0)
        pl.when(two)(lambda: one(1))

    def w1_in(j, q, slot, go):
        def load(i, ref, at):
            c = pltpu.make_async_copy(ref.at[at], wb.at[slot, i * half : (i + 1) * half], w_sem.at[slot, i])
            c.start() if go else c.wait()

        if not go:
            for i in BOTH:
                load(i, w1far, cols1(j))
            return
        pl.when((q == 0) & (j < N1))(lambda: load(0, w1, cols1(j)))
        pl.when((q == 0) & (j >= N1))(lambda: load(0, w1e, cols1(j - N1)))
        pl.when(q == 0)(lambda: load(1, w1far, cols1(j)))

        @pl.when(q == 1)
        def _():
            load(0, w1so, cols1(j))
            load(1, w1sf, cols1(j))

    starts1, total1 = _bounds1()
    first2, first3, first4 = (
        next(at for at, (_, (m0, nm)) in zip(starts1, STEPS1) if m0 == m) for m in (2, 4, 5)
    )

    def arrive1(s):
        j, q, m = _step1(s)
        first = (m == _first_tile(j)) & (j < NT)

        @pl.when((m == 0) & (q == 0))
        def _():
            pl.when(j == NT)(lambda: (w1_yo().wait_recv(), w1_fo().start()) and None)
            pl.when(j == N1)(lambda: (w1_ye().wait_recv(), w1_fe().start()) and None)

        @pl.when((m == 0) & (q == 1))
        def _():
            pl.when(j == NT)(lambda: w1_fo().wait_recv())
            pl.when(j == NR)(lambda: w1_c(j).wait_recv())
            pl.when(j == N1)(lambda: (w1_ce().wait_recv(), w1_fe().wait_recv()) and None)

        @pl.when(first & (q == 0))
        def _():
            w1_y(j).wait_recv()
            w1_f(j).start()

            @pl.when(j + AHEAD < NT)
            def _():
                w1_y(j + AHEAD).start()

            @pl.when(j + AHEAD == NT)
            def _():
                for t in range(len(tail)):
                    w1_yt(t).start()
                w1_e().start()
                w2_e().start()

            @pl.when(j == 2)
            def _():
                for t in range(NX // 2, NX):
                    xn_x(t).start()

            @pl.when(j == 4)
            def _():
                for k in range(N2):
                    w2_c(k).start()

        @pl.when(first & (q == 1))
        def _():
            w1_c(j).wait_recv()
            w1_f(j).wait_recv()

        for at, lo, hi in ((first2, 0, 4), (first3, 4, 6), (first4, 6, 8)):

            @pl.when(s == at)
            def _():
                for t in range(lo, hi):
                    xn_x(t).wait_recv()

    def load1(s, aslot, wslot, a_new, w_new):
        j, q, m = _step1(s)
        pl.when(a_new)(lambda: a1_in(m, aslot, True))
        pl.when(w_new)(lambda: w1_in(j, q, wslot, True))

    def h_out(s, i, go):
        j, q, m = _step1(s)
        r0, _ = tile_rows(m)
        slot = s % 2
        full = fr - t0

        def part(at, w, col, sem):
            c = pltpu.make_async_copy(
                hout.at[slot, pl.ds(pl.multiple_of(i * sub, sub), sub), at : at + w],
                h.at[hrows(r0 + i), pl.ds(pl.multiple_of(col, c1 - full), w)],
                h_sem.at[sem, i],
            )
            c.start() if go else c.wait()

        own, ext = kr + q * ce, kr + (2 + q) * ce
        pl.when(j < NT)(lambda: part(0, c1, q * fr + j * c1, slot))

        @pl.when(j == NT)
        def _():
            part(0, full, q * fr + t0, slot)
            part(full, c1 - full, own, 2 + slot)

        pl.when(j == NR)(lambda: part(0, c1, own + c1 - full, slot))
        pl.when(j == N1)(lambda: part(0, c1, ext, slot))
        pl.when(j > N1)(lambda: part(0, ce - c1, ext + c1, slot))

    def h_done(s):
        _, two = tile_rows(_step1(s)[2])
        h_out(s, 0, False)
        pl.when(two)(lambda: h_out(s, 1, False))

    def first_product(lo, hi):
        arrive1(lo)
        load1(lo, 0, 0, True, True)

        def step(s, carry):
            aslot, wslot, a_fresh, w_fresh = carry
            j, q, m = _step1(s)
            nj, nq, nm = _step1(s + 1)
            more = s + 1 < hi
            a_new = more & (nm != m)
            w_new = more & ((nj != j) | (nq != q))
            na = _where(a_new, 1 - aslot, aslot)
            nw = _where(w_new, 1 - wslot, wslot)
            pl.when(more)(lambda: arrive1(s + 1))
            load1(s + 1, na, nw, a_new, w_new)
            pl.when(a_fresh == 1)(lambda: a1_in(m, aslot, False))
            pl.when(w_fresh == 1)(lambda: w1_in(j, q, wslot, False))
            pl.when(s >= lo + 2)(lambda: h_done(s - 2))
            _, two = tile_rows(m)

            @pl.loop(0, _where(two, 2, 1))
            def _(i):
                u = jnp.dot(
                    act[aslot, :, pl.ds(pl.multiple_of(i * d, d), d)], wb[wslot, :d], preferred_element_type=F32
                )
                hout[s % 2, pl.ds(pl.multiple_of(i * sub, sub), sub)] = jax.nn.gelu(u, approximate=True).astype(BF16)
                h_out(s, i, True)

            return na, nw, _where(a_new, 1, 0), _where(w_new, 1, 0)

        one, nil = jnp.int32(1), jnp.int32(0)
        lax.fori_loop(lo, hi, step, (nil, nil, one, one))
        h_done(hi - 2)
        h_done(hi - 1)

    def p_in(i, k, slot):
        return pltpu.make_async_copy(precv.at[hrows(i), cols2(k)], pin.at[slot], in_sem.at[slot, 2])

    def a2_in(typ, k, i, slot, go):
        r = _where(typ == REM, 4, 0) + i

        def wait_or_start(c):
            c.start() if go else c.wait()

        @pl.when(typ != END)
        def _():
            wait_or_start(pltpu.make_async_copy(h.at[hrows(r), :kr], act.at[slot, :, :kr], act_sem.at[slot, 0]))

        @pl.when(typ == END)
        def _():
            wait_or_start(
                pltpu.make_async_copy(h.at[hrows(r), kr : kr + ke], act.at[slot, :, :ke], act_sem.at[slot, 0])
            )
            ycol = pl.multiple_of(_where(k < N2, near, away) + (k % N2) * c2, c2)
            wait_or_start(pltpu.make_async_copy(pown.at[hrows(i), cols2(k)], pback.at[slot], in_sem.at[slot, 0]))
            wait_or_start(pltpu.make_async_copy(x.at[hrows(i), pl.ds(ycol, c2)], xin.at[slot], in_sem.at[slot, 1]))
            if go:

                @pl.when((k < LAST) | (i < 2))
                def _():
                    p_x(i, k).wait_recv()
                    p_in(i, k, slot).start()

    def w2_in(typ, k, slot, go):
        def load(n, at, rows_, ref, from_, kk):
            c = pltpu.make_async_copy(
                ref.at[pl.ds(from_, rows_), cols2(kk)], wb.at[slot, at : at + rows_], w_sem.at[slot, n]
            )
            c.start() if go else c.wait()

        def main(own, sib, kk):
            load(0, 0, fr, own, 0, kk)
            load(1, fr, fr, sib, 0, kk)

        def rest(own, ext, ext_at, sib, kk):
            for n, (ref, from_) in enumerate(((own, fr), (sib, fr), (ext, ext_at), (sib, fq))):
                load(n, n * ce, ce, ref, from_, kk)

        def both(side, kk, own, ext, ext_at, sib):
            pl.when(side & (typ != END))(lambda: main(own, sib, kk))
            pl.when(side & (typ == END))(lambda: rest(own, ext, ext_at, sib, kk))

        if not go:
            pl.when(typ != END)(lambda: main(w2far, w2sf, 0))
            pl.when(typ == END)(lambda: rest(w2far, w2far, fq, w2sf, 0))
            return
        both(k < N2, k, w2, w2e, 0, w2so)
        both(k >= N2, k - N2, w2far, w2far, fq, w2sf)

    def arrive2(v):
        at = {visit: n for n, visit in enumerate(VISITS)}
        for n in range(len(VISITS)):
            visit = VISITS[n]
            todo = []
            for u in SEND_F.get(visit, ()):
                todo.append(lambda u=u: w2_yf(u).start())
            for g in SEND_G.get(visit, ()):
                todo.append(lambda g=g: [c.start() for c in w2_yg(g)])
            if visit in PASS_F:
                u = PASS_F[visit]
                todo.append(lambda u=u: (w2_yf(u).wait_recv(), w2_ff(u).start()))
            if visit in PASS_G:
                g = PASS_G[visit]
                todo.append(lambda g=g: ([c.wait_recv() for c in w2_yg(g)], w2_fg(g).start()))
            if visit[0] == REM:
                k = visit[1]
                todo.append(lambda k=k: w2_c(k).wait_recv() if k < N2 else w2_ff(k - N2).wait_recv())
            if n == min(at[B(k)] for k in range(N2)):
                todo.append(lambda: w2_ce().wait_recv())
            if visit[0] == END and visit[1] >= N2:
                todo.append(lambda g=visit[1] - N2: w2_fg(g).wait_recv())
            if todo:

                @pl.when(v == n)
                def _(todo=todo):
                    for f in todo:
                        f()

    def p_out(to, k, i, slot):
        return pltpu.make_async_copy(pout.at[slot], to.at[hrows(i), cols2(k)], out_sem.at[slot])

    def y_out(k, i):
        ycol = pl.multiple_of(_where(k < N2, near, away) + (k % N2) * c2, c2)
        return pltpu.make_async_copy(yout, y.at[hrows(i), pl.ds(ycol, c2)], out_sem.at[2])

    def last_out(to, slot):
        return pltpu.make_async_copy(pout.at[slot], to, out_sem.at[slot])

    def finish(typ, k, i, slot):
        outside = (k == LAST) & (i >= 2)

        @pl.when((typ == REM) | (typ == OWN) | ((typ == END) & outside))
        def _():
            p_out(pown, k, i, slot).wait()

        @pl.when((typ == REM) & ((k < LAST) | (i < 3)))
        def _():
            p_x(i, k).start()

        @pl.when((typ == END) & jnp.logical_not(outside))
        def _():
            y_out(k, i).wait()

    def second_product(lo, hi):
        arrive2(lo)
        typ0, k0 = _visit(lo)
        w2_in(typ0, k0, 0, True)
        a2_in(typ0, k0, jnp.int32(0), 0, True)

        def visit(v, carry):
            typ, k, ptyp, pk = carry
            more = v + 1 < hi
            ntyp, nk = _visit(v + 1)
            wslot = (v - lo) % 2

            def tile(i, before):
                btyp, bk, bi = before
                slot = i % 2
                last = i == 3

                @pl.when(more | (i < 3))
                def _():
                    a2_in(_where(last, ntyp, typ), _where(last, nk, k), _where(last, 0, i + 1), 1 - slot, True)

                @pl.when(last & more)
                def _():
                    arrive2(v + 1)
                    w2_in(ntyp, nk, 1 - wslot, True)

                a2_in(typ, k, i, slot, False)
                pl.when(i == 0)(lambda: w2_in(typ, k, wslot, False))

                @pl.when(typ != END)
                def _():
                    pout[slot] = jnp.dot(act[slot, :, :kr], wb[wslot, :kr], preferred_element_type=F32)

                @pl.when(typ == END)
                def _():
                    pout[slot] = jnp.dot(act[slot, :, :ke], wb[wslot, :ke], preferred_element_type=F32)

                finish(btyp, bk, bi, 1 - slot)
                pl.when(typ == OWN)(lambda: p_out(pown, k, i, slot).start())
                outside = (k == LAST) & (i >= 2)
                inside = jnp.logical_not(outside)
                final = (k == LAST) & last
                pl.when((typ == REM) & jnp.logical_not(final))(lambda: p_out(psend, k, i, slot).start())
                pl.when((typ == REM) & final)(lambda: last_out(xlast, slot).start())

                @pl.when((typ == END) & outside)
                def _():
                    pout[slot] = pback[slot] + pout[slot]
                    last_out(olast.at[pl.ds(pl.multiple_of((i - 2) * sub, sub), sub)], slot).start()

                @pl.when((typ == END) & inside)
                def _():
                    p_in(i, k, slot).wait()
                    total = (pback[slot] + pout[slot]) + pin[slot]
                    yout[...] = (xin[slot].astype(F32) + total).astype(BF16)
                    y_out(k, i).start()

                return typ, k, i

            ptyp, pk, _ = lax.fori_loop(0, 4, tile, (ptyp, pk, jnp.int32(3)))
            return ntyp, nk, ptyp, pk

        _, _, ptyp, pk = lax.fori_loop(lo, hi, visit, (typ0, k0, jnp.int32(3), jnp.int32(0)))
        finish(ptyp, pk, jnp.int32(3), 1)

    def junction():
        final = len(tail) - 1

        def lanes(t):
            at = 0 if t < 2 else 2 * sum(w for _, w in tail[1:t])
            return (0 if t == 0 else d), at

        def w_tail(t, part):
            refs = ((w1, w1so), (w1far, w1sf))[part]
            r, at = lanes(t)
            w = tail[t][1]
            return [
                pltpu.make_async_copy(
                    refs[q].at[cols_t(t)],
                    wb.at[0, r + part * half : r + (part + 1) * half, at + q * w : at + (q + 1) * w],
                    tail_sem.at[t, part, q],
                )
                for q in BOTH
            ]

        def xn_in(i):
            return pltpu.make_async_copy(xn.at[hrows(4 + i)], act.at[1, :, :d], act_sem.at[1, 0])

        def h_at(i, q, col, width):
            return h.at[hrows(4 + i), q * fr + col : q * fr + col + width]

        def h_in(i):
            return [
                pltpu.make_async_copy(h_at(i, q, 0, t0), act.at[0, :, q * fr : q * fr + t0], act_sem.at[0, q])
                for q in BOTH
            ]

        def first_sum(block):
            return remote(pout.at[0, block], precv.at[block, :c2], p_s.at[0], p_r.at[0], to_x)

        def hidden(t, block=everything):
            r, at = lanes(t)
            u = jnp.dot(act[1, block, :d], wb[0, r : r + d, at : at + 2 * tail[t][1]], preferred_element_type=F32)
            return jax.nn.gelu(u, approximate=True).astype(BF16)

        def arrive(t, meanwhile=lambda: None):
            w1_yt(t).wait_recv()
            w1_ft(t).start()
            w_tail(t, 1)[0].start()
            meanwhile()
            if t == final:
                w1_yo().start()
                w1_e().wait_recv()
                w1_ye().start()
                w2_yf(0).start()
                w2_yf(1).start()
                w2_e().wait_recv()
            w1_ft(t).wait_recv()
            w_tail(t, 1)[1].start()
            if t == final:
                w1_ce().start()
                w2_ce().start()
            for part in BOTH:
                for c in w_tail(t, part):
                    c.wait()

        w1_c(NT).wait_recv()
        for t in range(len(tail)):
            for c in w_tail(t, 0):
                c.start()
        xn_in(0).start()
        rem, zero = jnp.int32(REM), jnp.int32(0)

        def rest():
            for c in h_in(0):
                c.start()
            w2_c(0).wait_recv()
            w2_in(rem, zero, 1, True)

        arrive(0, rest)

        def tile_(i, carry):
            xn_in(i).wait()
            out = []
            for t in range(final):
                if t > 0:
                    pl.when(i == 0)(lambda t=t: arrive(t))
                g = hidden(t)
                if t == 0:
                    for c in h_in(i):
                        c.wait()
                off, w = tail[t]
                for q in BOTH:
                    at = q * fr + t0 + off
                    act[0, :, at : at + w] = g[:, q * w : (q + 1) * w]
                    out.append(
                        pltpu.make_async_copy(act.at[0, :, at : at + w], h_at(i, q, t0 + off, w), h_sem.at[t, q])
                    )
                    out[-1].start()
            pl.when(i == 0)(lambda: w2_in(rem, zero, 1, False))
            off, w = tail[final]
            n = fr - w
            slot = _where(i == 0, 0, 1)
            pout[slot] = jnp.dot(act[0, :, :n], wb[1, :n], preferred_element_type=F32) + jnp.dot(
                act[0, :, fr : fr + n], wb[1, fr : fr + n], preferred_element_type=F32
            )
            for c in out:
                c.wait()

            @pl.when(i < 3)
            def _():
                for c in h_in(i + 1):
                    c.start()

            pl.when(i == 0)(lambda: arrive(final))
            block = sub // 2

            @pl.loop(0, 2)
            def _(m):
                at = pl.ds(pl.multiple_of(m * block, block), block)
                g = hidden(final, at)
                hout[0, at, :2 * w] = g
                pout[slot, at] += jnp.dot(g[:, :w], wb[1, n:fr], preferred_element_type=F32) + jnp.dot(
                    g[:, w : 2 * w], wb[1, fr + n : kr], preferred_element_type=F32
                )
                pl.when(i == 0)(lambda: first_sum(at).start())

            pl.when(i < 3)(lambda: xn_in(i + 1).start())
            out = []
            for q in BOTH:
                out.append(
                    pltpu.make_async_copy(
                        hout.at[0, :sub, q * w : (q + 1) * w], h_at(i, q, t0 + off, w), h_sem.at[2, q]
                    )
                )
                out[-1].start()

            @pl.when(i > 0)
            def _():
                sent = p_out(psend, zero, i, 1)
                sent.start()
                sent.wait()
                p_x(i, 0).start()

            for c in out:
                c.wait()
            return carry

        lax.fori_loop(0, 4, tile_, jnp.int32(0))
        p_x(0, 0).wait_send()

    @pl.loop(0, 2)
    def _(phase):
        early = phase == 0
        cut = starts1[BREAK1]
        first_product(_where(early, 0, cut), _where(early, cut, total1))
        pl.when(early)(junction)
        second_product(_where(early, 0, BREAK2), _where(early, BREAK2, len(VISITS)))

    p_x(2, LAST).wait_recv()

    @pl.loop(0, N1)
    def _(j):
        w1_c(j).wait_send()

    @pl.loop(0, NT)
    def _(j):
        w1_y(j).wait_send()
        w1_f(j).wait_send()

    for c in (w1_yo(), w1_ye(), w1_fo(), w1_fe(), w1_ce()):
        c.wait_send()

    for t in range(len(tail)):
        w1_yt(t).wait_send()
        w1_ft(t).wait_send()

    @pl.loop(0, N2)
    def _(k):
        w2_yf(k).wait_send()
        w2_c(k).wait_send()
        w2_ff(k).wait_send()

    w1_e().wait_send()
    w2_e().wait_send()
    w2_ce().wait_send()
    for g in range(N2):
        for c in w2_yg(g):
            c.wait_send()
        w2_fg(g).wait_send()

    @pl.loop(0, NX)
    def _(t):
        xn_x(t).wait_send()

    @pl.loop(1, 2 * N2 * 4 - 1)
    def _(s):
        p_x(s % 4, s // 4).wait_send()


PUTS = 16


def _put(src, dst, buf, sems_in, sems_out):
    n = src.shape[0] // PUTS

    def get(i):
        return pltpu.make_async_copy(src.at[i * n : (i + 1) * n], buf.at[i], sems_in.at[i])

    def put(i):
        return pltpu.make_async_copy(buf.at[i], dst.at[i * n : (i + 1) * n], sems_out.at[i])

    for i in range(PUTS):
        get(i).start()
    for i in range(PUTS):
        get(i).wait()
        put(i).start()
    for i in range(PUTS):
        put(i).wait()


def solution(mesh):
    def body(x, gamma, w1, w2):
        rows, d = x.shape
        half, fq = w1.shape
        sub = rows // 4
        c1, c2 = fq // N1, half // N2
        ce = fq - NT * c1 - sum(w for _, w in _tail(c1))

        def hbm(*shape, dtype=BF16):
            return jax.ShapeDtypeStruct(shape, dtype)

        dma = pltpu.SemaphoreType.DMA
        outs = (
            hbm(rows, d),
            hbm(sub, c2, dtype=F32),
            hbm(2 * sub, c2, dtype=F32),
            hbm(2 * rows, d),
            hbm(half, 2 * c1), *[hbm(half, fq + 2 * c1) for _ in range(3)],
            hbm(ce, half), *[hbm(fq + ce, half) for _ in range(3)],
            hbm(2 * rows, 2 * (fq + ce)),
            hbm(rows, d, dtype=F32), hbm(rows, d, dtype=F32), hbm(rows, d, dtype=F32),
        )
        sent = (NX, 2, N1 + 3, N1 + 1, N1 + 3, 3 * N2, N2 + 1, 2 * N2, 8 * N2)
        out = pl.pallas_call(
            _kernel,
            name="mlp",
            out_shape=outs,
            in_specs=[pl.BlockSpec(memory_space=pl.ANY)] * 4,
            out_specs=tuple([pl.BlockSpec(memory_space=pl.ANY)] * len(outs)),
            scratch_shapes=[
                pltpu.VMEM((2, sub, 2 * d), BF16),
                pltpu.VMEM((2, 2 * fq, c2), BF16),
                pltpu.VMEM((2, 2 * sub, c1), BF16),
                pltpu.VMEM((2, sub, c2), F32),
                pltpu.VMEM((2, sub, c2), F32),
                pltpu.VMEM((2, sub, c2), F32),
                pltpu.VMEM((2, sub, c2), BF16),
                pltpu.VMEM((sub, c2), BF16),
                pltpu.VMEM((1, d), F32),
                *(dma(n) for n in ((2, 2), (2, 4), (4, 2), (3,), (3,), (2, 3), (2, 2, 2))),
                *(dma((n,)) for n in sent for _ in BOTH),
            ],
            compiler_params=pltpu.CompilerParams(
                collective_id=0, has_side_effects=True, vmem_limit_bytes=67_000_000
            ),
        )(x, gamma.reshape(1, d), w1, w2)
        got = lax.ppermute(out[1], "tp", [(i, (i + 2) % 4) for i in range(4)])
        y = pl.pallas_call(
            _put,
            name="put",
            out_shape=hbm(rows, d),
            in_specs=[pl.BlockSpec(memory_space=pl.ANY)],
            out_specs=pl.BlockSpec(memory_space=pl.ANY),
            scratch_shapes=[pltpu.VMEM((PUTS, rows // PUTS, d), BF16), dma((PUTS,)), dma((PUTS,))],
            compiler_params=pltpu.CompilerParams(vmem_limit_bytes=40_000_000),
            cost_estimate=pl.CostEstimate(flops=30_000_000_000, bytes_accessed=4 * rows * d, transcendentals=0),
        )(out[0])
        col = (1 - lax.axis_index("fsdp")) * half + (N2 - 1) * c2
        recv = (out[-1][2 * sub : 3 * sub, LAST * c2 :], got)
        for i in BOTH:
            at = ((2 + i) * sub, col)
            total = out[2][i * sub : (i + 1) * sub] + recv[i]
            y = lax.dynamic_update_slice(y, (lax.dynamic_slice(x, at, (sub, c2)).astype(F32) + total).astype(BF16), at)
        return y

    return jax.shard_map(
        body,
        mesh=mesh,
        in_specs=(P(("fsdp", "tp"), None), P(None), P("fsdp", "tp"), P("tp", "fsdp")),
        out_specs=P(("fsdp", "tp"), None),
        check_vma=False,
    )
```

```python
import jax
import jax.numpy as jnp
from jax import lax
from jax.experimental import pallas as pl
from jax.experimental.pallas import tpu as pltpu
from jax.sharding import PartitionSpec as P

EPS = 1e-6
F32 = jnp.float32
BF16 = jnp.bfloat16
MESH = pl.DeviceIdType.MESH

N1 = 12
NR = N1 - 1
NT = NR - 1
N2 = 6
NX = 8
BOTH = range(2)
AHEAD = 3

STEPS1 = (
    ((0, 4), (0, 2)),
    ((0, 4), (2, 1)),
    ((4, 2), (0, 3)),
    ((0, 3), (4, 1)),
    ((6, 1), (0, 3)),
    ((3, 4), (4, 1)),
    ((7, 1), (2, 1)),
    ((7, 1), (4, 1)),
    ((0, 8), (5, 1)),
    ((8, 2), (2, 2)),
    ((7, 7), (0, 2)),
)
BREAK1 = 10

REM, OWN, END = 0, 1, 2
LAST = 2 * N2 - 1
R, A, B = ((lambda k, t=t: (t, k)) for t in (REM, OWN, END))
VISITS = (
    *map(R, range(1, 6)),
    A(0), A(1), R(6), A(2), B(0), B(1), A(3), R(7), B(2), A(4), A(5), R(8), B(3), A(6), A(7), B(4), B(5),
    R(9), A(8), A(9), R(10), A(10), R(11), A(11), *map(B, range(N2, N2 + N2)),
)
BREAK2 = 4
PASS_F = {A(1): 0, B(1): 1, A(5): 2, B(5): 3, A(9): 4, R(11): 5}
PASS_G = {A(11): 0, B(6): 1, B(7): 2, B(9): 3, B(10): 4, B(11): 5}
SEND_F = {R(2): (2,), R(5): (3, 4), R(7): (5,)}
SEND_G = {R(7): range(N2)}


def _tail(c1):
    w = c1 // 2
    return ((0, w), (w, w // 2))


def _where(cond, a, b):
    return jnp.where(cond, jnp.int32(a), jnp.int32(b))


def _bounds1():
    at, out = 0, []
    for (_, nj), (_, nt) in STEPS1:
        out.append(at)
        at += nj * 2 * nt
    return out, at


def _step1(s):
    starts, _ = _bounds1()
    rows = [(at, j0, nt, t0) for at, ((j0, _), (t0, nt)) in zip(starts, STEPS1)]
    start, j0, nt, t0 = (jnp.int32(v) for v in rows[0])
    for row in rows[1:]:
        late = s >= row[0]
        start, j0, nt, t0 = (_where(late, new, old) for new, old in zip(row, (start, j0, nt, t0)))
    u = s - start
    pair = u // nt
    return j0 + pair // 2, pair % 2, t0 + u % nt


def _first_tile(j):
    return _where((j >= 7) & (j < NT), 2, 0)


def _visit(v):
    code = jnp.int32(0)
    for n, (t, k) in enumerate(VISITS):
        code = _where(v == n, t * 16 + k, code)
    return code // 16, code % 16


def _kernel(
    x, gamma, w1, w2,
    y, xlast, olast, xn, w1e, w1far, w1so, w1sf, w2e, w2far, w2so, w2sf, h, psend, pown, precv,
    act, wb, hout, pout, pin, pback, xin, yout, gam,
    act_sem, w_sem, h_sem, io_sem, out_sem, in_sem, tail_sem,
    xn_s, xn_r, e_s, e_r, w1y_s, w1y_r, w1c_s, w1c_r, w1f_s, w1f_r,
    w2y_s, w2y_r, w2c_s, w2c_r, w2f_s, w2f_r, p_s, p_r,
):
    a = lax.axis_index("fsdp")
    b = lax.axis_index("tp")
    to_y = {"fsdp": 1 - a}
    to_x = {"tp": lax.rem(b + 2, 4)}
    to_c = {"tp": b + 1 - 2 * lax.rem(b, 2)}
    rows, d = x.shape
    half, fq = w1.shape
    sub = rows // 4
    c1 = fq // N1
    c2 = half // N2
    tail = _tail(c1)
    t0 = NT * c1
    fr = t0 + sum(w for _, w in tail)
    ce = fq - fr
    kr = 2 * fr
    ke = 4 * ce
    piece = rows // NX
    near = pl.multiple_of(a * half, half)
    away = pl.multiple_of((1 - a) * half, half)
    everything = slice(None)

    def remote(src, dst, ssem, rsem, to):
        return pltpu.make_async_remote_copy(
            src_ref=src, dst_ref=dst, send_sem=ssem, recv_sem=rsem, device_id=to, device_id_type=MESH
        )

    def cols1(j):
        return (everything, pl.ds(pl.multiple_of(j * c1, c1), c1))

    def cols2(k):
        return pl.ds(pl.multiple_of(k * c2, c2), c2)

    own_e = (everything, pl.ds(fr, ce))
    ext_e = (everything, pl.ds(fq, ce))

    def w1_y(j):
        return remote(w1.at[cols1(j)], w1far.at[cols1(j)], w1y_s.at[j], w1y_r.at[j], to_y)

    def w1_yo():
        return remote(w1.at[own_e], w1far.at[own_e], w1y_s.at[NR], w1y_r.at[NR], to_y)

    def w1_ye():
        return remote(w1e.at[:, :ce], w1far.at[ext_e], w1y_s.at[N1], w1y_r.at[N1], to_y)

    def w1_c(j):
        return remote(w1.at[cols1(j)], w1so.at[cols1(j)], w1c_s.at[j], w1c_r.at[j], to_c)

    def w1_ce():
        return remote(w1e.at[:, :ce], w1so.at[ext_e], w1c_s.at[N1], w1c_r.at[N1], to_c)

    def w1_f(j):
        return remote(w1far.at[cols1(j)], w1sf.at[cols1(j)], w1f_s.at[j], w1f_r.at[j], to_c)

    def w1_fo():
        return remote(w1far.at[own_e], w1sf.at[own_e], w1f_s.at[NR], w1f_r.at[NR], to_c)

    def w1_fe():
        return remote(w1far.at[ext_e], w1sf.at[ext_e], w1f_s.at[N1], w1f_r.at[N1], to_c)

    def cols_t(t):
        return (everything, pl.ds(t0 + tail[t][0], tail[t][1]))

    def tail_at(t):
        return NT if t == 0 else N1 + t

    def w1_yt(t):
        return remote(w1.at[cols_t(t)], w1far.at[cols_t(t)], w1y_s.at[tail_at(t)], w1y_r.at[tail_at(t)], to_y)

    def w1_ft(t):
        return remote(w1far.at[cols_t(t)], w1sf.at[cols_t(t)], w1f_s.at[tail_at(t)], w1f_r.at[tail_at(t)], to_c)

    def w1_e():
        return remote(w1.at[own_e], w1e.at[:, :ce], e_s.at[0], e_r.at[0], to_x)

    def w2_e():
        return remote(w2.at[fr:fq], w2e, e_s.at[1], e_r.at[1], to_x)

    def w2_yf(k):
        at = (pl.ds(0, fr), cols2(k))
        return remote(w2.at[at], w2far.at[at], w2y_s.at[k], w2y_r.at[k], to_y)

    def w2_yg(g):
        at, to, n = (pl.ds(fr, ce), cols2(g)), (pl.ds(fq, ce), cols2(g)), N2 + g + g
        return (
            remote(w2.at[at], w2far.at[at], w2y_s.at[n], w2y_r.at[n], to_y),
            remote(w2e.at[:, cols2(g)], w2far.at[to], w2y_s.at[n + 1], w2y_r.at[n + 1], to_y),
        )

    def w2_c(k):
        at = (everything, cols2(k))
        return remote(w2.at[at], w2so.at[pl.ds(0, fq), cols2(k)], w2c_s.at[k], w2c_r.at[k], to_c)

    def w2_ce():
        return remote(w2e, w2so.at[fq : fq + ce], w2c_s.at[N2], w2c_r.at[N2], to_c)

    def w2_ff(k):
        at = (pl.ds(0, fr), cols2(k))
        return remote(w2far.at[at], w2sf.at[at], w2f_s.at[k], w2f_r.at[k], to_c)

    def w2_fg(g):
        out = []
        for part, row in enumerate((fr, fq)):
            at, n = (pl.ds(row, ce), cols2(g)), N2 + g + g + part
            out.append(remote(w2far.at[at], w2sf.at[at], w2f_s.at[n], w2f_r.at[n], to_c))
        return out

    def xrows(t):
        return pl.ds(pl.multiple_of(t * piece, piece), piece)

    def xn_x(t):
        return remote(xn.at[xrows(t)], xn.at[xrows(t + NX)], xn_s.at[t], xn_r.at[t], to_x)

    def p_x(i, k):
        at = (pl.ds(pl.multiple_of(i * sub, sub), sub), cols2(k))
        return remote(psend.at[at], precv.at[at], p_s.at[k * 4 + i], p_r.at[k * 4 + i], to_x)

    barrier = pltpu.get_barrier_semaphore()
    for to in (to_y, to_x, to_c):
        pl.semaphore_signal(barrier, inc=1, device_id=to, device_id_type=MESH)
    pl.semaphore_wait(barrier, 3)

    for j in range(AHEAD):
        w1_y(j).start()

    @pl.loop(0, N1)
    def _(j):
        w1_c(j).start()

    def gam_in():
        return [
            pltpu.make_async_copy(gamma.at[:, pl.ds(off, half)], gam.at[:, i * half : (i + 1) * half], io_sem.at[i])
            for i, off in enumerate((near, away))
        ]

    def x_in(t, slot):
        return [
            pltpu.make_async_copy(
                x.at[xrows(t), pl.ds(off, half)],
                act.at[slot, :piece, i * half : (i + 1) * half],
                act_sem.at[slot, i],
            )
            for i, off in enumerate((near, away))
        ]

    for c in gam_in():
        c.start()
    for c in x_in(0, 0):
        c.start()
    for c in gam_in():
        c.wait()

    @pl.loop(0, NX)
    def _(t):
        slot = t % 2

        @pl.when(t + 1 < NX)
        def _():
            for c in x_in(t + 1, 1 - slot):
                c.start()

        for c in x_in(t, slot):
            c.wait()

        @pl.loop(0, piece // 16)
        def _(r):
            at = pl.multiple_of(r * 16, 16)
            xs = act[slot, pl.ds(at, 16), :d].astype(F32)
            xc = xs - jnp.mean(xs, axis=1, keepdims=True)
            var = jnp.mean(xc * xc, axis=1, keepdims=True)
            act[slot, pl.ds(piece + at, 16), :d] = (xc * lax.rsqrt(var + EPS) * gam[...]).astype(BF16)

        out = pltpu.make_async_copy(act.at[slot, piece : 2 * piece, :d], xn.at[xrows(t)], io_sem.at[2])
        out.start()
        out.wait()

        @pl.when(t < NX // 2)
        def _():
            xn_x(t).start()

    def tile_rows(m):
        return _where(m < 4, 2 * m, 2 + m), m < 4

    def hrows(r):
        return pl.ds(pl.multiple_of(r * sub, sub), sub)

    def a1_in(m, slot, go):
        r0, two = tile_rows(m)

        def one(i):
            c = pltpu.make_async_copy(
                xn.at[hrows(r0 + i)], act.at[slot, :, i * d : (i + 1) * d], act_sem.at[slot, i]
            )
            c.start() if go else c.wait()

        one(0)
        pl.when(two)(lambda: one(1))

    def w1_in(j, q, slot, go):
        def load(i, ref, at):
            c = pltpu.make_async_copy(ref.at[at], wb.at[slot, i * half : (i + 1) * half], w_sem.at[slot, i])
            c.start() if go else c.wait()

        if not go:
            for i in BOTH:
                load(i, w1far, cols1(j))
            return
        pl.when((q == 0) & (j < N1))(lambda: load(0, w1, cols1(j)))
        pl.when((q == 0) & (j >= N1))(lambda: load(0, w1e, cols1(j - N1)))
        pl.when(q == 0)(lambda: load(1, w1far, cols1(j)))

        @pl.when(q == 1)
        def _():
            load(0, w1so, cols1(j))
            load(1, w1sf, cols1(j))

    starts1, total1 = _bounds1()
    first2, first3, first4 = (
        next(at for at, (_, (m0, nm)) in zip(starts1, STEPS1) if m0 == m) for m in (2, 4, 5)
    )

    def arrive1(s):
        j, q, m = _step1(s)
        first = (m == _first_tile(j)) & (j < NT)

        @pl.when((m == 0) & (q == 0))
        def _():
            pl.when(j == NT)(lambda: (w1_yo().wait_recv(), w1_fo().start()) and None)
            pl.when(j == N1)(lambda: (w1_ye().wait_recv(), w1_fe().start()) and None)

        @pl.when((m == 0) & (q == 1))
        def _():
            pl.when(j == NT)(lambda: w1_fo().wait_recv())
            pl.when(j == NR)(lambda: w1_c(j).wait_recv())
            pl.when(j == N1)(lambda: (w1_ce().wait_recv(), w1_fe().wait_recv()) and None)

        pl.when((j == NT - 1) & (q == 1) & (m == 3))(lambda: (w1_yt(0).wait_recv(), w1_ft(0).start()) and None)

        @pl.when(first & (q == 0))
        def _():
            w1_y(j).wait_recv()
            w1_f(j).start()

            @pl.when(j + AHEAD < NT)
            def _():
                w1_y(j + AHEAD).start()

            @pl.when(j + AHEAD == NT)
            def _():
                for t in range(len(tail)):
                    w1_yt(t).start()
                w1_e().start()
                w2_e().start()

            @pl.when(j == 2)
            def _():
                for t in range(NX // 2, NX):
                    xn_x(t).start()

            @pl.when(j == 4)
            def _():
                for k in range(N2):
                    w2_c(k).start()

        @pl.when(first & (q == 1))
        def _():
            w1_c(j).wait_recv()
            w1_f(j).wait_recv()

        for at, lo, hi in ((first2, 0, 4), (first3, 4, 6), (first4, 6, 8)):

            @pl.when(s == at)
            def _():
                for t in range(lo, hi):
                    xn_x(t).wait_recv()

    def load1(s, aslot, wslot, a_new, w_new):
        j, q, m = _step1(s)
        pl.when(a_new)(lambda: a1_in(m, aslot, True))
        pl.when(w_new)(lambda: w1_in(j, q, wslot, True))

    def h_out(s, i, go):
        j, q, m = _step1(s)
        r0, _ = tile_rows(m)
        slot = s % 2
        full = fr - t0

        def part(at, w, col, sem):
            c = pltpu.make_async_copy(
                hout.at[slot, pl.ds(pl.multiple_of(i * sub, sub), sub), at : at + w],
                h.at[hrows(r0 + i), pl.ds(pl.multiple_of(col, c1 - full), w)],
                h_sem.at[sem, i],
            )
            c.start() if go else c.wait()

        own, ext = kr + q * ce, kr + (2 + q) * ce
        pl.when(j < NT)(lambda: part(0, c1, q * fr + j * c1, slot))

        @pl.when(j == NT)
        def _():
            part(0, full, q * fr + t0, slot)
            part(full, c1 - full, own, 2 + slot)

        pl.when(j == NR)(lambda: part(0, c1, own + c1 - full, slot))
        pl.when(j == N1)(lambda: part(0, c1, ext, slot))
        pl.when(j > N1)(lambda: part(0, ce - c1, ext + c1, slot))

    def h_done(s):
        _, two = tile_rows(_step1(s)[2])
        h_out(s, 0, False)
        pl.when(two)(lambda: h_out(s, 1, False))

    def first_product(lo, hi):
        arrive1(lo)
        load1(lo, 0, 0, True, True)

        def step(s, carry):
            aslot, wslot, a_fresh, w_fresh = carry
            j, q, m = _step1(s)
            nj, nq, nm = _step1(s + 1)
            more = s + 1 < hi
            a_new = more & (nm != m)
            w_new = more & ((nj != j) | (nq != q))
            na = _where(a_new, 1 - aslot, aslot)
            nw = _where(w_new, 1 - wslot, wslot)
            pl.when(more)(lambda: arrive1(s + 1))
            load1(s + 1, na, nw, a_new, w_new)
            pl.when(a_fresh == 1)(lambda: a1_in(m, aslot, False))
            pl.when(w_fresh == 1)(lambda: w1_in(j, q, wslot, False))
            pl.when(s >= lo + 2)(lambda: h_done(s - 2))
            _, two = tile_rows(m)

            @pl.loop(0, _where(two, 2, 1))
            def _(i):
                u = jnp.dot(
                    act[aslot, :, pl.ds(pl.multiple_of(i * d, d), d)], wb[wslot, :d], preferred_element_type=F32
                )
                hout[s % 2, pl.ds(pl.multiple_of(i * sub, sub), sub)] = jax.nn.gelu(u, approximate=True).astype(BF16)
                h_out(s, i, True)

            return na, nw, _where(a_new, 1, 0), _where(w_new, 1, 0)

        one, nil = jnp.int32(1), jnp.int32(0)
        lax.fori_loop(lo, hi, step, (nil, nil, one, one))
        h_done(hi - 2)
        h_done(hi - 1)

    def p_in(i, k, slot):
        return pltpu.make_async_copy(precv.at[hrows(i), cols2(k)], pin.at[slot], in_sem.at[slot, 2])

    def a2_in(typ, k, i, slot, go):
        r = _where(typ == REM, 4, 0) + i

        def wait_or_start(c):
            c.start() if go else c.wait()

        @pl.when(typ != END)
        def _():
            wait_or_start(pltpu.make_async_copy(h.at[hrows(r), :kr], act.at[slot, :, :kr], act_sem.at[slot, 0]))

        @pl.when(typ == END)
        def _():
            wait_or_start(
                pltpu.make_async_copy(h.at[hrows(r), kr : kr + ke], act.at[slot, :, :ke], act_sem.at[slot, 0])
            )
            ycol = pl.multiple_of(_where(k < N2, near, away) + (k % N2) * c2, c2)
            wait_or_start(pltpu.make_async_copy(pown.at[hrows(i), cols2(k)], pback.at[slot], in_sem.at[slot, 0]))
            wait_or_start(pltpu.make_async_copy(x.at[hrows(i), pl.ds(ycol, c2)], xin.at[slot], in_sem.at[slot, 1]))
            if go:

                @pl.when((k < LAST) | (i < 2))
                def _():
                    p_x(i, k).wait_recv()
                    p_in(i, k, slot).start()

    def w2_in(typ, k, slot, go):
        def load(n, at, rows_, ref, from_, kk):
            c = pltpu.make_async_copy(
                ref.at[pl.ds(from_, rows_), cols2(kk)], wb.at[slot, at : at + rows_], w_sem.at[slot, n]
            )
            c.start() if go else c.wait()

        def main(own, sib, kk):
            load(0, 0, fr, own, 0, kk)
            load(1, fr, fr, sib, 0, kk)

        def rest(own, ext, ext_at, sib, kk):
            load(0, 0, ce, own, fr, kk)
            load(2, 2 * ce, ce, ext, ext_at, kk)
            if go and sib is w2sf:
                for c in w2_fg(kk):
                    c.wait_recv()
            load(1, ce, ce, sib, fr, kk)
            load(3, 3 * ce, ce, sib, fq, kk)

        def both(side, kk, own, ext, ext_at, sib):
            pl.when(side & (typ != END))(lambda: main(own, sib, kk))
            pl.when(side & (typ == END))(lambda: rest(own, ext, ext_at, sib, kk))

        if not go:
            pl.when(typ != END)(lambda: main(w2far, w2sf, 0))
            pl.when(typ == END)(lambda: rest(w2far, w2far, fq, w2sf, 0))
            return
        both(k < N2, k, w2, w2e, 0, w2so)
        both(k >= N2, k - N2, w2far, w2far, fq, w2sf)

    def arrive2(v):
        at = {visit: n for n, visit in enumerate(VISITS)}
        for n in range(len(VISITS)):
            visit = VISITS[n]
            todo = []
            for u in SEND_F.get(visit, ()):
                todo.append(lambda u=u: w2_yf(u).start())
            for g in SEND_G.get(visit, ()):
                todo.append(lambda g=g: [c.start() for c in w2_yg(g)])
            if visit in PASS_F:
                u = PASS_F[visit]
                todo.append(lambda u=u: (w2_yf(u).wait_recv(), w2_ff(u).start()))
            if visit in PASS_G:
                g = PASS_G[visit]
                todo.append(lambda g=g: [(c.wait_recv(), f.start()) for c, f in zip(w2_yg(g), w2_fg(g))])
            if visit[0] == REM:
                k = visit[1]
                todo.append(lambda k=k: w2_c(k).wait_recv() if k < N2 else w2_ff(k - N2).wait_recv())
            if n == min(at[B(k)] for k in range(N2)):
                todo.append(lambda: w2_ce().wait_recv())
            if todo:

                @pl.when(v == n)
                def _(todo=todo):
                    for f in todo:
                        f()

    def p_out(to, k, i, slot):
        return pltpu.make_async_copy(pout.at[slot], to.at[hrows(i), cols2(k)], out_sem.at[slot])

    def y_out(k, i):
        ycol = pl.multiple_of(_where(k < N2, near, away) + (k % N2) * c2, c2)
        return pltpu.make_async_copy(yout, y.at[hrows(i), pl.ds(ycol, c2)], out_sem.at[2])

    def last_out(to, slot):
        return pltpu.make_async_copy(pout.at[slot], to, out_sem.at[slot])

    def finish(typ, k, i, slot):
        outside = (k == LAST) & (i >= 2)

        @pl.when((typ == REM) | (typ == OWN) | ((typ == END) & outside))
        def _():
            p_out(pown, k, i, slot).wait()

        @pl.when((typ == REM) & ((k < LAST) | (i < 3)))
        def _():
            p_x(i, k).start()

        @pl.when((typ == END) & jnp.logical_not(outside))
        def _():
            y_out(k, i).wait()

    def second_product(lo, hi):
        arrive2(lo)
        typ0, k0 = _visit(lo)
        w2_in(typ0, k0, 0, True)
        a2_in(typ0, k0, jnp.int32(0), 0, True)

        def visit(v, carry):
            typ, k, ptyp, pk = carry
            more = v + 1 < hi
            ntyp, nk = _visit(v + 1)
            wslot = (v - lo) % 2

            def tile(i, before):
                btyp, bk, bi = before
                slot = i % 2
                last = i == 3

                @pl.when(more | (i < 3))
                def _():
                    a2_in(_where(last, ntyp, typ), _where(last, nk, k), _where(last, 0, i + 1), 1 - slot, True)

                @pl.when(last & more)
                def _():
                    arrive2(v + 1)
                    w2_in(ntyp, nk, 1 - wslot, True)

                a2_in(typ, k, i, slot, False)
                pl.when(i == 0)(lambda: w2_in(typ, k, wslot, False))

                @pl.when(typ != END)
                def _():
                    pout[slot] = jnp.dot(act[slot, :, :kr], wb[wslot, :kr], preferred_element_type=F32)

                @pl.when(typ == END)
                def _():
                    pout[slot] = jnp.dot(act[slot, :, :ke], wb[wslot, :ke], preferred_element_type=F32)

                finish(btyp, bk, bi, 1 - slot)
                pl.when(typ == OWN)(lambda: p_out(pown, k, i, slot).start())
                outside = (k == LAST) & (i >= 2)
                inside = jnp.logical_not(outside)
                final = (k == LAST) & last
                pl.when((typ == REM) & jnp.logical_not(final))(lambda: p_out(psend, k, i, slot).start())
                pl.when((typ == REM) & final)(lambda: last_out(xlast, slot).start())

                @pl.when((typ == END) & outside)
                def _():
                    pout[slot] = pback[slot] + pout[slot]
                    last_out(olast.at[pl.ds(pl.multiple_of((i - 2) * sub, sub), sub)], slot).start()

                @pl.when((typ == END) & inside)
                def _():
                    p_in(i, k, slot).wait()
                    total = (pback[slot] + pout[slot]) + pin[slot]
                    yout[...] = (xin[slot].astype(F32) + total).astype(BF16)
                    y_out(k, i).start()

                return typ, k, i

            ptyp, pk, _ = lax.fori_loop(0, 4, tile, (ptyp, pk, jnp.int32(3)))
            return ntyp, nk, ptyp, pk

        _, _, ptyp, pk = lax.fori_loop(lo, hi, visit, (typ0, k0, jnp.int32(3), jnp.int32(0)))
        finish(ptyp, pk, jnp.int32(3), 1)

    def junction():
        final = len(tail) - 1

        def lanes(t):
            at = 0 if t < 2 else 2 * sum(w for _, w in tail[1:t])
            return (0 if t == 0 else d), at

        def w_tail(t, part):
            refs = ((w1, w1so), (w1far, w1sf))[part]
            r, at = lanes(t)
            w = tail[t][1]
            return [
                pltpu.make_async_copy(
                    refs[q].at[cols_t(t)],
                    wb.at[0, r + part * half : r + (part + 1) * half, at + q * w : at + (q + 1) * w],
                    tail_sem.at[t, part, q],
                )
                for q in BOTH
            ]

        def xn_in(i):
            return pltpu.make_async_copy(xn.at[hrows(4 + i)], act.at[1, :, :d], act_sem.at[1, 0])

        def h_at(i, q, col, width):
            return h.at[hrows(4 + i), q * fr + col : q * fr + col + width]

        def h_in(i):
            return [
                pltpu.make_async_copy(h_at(i, q, 0, t0), act.at[0, :, q * fr : q * fr + t0], act_sem.at[0, q])
                for q in BOTH
            ]

        def first_sum(block):
            return remote(pout.at[0, block], precv.at[block, :c2], p_s.at[0], p_r.at[0], to_x)

        def hidden(t, block=everything):
            r, at = lanes(t)
            u = jnp.dot(act[1, block, :d], wb[0, r : r + d, at : at + 2 * tail[t][1]], preferred_element_type=F32)
            return jax.nn.gelu(u, approximate=True).astype(BF16)

        def reach(t):
            if t == final:
                w1_yt(t).wait_recv()
                w1_ft(t).start()
            w_tail(t, 1)[0].start()
            if t == final:
                w1_yo().start()
                w1_e().wait_recv()
                w1_ye().start()
                w2_yf(0).start()
                w2_yf(1).start()
                w2_e().wait_recv()

        def arrive(t):
            w1_ft(t).wait_recv()
            w_tail(t, 1)[1].start()
            if t == final:
                w1_ce().start()
                w2_ce().start()
            for part in BOTH:
                for c in w_tail(t, part):
                    c.wait()

        w1_c(NT).wait_recv()
        for t in range(len(tail)):
            for c in w_tail(t, 0):
                c.start()
        xn_in(0).start()
        rem, zero = jnp.int32(REM), jnp.int32(0)

        def rest():
            for c in h_in(0):
                c.start()
            w2_c(0).wait_recv()
            w2_in(rem, zero, 1, True)

        reach(0)
        rest()
        arrive(0)

        def tile_(i, carry):
            xn_in(i).wait()
            out = []
            for t in range(final):
                if t > 0:
                    pl.when(i == 0)(lambda t=t: arrive(t))
                g = hidden(t)
                if t == 0:
                    for c in h_in(i):
                        c.wait()
                off, w = tail[t]
                for q in BOTH:
                    at = q * fr + t0 + off
                    act[0, :, at : at + w] = g[:, q * w : (q + 1) * w]
                    out.append(
                        pltpu.make_async_copy(act.at[0, :, at : at + w], h_at(i, q, t0 + off, w), h_sem.at[t, q])
                    )
                    out[-1].start()

            @pl.when(i == 0)
            def _():
                reach(final)
                w2_in(rem, zero, 1, False)

            off, w = tail[final]
            n = fr - w
            slot = _where(i == 0, 0, 1)
            pout[slot] = jnp.dot(act[0, :, :n], wb[1, :n], preferred_element_type=F32) + jnp.dot(
                act[0, :, fr : fr + n], wb[1, fr : fr + n], preferred_element_type=F32
            )
            for c in out:
                c.wait()

            @pl.when(i < 3)
            def _():
                for c in h_in(i + 1):
                    c.start()

            pl.when(i == 0)(lambda: arrive(final))
            block = sub // 2

            @pl.loop(0, 2)
            def _(m):
                at = pl.ds(pl.multiple_of(m * block, block), block)
                g = hidden(final, at)
                hout[0, at, :2 * w] = g
                pout[slot, at] += jnp.dot(g[:, :w], wb[1, n:fr], preferred_element_type=F32) + jnp.dot(
                    g[:, w : 2 * w], wb[1, fr + n : kr], preferred_element_type=F32
                )
                pl.when(i == 0)(lambda: first_sum(at).start())

            pl.when(i < 3)(lambda: xn_in(i + 1).start())
            out = []
            for q in BOTH:
                out.append(
                    pltpu.make_async_copy(
                        hout.at[0, :sub, q * w : (q + 1) * w], h_at(i, q, t0 + off, w), h_sem.at[2, q]
                    )
                )
                out[-1].start()

            @pl.when(i > 0)
            def _():
                sent = p_out(psend, zero, i, 1)
                sent.start()
                sent.wait()
                p_x(i, 0).start()

            for c in out:
                c.wait()
            return carry

        lax.fori_loop(0, 4, tile_, jnp.int32(0))
        p_x(0, 0).wait_send()

    @pl.loop(0, 2)
    def _(phase):
        early = phase == 0
        cut = starts1[BREAK1]
        first_product(_where(early, 0, cut), _where(early, cut, total1))
        pl.when(early)(junction)
        second_product(_where(early, 0, BREAK2), _where(early, BREAK2, len(VISITS)))

    p_x(2, LAST).wait_recv()

    @pl.loop(0, N1)
    def _(j):
        w1_c(j).wait_send()

    @pl.loop(0, NT)
    def _(j):
        w1_y(j).wait_send()
        w1_f(j).wait_send()

    for c in (w1_yo(), w1_ye(), w1_fo(), w1_fe(), w1_ce()):
        c.wait_send()

    for t in range(len(tail)):
        w1_yt(t).wait_send()
        w1_ft(t).wait_send()

    @pl.loop(0, N2)
    def _(k):
        w2_yf(k).wait_send()
        w2_c(k).wait_send()
        w2_ff(k).wait_send()

    w1_e().wait_send()
    w2_e().wait_send()
    w2_ce().wait_send()
    for g in range(N2):
        for c in w2_yg(g):
            c.wait_send()
        for c in w2_fg(g):
            c.wait_send()

    @pl.loop(0, NX)
    def _(t):
        xn_x(t).wait_send()

    @pl.loop(1, 2 * N2 * 4 - 1)
    def _(s):
        p_x(s % 4, s // 4).wait_send()


PUTS = 16


def _put(src, dst, buf, sems_in, sems_out):
    n = src.shape[0] // PUTS

    def get(i):
        return pltpu.make_async_copy(src.at[i * n : (i + 1) * n], buf.at[i], sems_in.at[i])

    def put(i):
        return pltpu.make_async_copy(buf.at[i], dst.at[i * n : (i + 1) * n], sems_out.at[i])

    for i in range(PUTS):
        get(i).start()
    for i in range(PUTS):
        get(i).wait()
        put(i).start()
    for i in range(PUTS):
        put(i).wait()


def solution(mesh):
    def body(x, gamma, w1, w2):
        rows, d = x.shape
        half, fq = w1.shape
        sub = rows // 4
        c1, c2 = fq // N1, half // N2
        ce = fq - NT * c1 - sum(w for _, w in _tail(c1))

        def hbm(*shape, dtype=BF16):
            return jax.ShapeDtypeStruct(shape, dtype)

        dma = pltpu.SemaphoreType.DMA
        outs = (
            hbm(rows, d),
            hbm(sub, c2, dtype=F32),
            hbm(2 * sub, c2, dtype=F32),
            hbm(2 * rows, d),
            hbm(half, 2 * c1), *[hbm(half, fq + 2 * c1) for _ in range(3)],
            hbm(ce, half), *[hbm(fq + ce, half) for _ in range(3)],
            hbm(2 * rows, 2 * (fq + ce)),
            hbm(rows, d, dtype=F32), hbm(rows, d, dtype=F32), hbm(rows, d, dtype=F32),
        )
        sent = (NX, 2, N1 + 3, N1 + 1, N1 + 3, 3 * N2, N2 + 1, 3 * N2, 8 * N2)
        out = pl.pallas_call(
            _kernel,
            name="mlp",
            out_shape=outs,
            in_specs=[pl.BlockSpec(memory_space=pl.ANY)] * 4,
            out_specs=tuple([pl.BlockSpec(memory_space=pl.ANY)] * len(outs)),
            scratch_shapes=[
                pltpu.VMEM((2, sub, 2 * d), BF16),
                pltpu.VMEM((2, 2 * fq, c2), BF16),
                pltpu.VMEM((2, 2 * sub, c1), BF16),
                pltpu.VMEM((2, sub, c2), F32),
                pltpu.VMEM((2, sub, c2), F32),
                pltpu.VMEM((2, sub, c2), F32),
                pltpu.VMEM((2, sub, c2), BF16),
                pltpu.VMEM((sub, c2), BF16),
                pltpu.VMEM((1, d), F32),
                *(dma(n) for n in ((2, 2), (2, 4), (4, 2), (3,), (3,), (2, 3), (2, 2, 2))),
                *(dma((n,)) for n in sent for _ in BOTH),
            ],
            compiler_params=pltpu.CompilerParams(
                collective_id=0, has_side_effects=True, vmem_limit_bytes=67_000_000
            ),
        )(x, gamma.reshape(1, d), w1, w2)
        got = lax.ppermute(out[1], "tp", [(i, (i + 2) % 4) for i in range(4)])
        y = pl.pallas_call(
            _put,
            name="put",
            out_shape=hbm(rows, d),
            in_specs=[pl.BlockSpec(memory_space=pl.ANY)],
            out_specs=pl.BlockSpec(memory_space=pl.ANY),
            scratch_shapes=[pltpu.VMEM((PUTS, rows // PUTS, d), BF16), dma((PUTS,)), dma((PUTS,))],
            compiler_params=pltpu.CompilerParams(vmem_limit_bytes=40_000_000),
            cost_estimate=pl.CostEstimate(flops=30_000_000_000, bytes_accessed=4 * rows * d, transcendentals=0),
        )(out[0])
        col = (1 - lax.axis_index("fsdp")) * half + (N2 - 1) * c2
        recv = (out[-1][2 * sub : 3 * sub, LAST * c2 :], got)
        for i in BOTH:
            at = ((2 + i) * sub, col)
            total = out[2][i * sub : (i + 1) * sub] + recv[i]
            y = lax.dynamic_update_slice(y, (lax.dynamic_slice(x, at, (sub, c2)).astype(F32) + total).astype(BF16), at)
        return y

    return jax.shard_map(
        body,
        mesh=mesh,
        in_specs=(P(("fsdp", "tp"), None), P(None), P("fsdp", "tp"), P("tp", "fsdp")),
        out_specs=P(("fsdp", "tp"), None),
        check_vma=False,
    )
```
